32 devices in a mesh: section: 2 (over y), dp: 4 (over x, core), mp: 4 (over z).
Axes of the slice: x: 2, y: 2, z: 4, core: 2. Of those that a mesh axis runs over, the one named last changes fastest.
Arguments:
- latents_in: bfloat16 [2, 4, 512, 1152], P(None, 'dp', 'mp'), may hold values from -6 to 6
- condition: bfloat16 [2, 4, 1152], P(None, 'dp'), may hold values from -1.5 to 1.5
- cotangent: bfloat16 [2, 4, 512, 1152], P(None, 'dp', 'mp'), may hold values from -6 to 6
- modulation_weight: bfloat16 [2, 1152, 6912], P('section', 'dp', 'mp'), may hold values from -0.1875 to 0.1875
- modulation_bias: bfloat16 [2, 6912], P('section', 'mp'), may hold values from -2.5 to 2.5
- query_key_value_weight: bfloat16 [2, 1152, 3, 1152], P('section', 'dp', None, 'mp'), may hold values from -0.1875 to 0.1875
- query_value_bias: bfloat16 [2, 2, 1152], P('section', None, 'mp'), may hold values from -2.5 to 2.5
- output_proj_weight: bfloat16 [2, 1152, 1152], P('section', 'mp', 'dp'), may hold values from -2 to 2
- output_proj_bias: bfloat16 [2, 1152], P('section'), may hold values from -2.5 to 2.5
- first_dense_weight: bfloat16 [2, 1152, 4608], P('section', 'dp', 'mp'), may hold values from -0.1875 to 0.1875
- first_dense_bias: bfloat16 [2, 4608], P('section', 'mp'), may hold values from -2.5 to 2.5
- second_dense_weight: bfloat16 [2, 4608, 1152], P('section', 'mp', 'dp'), may hold values from -0.09375 to 0.09375
- second_dense_bias: bfloat16 [2, 1152], P('section'), may hold values from -2.5 to 2.5
Outputs:
- acts: bfloat16 [2, 2, 4, 512, 1152], P('section', None, 'dp', 'mp')
- grad_input: float32 [2, 2, 4, 512, 1152], P('section', None, 'dp', 'mp')
- grad_cond: float32 [2, 4, 1152], P(None, 'dp')
- grad_weight_ada: float32 [2, 1152, 6912], P('section', 'dp', 'mp')
- grad_bias_ada: float32 [2, 6912], P('section', ('mp', 'dp'))
- grad_weight_qkv: float32 [2, 1152, 3, 1152], P('section', 'dp', None, 'mp')
- grad_bias_qv: float32 [2, 2, 1152], P('section', None, ('mp', 'dp'))
- grad_weight_proj: float32 [2, 1152, 1152], P('section', 'mp', 'dp')
- grad_bias_proj: float32 [2, 1152], P('section', 'dp')
- grad_weight_fc1: float32 [2, 1152, 4608], P('section', 'dp', 'mp')
- grad_bias_fc1: float32 [2, 4608], P('section', ('mp', 'dp'))
- grad_weight_fc2: float32 [2, 4608, 1152], P('section', 'mp', 'dp')
- grad_bias_fc2: float32 [2, 1152], P('section', 'dp')
The draws below stay inside these ranges and needn't reach their ends.
All inputs are finite; a program needn't handle non-finite values.
Results may differ from the reference program's by a relative error of at most 0.015.
Values may be sent and summed in bfloat16 or wider, within the bound.
A program may use at most 192 MiB of HBM per device.

```python
import jax
import jax.numpy as jnp
from jax import lax

D = 1152
HEADS = 16
HEAD_SIZE = 72
FF = 4608
SEQ = 512
MB = 2
LAT_MB = 1
LAT = 4
N_DP = 4


def block_scale(stream_key, shape, shards, least, largest):
    factor_of, own = 1.0, jax.random.fold_in(stream_key, 6)
    for position, parts in shards:
        draws = jnp.exp(jax.random.uniform(jax.random.fold_in(own, position), (parts,), jnp.float32, least / len(shards), largest / len(shards)))
        factor_of = factor_of * jnp.repeat(draws, shape[position] // parts).reshape([-1 if axis == position else 1 for axis in range(len(shape))])
    return factor_of


def centred(stream_key, extent, scale, bound, cuts=(), dtype=jnp.bfloat16):
    values = scale * jax.random.normal(stream_key, extent, jnp.float32)
    if cuts:
        values = values * block_scale(stream_key, extent, cuts, -0.22, 0.18)
    return jnp.clip(values, -bound, bound).astype(dtype)


def setup_inputs(seed: int = 0) -> dict:
    keys = jax.random.split(jax.random.key(seed), 14)
    latents_in = centred(keys[0], (MB, LAT, SEQ, D), 1.0, 6.0, ((1, 4), (2, 4)))
    condition = jnp.clip(jax.random.uniform(keys[1], (MB, LAT, D), jnp.float32, -1.5, 1.5) * block_scale(keys[1], (MB, LAT, D), ((1, 4),), -0.4, 0.0), -1.5, 1.5).astype(jnp.bfloat16)
    cotangent = centred(keys[2], (MB, LAT, SEQ, D), 1.0, 6.0, ((1, 4), (2, 4)))
    modulation_weight = centred(keys[3], (2, D, 6 * D), D ** -0.5, 0.1875, ((0, 2), (1, 4), (2, 4)))
    modulation_bias = centred(keys[4], (2, 6 * D), 0.4, 2.5, ((0, 2), (1, 4)))
    query_key_value_weight = centred(keys[5], (2, D, 3, D), D ** -0.5, 0.1875, ((0, 2), (1, 4), (3, 4)))
    query_value_bias = centred(keys[6], (2, 2, D), 0.5, 2.5, ((0, 2), (2, 4)))
    output_proj_weight = centred(keys[7], (2, D, D), (max(D // 128, 1)) ** -0.5, 2.0, ((0, 2), (1, 4), (2, 4)))
    output_proj_bias = centred(keys[8], (2, D), 0.5, 2.5, ((0, 2),))
    first_dense_weight = centred(keys[9], (2, D, FF), D ** -0.5, 0.1875, ((0, 2), (1, 4), (2, 4)))
    first_dense_bias = centred(keys[10], (2, FF), 0.5, 2.5, ((0, 2), (1, 4)))
    second_dense_weight = centred(keys[11], (2, FF, D), FF ** -0.5, 0.09375, ((0, 2), (1, 4), (2, 4)))
    second_dense_bias = centred(keys[12], (2, D), 0.5, 2.5, ((0, 2),))
    return dict(latents_in=latents_in, condition=condition, cotangent=cotangent, modulation_weight=modulation_weight, modulation_bias=modulation_bias, query_key_value_weight=query_key_value_weight, query_value_bias=query_value_bias, output_proj_weight=output_proj_weight, output_proj_bias=output_proj_bias, first_dense_weight=first_dense_weight, first_dense_bias=first_dense_bias, second_dense_weight=second_dense_weight, second_dense_bias=second_dense_bias)


@jax.custom_vjp
def low(v):
    return lax.optimization_barrier(v.astype(jnp.bfloat16)).astype(jnp.float32)

@jax.custom_vjp
def reduced_backward(v):
    return v

def low_keep(v):
    return (low(v), None)

def low_pass(kept, grad):
    return (grad,)

def back_keep(v):
    return (v, None)

def back_low(kept, grad):
    return (low(grad),)
low.defvjp(low_keep, low_pass)
reduced_backward.defvjp(back_keep, back_low)
exact_flag = lax.Precision.HIGHEST

def norm_rows(values):
    center = values - lax.optimization_barrier(jnp.mean(values, axis=-1, keepdims=True))
    spread = lax.optimization_barrier(jnp.mean(center * center, axis=-1, keepdims=True))
    return center * lax.rsqrt(spread + 1e-06)

def attend_latent(query_rows, key_input, value_input):
    logit_scores = jnp.einsum('cla,vla->lcv', query_rows, key_input, precision=exact_flag) * HEAD_SIZE ** (-0.5)
    logit_scores = reduced_backward(logit_scores)
    powered = jnp.exp(logit_scores)
    attention_probs = low(powered / lax.optimization_barrier(jnp.sum(powered, axis=-1, keepdims=True)))
    return jnp.einsum('cad,dce->ace', attention_probs, value_input, precision=exact_flag)

def diffusion_layer(hidden_input, condition, modulation_weight, modulation_bias, query_key_value_weight, query_value_bias, output_proj_weight, output_proj_bias, first_dense_weight, first_dense_bias, second_dense_weight, second_dense_bias):
    latent_count = hidden_input.shape[0]
    modul = reduced_backward(jnp.dot(low(jax.nn.silu(condition)), modulation_weight, precision=exact_flag) + modulation_bias)
    pieces = [modul[:, None, block_index * D:(block_index + 1) * D] for block_index in range(6)]
    shift_att, scale_att, gate_att, shift_mlp, scale_mlp, gate_mlp = pieces
    normed = low(norm_rows(hidden_input) * (1.0 + scale_att) + shift_att)
    qkv_bias = jnp.stack([query_value_bias[0], jnp.zeros_like(query_value_bias[0]), query_value_bias[1]])
    project = jnp.einsum('lsd,dcf->lscf', normed, query_key_value_weight, precision=exact_flag) + qkv_bias
    project = reduced_backward(low(project))
    head_shape = (latent_count, SEQ, HEADS, HEAD_SIZE)
    guarded = jax.checkpoint(attend_latent)
    attended_rows = lax.map(lambda triple: guarded(triple[0], triple[1], triple[2]), (project[:, :, 0].reshape(head_shape), project[:, :, 1].reshape(head_shape), project[:, :, 2].reshape(head_shape)))
    attended_rows = reduced_backward(low(attended_rows.reshape(latent_count, SEQ, D)))
    attention_branch = reduced_backward(jnp.einsum('qru,uw->qrw', attended_rows, output_proj_weight, precision=exact_flag) + output_proj_bias)
    middle = hidden_input + gate_att * attention_branch
    dense_normed = low(norm_rows(middle) * (1.0 + scale_mlp) + shift_mlp)
    preactivation = reduced_backward(jnp.einsum('vya,ae->vye', dense_normed, first_dense_weight, precision=exact_flag) + first_dense_bias)
    gelu_result = low(jax.nn.gelu(preactivation, approximate=True))
    dense_branch = reduced_backward(jnp.einsum('qru,uw->qrw', gelu_result, second_dense_weight, precision=exact_flag) + second_dense_bias)
    return middle + gate_mlp * dense_branch

def two_blocks(first_input, bridge_zero, condition, first_parameters, second_parameters):
    first_output = diffusion_layer(first_input, condition, *first_parameters)
    bridge_tensor = reduced_backward(low(first_output)) + bridge_zero
    second_output = diffusion_layer(bridge_tensor, condition, *second_parameters)
    return (low(second_output), low(first_output))

def reference(latents_in, condition, cotangent, modulation_weight, modulation_bias, query_key_value_weight, query_value_bias, output_proj_weight, output_proj_bias, first_dense_weight, first_dense_bias, second_dense_weight, second_dense_bias):
    arrays = tuple((item.astype(jnp.float32) for item in (modulation_weight, modulation_bias, query_key_value_weight, query_value_bias, output_proj_weight, output_proj_bias, first_dense_weight, first_dense_bias, second_dense_weight, second_dense_bias)))
    first_parameters = tuple((item[0] for item in arrays))
    second_parameters = tuple((item[1] for item in arrays))
    group_count = MB * N_DP
    inputs_grouped = latents_in.reshape(group_count, LAT_MB, SEQ, D)
    cond_grouped = condition.reshape(group_count, LAT_MB, D)
    cot_grouped = cotangent.reshape(group_count, LAT_MB, SEQ, D)
    start_sums = (jax.tree.map(jnp.zeros_like, first_parameters), jax.tree.map(jnp.zeros_like, second_parameters))

    def step_group(carry, item):
        group_in, group_cond, group_cot = item
        bridge_zero = jnp.zeros((LAT_MB, SEQ, D), jnp.float32)
        second_output, back_fn, first_output = jax.vjp(two_blocks, group_in.astype(jnp.float32), bridge_zero, group_cond.astype(jnp.float32), first_parameters, second_parameters, has_aux=True)
        grad_first_in, grad_bridge, grad_cond, grads_first, grads_second = back_fn(group_cot.astype(jnp.float32))
        carry = (jax.tree.map(jnp.add, carry[0], grads_first), jax.tree.map(jnp.add, carry[1], grads_second))
        return (carry, (first_output.astype(jnp.bfloat16), second_output.astype(jnp.bfloat16), grad_first_in, grad_bridge, grad_cond))
    sums, outputs = lax.scan(step_group, start_sums, (inputs_grouped, cond_grouped, cot_grouped))
    first_output, second_output, grad_first_in, grad_bridge, grad_cond = outputs
    full_shape = (MB, LAT_MB * N_DP, SEQ, D)
    acts = jnp.stack([first_output.reshape(full_shape), second_output.reshape(full_shape)])
    grad_input = jnp.stack([grad_first_in.reshape(full_shape), grad_bridge.reshape(full_shape)])
    grad_cond_all = grad_cond.reshape(MB, LAT_MB * N_DP, D)
    stacked = tuple((jnp.stack([first_item, second_item]) for first_item, second_item in zip(sums[0], sums[1])))
    return (acts, grad_input, grad_cond_all, stacked[0], stacked[1], stacked[2], stacked[3], stacked[4], stacked[5], stacked[6], stacked[7], stacked[8], stacked[9])
```

```python
import functools

import jax
import jax.numpy as jnp
from jax import lax
from jax.experimental import pallas as pl
from jax.experimental.pallas import tpu as pltpu
from jax.sharding import Mesh
from jax.sharding import PartitionSpec as P

HEAD_SIZE = 72
EPS = 1e-06
MESH = pl.DeviceIdType.MESH
BF16 = jnp.bfloat16
F32 = jnp.float32
GELU_C = 0.7978845608028654
GELU_A = 0.044715
NT = (((1,), (1,)), ((), ()))
TN = (((0,), (0,)), ((), ()))
GROUP = ("section", "ml")
OTHERS = ("mh", "dp")
VMEM_LIMIT = 60 * 1024 * 1024


def dot_nn(a, b):
    return jnp.dot(a, b, preferred_element_type=F32)


def dot_nt(a, b):
    return lax.dot_general(a, b, NT, preferred_element_type=F32)


def dot_tn(a, b):
    return lax.dot_general(a, b, TN, preferred_element_type=F32)


def norm_parts(values):
    center = values - jnp.mean(values, axis=-1, keepdims=True)
    spread = jnp.mean(center * center, axis=-1, keepdims=True)
    rstd = lax.rsqrt(spread + EPS)
    return center * rstd, rstd


def norm_back(grad, normed, rstd, scale):
    dn = grad * (1.0 + scale)
    first = jnp.mean(dn, axis=-1, keepdims=True)
    second = jnp.mean(dn * normed, axis=-1, keepdims=True)
    return (dn - first - normed * second) * rstd


def col_sum(values):
    return jnp.sum(values, axis=0, keepdims=True)


class Group:
    def __init__(self):
        self.low = lax.axis_size("ml")
        self.size = lax.axis_size("section") * self.low
        self.me = lax.axis_index("section") * self.low + lax.axis_index("ml")

    def device(self, member):
        return (
            lax.div(member, self.low),
            lax.axis_index("dp"),
            lax.axis_index("mh"),
            lax.rem(member, self.low),
        )

    def peer(self, step):
        return lax.rem(self.me + step, self.size)

    def enter(self):
        barrier = pltpu.get_barrier_semaphore()
        for step in range(1, self.size):
            pl.semaphore_signal(
                barrier, inc=1, device_id=self.device(self.peer(step)), device_id_type=MESH
            )
        pl.semaphore_wait(barrier, self.size - 1)

    def copy(self, src, dst, send_sem, recv_sem, member):
        return pltpu.make_async_remote_copy(
            src_ref=src,
            dst_ref=dst,
            send_sem=send_sem,
            recv_sem=recv_sem,
            device_id=self.device(member),
            device_id_type=MESH,
        )

    def spread(self, buf, send_sem, recv_sem):
        me = self.me
        for step in range(1, self.size):
            self.copy(
                buf.at[me], buf.at[me], send_sem.at[step], recv_sem.at[me], self.peer(step)
            ).start()

    def spread_wait(self, buf, send_sem, recv_sem, member):
        self.copy(buf.at[member], buf.at[member], send_sem.at[1], recv_sem.at[member], member).wait_recv()

    def spread_sent(self, buf, send_sem, recv_sem):
        me = self.me
        for step in range(1, self.size):
            self.copy(
                buf.at[me], buf.at[me], send_sem.at[step], recv_sem.at[me], self.peer(step)
            ).wait_send()

    def reduce_copy(self, stage, landing, send_sem, recv_sem, member):
        return self.copy(
            stage.at[member], landing.at[self.me], send_sem.at[member], recv_sem.at[self.me], member
        )

    def reduce_wait(self, landing, send_sem, recv_sem, member):
        self.copy(
            landing.at[member], landing.at[member], send_sem.at[member], recv_sem.at[member], member
        ).wait_recv()

    def landed_sum(self, own, stage, landing, send_sem, recv_sem):
        total = own
        for step in range(1, self.size):
            member = self.peer(step)
            self.reduce_wait(landing, send_sem, recv_sem, member)
            total = total + landing[member].astype(F32)
        for step in range(1, self.size):
            self.reduce_copy(stage, landing, send_sem, recv_sem, self.peer(step)).wait_send()
        return total


def load_rows(src, dst, sems, chunk):
    copies = []
    for part in range(src.shape[0]):
        copies.append(
            pltpu.make_async_copy(src.at[part], dst.at[pl.ds(part * chunk, chunk)], sems.at[part])
        )
    return copies


def load_stack(src, dst, sems, chunk):
    copies = []
    for part in range(src.shape[0]):
        copies.append(
            pltpu.make_async_copy(
                src.at[part], dst.at[:, pl.ds(part * chunk, chunk), :], sems.at[part]
            )
        )
    return copies


def lane_mask(shape, head):
    lanes = lax.broadcasted_iota(jnp.int32, shape, len(shape) - 1)
    return (lanes >= head * HEAD_SIZE) & (lanes < (head + 1) * HEAD_SIZE)


def row_mask(shape, head):
    rows = lax.broadcasted_iota(jnp.int32, shape, 0)
    return (rows >= head * HEAD_SIZE) & (rows < (head + 1) * HEAD_SIZE)


def stack_heads(block):
    heads = block.shape[-1] // HEAD_SIZE
    zero = jnp.zeros_like(block)
    return jnp.concatenate(
        [jnp.where(lane_mask(block.shape, head), block, zero) for head in range(heads)], axis=0
    )


def identity(size):
    rows = lax.broadcasted_iota(jnp.int32, (size, size), 0)
    cols = lax.broadcasted_iota(jnp.int32, (size, size), 1)
    return jnp.where(rows == cols, 1.0, 0.0).astype(BF16)


def att_fwd_kernel(
    hidden_ref, mod_ref, bias_ref, bproj_ref, w_ref,
    middle_ref, normed_ref, proj_ref, att_ref, branch_ref,
    w_buf, stage, landing, w_sem, ag_send, ag_recv, rs_send, rs_recv,
):
    group = Group()
    me, size = group.me, group.size
    tokens, width = hidden_ref.shape
    heads = att_ref.shape[-1] // HEAD_SIZE
    loads = load_stack(w_ref, w_buf, w_sem, w_ref.shape[2])
    for copy in loads:
        copy.start()
    hidden = hidden_ref[...].astype(F32)
    normed, _ = norm_parts(hidden)
    normed_ref[me] = (normed * (1.0 + mod_ref[1:2]) + mod_ref[0:1]).astype(BF16)
    group.enter()
    group.spread(normed_ref, ag_send, ag_recv)
    for copy in loads:
        copy.wait()

    def project(step, carry):
        member = group.peer(step)

        @pl.when(step > 0)
        def _():
            group.spread_wait(normed_ref, ag_send, ag_recv, member)

        rows = normed_ref[member]
        for part in range(3):
            out = dot_nn(rows, w_buf[part]) + bias_ref[part]
            proj_ref[part, member] = out.astype(BF16)
        return carry

    lax.fori_loop(0, size, project, 0)
    seq = size * tokens
    keys = proj_ref[1].reshape(seq, -1)
    values = proj_ref[2].reshape(seq, -1)

    def attend(member):
        stacked = stack_heads(proj_ref[0, member])
        powered = jnp.exp(dot_nt(stacked, keys) * HEAD_SIZE**-0.5)
        probs = powered * (1.0 / jnp.sum(powered, axis=-1, keepdims=True))
        mixed = dot_nn(probs.astype(BF16), values)
        out = mixed[:tokens]
        for head in range(1, heads):
            part = mixed[head * tokens : (head + 1) * tokens]
            out = jnp.where(lane_mask(part.shape, head), part, out)
        low = out.astype(BF16)
        att_ref[member] = low
        return dot_nt(low, w_buf[3])

    def send(step, carry):
        member = group.peer(step)
        stage[member] = attend(member).astype(BF16)
        group.reduce_copy(stage, landing, rs_send, rs_recv, member).start()
        return carry

    lax.fori_loop(1, size, send, 0)
    own = attend(me)
    group.spread_sent(normed_ref, ag_send, ag_recv)
    branch = group.landed_sum(own, stage, landing, rs_send, rs_recv) + bproj_ref[...]
    branch_ref[...] = branch
    middle_ref[...] = hidden_ref[...].astype(F32) + mod_ref[2:3] * branch


def mlp_fwd_kernel(
    middle_ref, mod_ref, b1_ref, b2_ref, w1_ref, w2_ref,
    out_ref, normed_ref, pre_ref, gelu_ref, branch_ref,
    w1_buf, w2_buf, stage, landing, w1_sem, w2_sem, ag_send, ag_recv, rs_send, rs_recv,
):
    group = Group()
    me, size = group.me, group.size
    loads = load_rows(w1_ref, w1_buf, w1_sem, w1_ref.shape[1]) + load_rows(
        w2_ref, w2_buf, w2_sem, w2_ref.shape[1]
    )
    for copy in loads:
        copy.start()
    normed, _ = norm_parts(middle_ref[...])
    normed_ref[me] = (normed * (1.0 + mod_ref[4:5]) + mod_ref[3:4]).astype(BF16)
    group.enter()
    group.spread(normed_ref, ag_send, ag_recv)
    for copy in loads:
        copy.wait()

    def dense(member):
        pre = dot_nn(normed_ref[member], w1_buf[...]) + b1_ref[...]
        pre_ref[member] = pre
        bent = jnp.tanh(GELU_C * (pre + GELU_A * pre * pre * pre))
        low = (0.5 * pre * (1.0 + bent)).astype(BF16)
        gelu_ref[member] = low
        return dot_nt(low, w2_buf[...])

    own = dense(me)

    def send(step, carry):
        member = group.peer(step)
        group.spread_wait(normed_ref, ag_send, ag_recv, member)
        stage[member] = dense(member).astype(BF16)
        group.reduce_copy(stage, landing, rs_send, rs_recv, member).start()
        return carry

    stage[me] = own.astype(BF16)
    lax.fori_loop(1, size, send, 0)
    group.spread_sent(normed_ref, ag_send, ag_recv)
    own = stage[me].astype(F32)
    branch = group.landed_sum(own, stage, landing, rs_send, rs_recv) + b2_ref[...]
    branch_ref[...] = branch
    out_ref[...] = (middle_ref[...] + mod_ref[5:6] * branch).astype(BF16)


def weight_grad(lhs_ref, rhs, out_ref, tile):
    def body(index, carry):
        cols = pl.ds(pl.multiple_of(index * tile, tile), tile)
        out_ref[cols, :] = dot_tn(lhs_ref[:, cols], rhs).astype(BF16)
        return carry

    lax.fori_loop(0, lhs_ref.shape[-1] // tile, body, 0)


def mlp_bwd_kernel(
    grad_ref, middle_ref, mod_ref, branch_ref, normed_ref, pre_ref, gelu_ref, w1_ref, w2_ref,
    gmid_ref, dw1_ref, dw2_ref, db1_ref, db2_ref, dmod_ref,
    w1_buf, w2_buf, dbr, dpre, stage, landing, w1_sem, w2_sem, ag_send, ag_recv, rs_send, rs_recv,
):
    group = Group()
    me, size = group.me, group.size
    tokens, width = grad_ref.shape
    loads = load_rows(w1_ref, w1_buf, w1_sem, w1_ref.shape[1]) + load_rows(
        w2_ref, w2_buf, w2_sem, w2_ref.shape[1]
    )
    for copy in loads:
        copy.start()
    grad = grad_ref[...].astype(F32)
    dbr[me] = (grad * mod_ref[5:6]).astype(BF16)
    group.enter()
    group.spread(dbr, ag_send, ag_recv)
    dmod_ref[2:3] = col_sum(grad * branch_ref[...])
    for copy in loads:
        copy.wait()

    def back(member):
        dgelu = dot_nn(dbr[member], w2_buf[...])
        pre = pre_ref[member]
        bent = jnp.tanh(GELU_C * (pre + GELU_A * pre * pre * pre))
        slope = 0.5 * (1.0 + bent) + 0.5 * pre * (1.0 - bent * bent) * (
            GELU_C * (1.0 + 3.0 * GELU_A * pre * pre)
        )
        low = (dgelu * slope).astype(BF16)
        dpre[member] = low
        return dot_nt(low, w1_buf[...])

    stage[me] = back(me).astype(BF16)

    def send(step, carry):
        member = group.peer(step)
        group.spread_wait(dbr, ag_send, ag_recv, member)
        stage[member] = back(member).astype(BF16)
        group.reduce_copy(stage, landing, rs_send, rs_recv, member).start()
        return carry

    lax.fori_loop(1, size, send, 0)
    seq = size * tokens
    dpre_all = dpre[...].reshape(seq, -1)
    gelu_all = gelu_ref[...].reshape(seq, -1)
    db1_ref[...] = col_sum(dpre_all.astype(F32))
    db2_ref[...] = col_sum(dbr[...].reshape(seq, -1).astype(F32))
    weight_grad(normed_ref.reshape(seq, width), dpre_all, dw1_ref, 128)
    weight_grad(dbr.reshape(seq, width), gelu_all, dw2_ref, 128)
    group.spread_sent(dbr, ag_send, ag_recv)
    total = group.landed_sum(stage[me].astype(F32), stage, landing, rs_send, rs_recv)
    normed, rstd = norm_parts(middle_ref[...])
    dmod_ref[0:1] = col_sum(total)
    dmod_ref[1:2] = col_sum(total * normed)
    gmid_ref[...] = norm_back(total, normed, rstd, mod_ref[4:5]) + grad_ref[...].astype(F32)


def att_bwd_kernel(
    gmid_ref, hidden_ref, mod_ref, branch_ref, normed_ref, proj_ref, att_ref, w_ref,
    gin_ref, dw_ref, dbqkv_ref, dbproj_ref, dmod_ref,
    w_buf, dba, dproj, dkey, dval, stage, landing, w_sem, ag_send, ag_recv, rs_send, rs_recv,
):
    group = Group()
    me, size = group.me, group.size
    tokens, width = gmid_ref.shape
    seq = size * tokens
    part_width = att_ref.shape[-1]
    heads = part_width // HEAD_SIZE
    loads = load_stack(w_ref, w_buf, w_sem, w_ref.shape[2])
    for copy in loads:
        copy.start()
    gmid = gmid_ref[...]
    dba[me] = (gmid * mod_ref[2:3]).astype(BF16)
    group.enter()
    group.spread(dba, ag_send, ag_recv)
    dmod_ref[2:3] = col_sum(gmid * branch_ref[...])
    keys = proj_ref[1].reshape(seq, part_width)
    values = proj_ref[2].reshape(seq, part_width)
    keys_t = dot_nt(identity(part_width), keys).astype(BF16)
    dkey[...] = jnp.zeros_like(dkey)
    dval[...] = jnp.zeros_like(dval)
    for copy in loads:
        copy.wait()

    def back(step, carry):
        member = group.peer(step)

        @pl.when(step > 0)
        def _():
            group.spread_wait(dba, ag_send, ag_recv, member)

        datt = dot_nn(dba[member], w_buf[3]).astype(BF16)
        datt_st = stack_heads(datt)
        query_st = stack_heads(proj_ref[0, member])
        powered = jnp.exp(dot_nt(keys, query_st) * HEAD_SIZE**-0.5)
        probs = powered * (1.0 / jnp.sum(powered, axis=0, keepdims=True))
        dval[...] += dot_nn(probs.astype(BF16), datt_st)
        dprobs = dot_nt(values, datt_st)
        dscore = (probs * (dprobs - jnp.sum(probs * dprobs, axis=0, keepdims=True))).astype(BF16)
        dkey[...] += dot_nn(dscore, query_st)
        dq_t = dot_nn(keys_t, dscore)
        picked = dq_t[:, :tokens]
        for head in range(1, heads):
            part = dq_t[:, head * tokens : (head + 1) * tokens]
            picked = jnp.where(row_mask(part.shape, head), part, picked)
        low = (picked * HEAD_SIZE**-0.5).astype(BF16)
        dproj[0, member] = dot_nt(identity(tokens), low).astype(BF16)
        return carry

    lax.fori_loop(0, size, back, 0)
    for member in range(size):
        rows = slice(member * tokens, (member + 1) * tokens)
        dproj[1, member] = (dkey[rows] * HEAD_SIZE**-0.5).astype(BF16)
        dproj[2, member] = dval[rows].astype(BF16)

    def partial_rows(member):
        total = dot_nt(dproj[0, member], w_buf[0])
        total += dot_nt(dproj[1, member], w_buf[1])
        return total + dot_nt(dproj[2, member], w_buf[2])

    def send(step, carry):
        member = group.peer(step)
        stage[member] = partial_rows(member).astype(BF16)
        group.reduce_copy(stage, landing, rs_send, rs_recv, member).start()
        return carry

    lax.fori_loop(1, size, send, 0)
    stage[me] = partial_rows(me).astype(BF16)
    for part in range(3):
        grads = dproj[part].reshape(seq, part_width)
        dbqkv_ref[part] = col_sum(grads.astype(F32))
        weight_grad(normed_ref.reshape(seq, width), grads, dw_ref.at[part], 128)
    dbproj_ref[...] = col_sum(dba[...].reshape(seq, width).astype(F32))
    weight_grad(
        dba.reshape(seq, width), att_ref[...].reshape(seq, part_width), dw_ref.at[3], 128
    )
    group.spread_sent(dba, ag_send, ag_recv)
    total = group.landed_sum(stage[me].astype(F32), stage, landing, rs_send, rs_recv)
    hidden = hidden_ref[...].astype(F32)
    normed, rstd = norm_parts(hidden)
    dmod_ref[0:1] = col_sum(total)
    dmod_ref[1:2] = col_sum(total * normed)
    gin_ref[...] = norm_back(total, normed, rstd, mod_ref[1:2]) + gmid_ref[...]


VM = pl.BlockSpec(memory_space=pltpu.VMEM)
ANY = pl.BlockSpec(memory_space=pl.ANY)


def call(kernel, outs, in_specs, scratch, cid, name):
    return pl.pallas_call(
        kernel,
        out_shape=tuple(jax.ShapeDtypeStruct(shape, dtype) for shape, dtype in outs),
        in_specs=in_specs,
        out_specs=tuple(VM for _ in outs),
        scratch_shapes=scratch,
        compiler_params=pltpu.CompilerParams(
            collective_id=cid, has_side_effects=True, vmem_limit_bytes=VMEM_LIMIT
        ),
        name=name,
    )


def comm_scratch(size, tokens, width):
    dma = pltpu.SemaphoreType.DMA((size,))
    return [pltpu.VMEM((size, tokens, width), BF16)] * 2, [dma] * 4


def att_fwd(hidden, mod, bias, bproj, w):
    tokens, width = hidden.shape
    size = lax.axis_size("section") * lax.axis_size("ml")
    parts, part_width = w.shape[1], w.shape[3]
    bufs, sems = comm_scratch(size, tokens, width)
    return call(
        att_fwd_kernel,
        [
            ((tokens, width), F32),
            ((size, tokens, width), BF16),
            ((3, size, tokens, part_width), BF16),
            ((size, tokens, part_width), BF16),
            ((tokens, width), F32),
        ],
        [VM, VM, VM, VM, ANY],
        [pltpu.VMEM((parts, width, part_width), BF16)]
        + bufs
        + [pltpu.SemaphoreType.DMA((w.shape[0],))]
        + sems,
        1,
        "att_fwd",
    )(hidden, mod, bias, bproj, w)


def mlp_fwd(middle, mod, b1, b2, w1, w2):
    tokens, width = middle.shape
    size = lax.axis_size("section") * lax.axis_size("ml")
    units = w1.shape[2]
    bufs, sems = comm_scratch(size, tokens, width)
    return call(
        mlp_fwd_kernel,
        [
            ((tokens, width), BF16),
            ((size, tokens, width), BF16),
            ((size, tokens, units), F32),
            ((size, tokens, units), BF16),
            ((tokens, width), F32),
        ],
        [VM, VM, VM, VM, ANY, ANY],
        [pltpu.VMEM((width, units), BF16)] * 2
        + bufs
        + [pltpu.SemaphoreType.DMA((w1.shape[0],))] * 2
        + sems,
        2,
        "mlp_fwd",
    )(middle, mod, b1, b2, w1, w2)


def mlp_bwd(grad, middle, mod, branch, normed, pre, gelu, w1, w2):
    tokens, width = middle.shape
    size = lax.axis_size("section") * lax.axis_size("ml")
    units = w1.shape[2]
    bufs, sems = comm_scratch(size, tokens, width)
    return call(
        mlp_bwd_kernel,
        [
            ((tokens, width), F32),
            ((width, units), BF16),
            ((width, units), BF16),
            ((1, units), F32),
            ((1, width), F32),
            ((3, width), F32),
        ],
        [VM] * 7 + [ANY, ANY],
        [pltpu.VMEM((width, units), BF16)] * 2
        + [pltpu.VMEM((size, tokens, width), BF16), pltpu.VMEM((size, tokens, units), BF16)]
        + bufs
        + [pltpu.SemaphoreType.DMA((w1.shape[0],))] * 2
        + sems,
        3,
        "mlp_bwd",
    )(grad, middle, mod, branch, normed, pre, gelu, w1, w2)


def att_bwd(gmid, hidden, mod, branch, normed, proj, att, w):
    tokens, width = gmid.shape
    size = lax.axis_size("section") * lax.axis_size("ml")
    parts, part_width = w.shape[1], w.shape[3]
    bufs, sems = comm_scratch(size, tokens, width)
    seq = size * tokens
    return call(
        att_bwd_kernel,
        [
            ((tokens, width), F32),
            ((parts, width, part_width), BF16),
            ((3, 1, part_width), F32),
            ((1, width), F32),
            ((3, width), F32),
        ],
        [VM] * 7 + [ANY],
        [
            pltpu.VMEM((parts, width, part_width), BF16),
            pltpu.VMEM((size, tokens, width), BF16),
            pltpu.VMEM((3, size, tokens, part_width), BF16),
            pltpu.VMEM((seq, part_width), F32),
            pltpu.VMEM((seq, part_width), F32),
        ]
        + bufs
        + [pltpu.SemaphoreType.DMA((w.shape[0],))]
        + sems,
        4,
        "att_bwd",
    )(gmid, hidden, mod, branch, normed, proj, att, w)


def swap(block):
    return lax.ppermute(
        block, ("section", "mh"), [(s * 2 + h, h * 2 + s) for s in range(2) for h in range(2)]
    )


def per_device(
    latents_in, condition, cotangent,
    modulation_weight, modulation_bias, query_key_value_weight, query_value_bias,
    output_proj_weight, output_proj_bias, first_dense_weight, first_dense_bias,
    second_dense_weight, second_dense_bias,
):
    section, dp = lax.axis_index("section"), lax.axis_index("dp")
    high, low = lax.axis_index("mh"), lax.axis_index("ml")
    n_dp, n_low = lax.axis_size("dp"), lax.axis_size("ml")
    n_mp = 2 * n_low
    mp = high * n_low + low
    member = section * n_low + low
    width = latents_in.shape[-1]
    rows = modulation_weight.shape[1]
    cols = modulation_weight.shape[2]
    part_width = query_key_value_weight.shape[3]
    units = first_dense_weight.shape[2]
    local = section == high

    both = jnp.stack([latents_in[:, 0], cotangent[:, 0]], axis=1)
    sent = lax.dynamic_index_in_dim(both, 1 - high, 0, keepdims=False)
    kept = lax.dynamic_index_in_dim(both, high, 0, keepdims=False)
    got = lax.ppermute(sent, "mh", [(0, 1), (1, 0)])
    mine = jnp.where(local, kept, got)
    latent, cot = mine[0], mine[1]

    cond_all = lax.all_gather(condition[:, 0], "dp", axis=1).reshape(2 * n_dp, width)
    cond_all = cond_all.astype(F32)
    act_all = jax.nn.silu(cond_all).astype(BF16)
    act_rows = lax.dynamic_slice_in_dim(act_all, dp * rows, rows, 1)
    share = jnp.dot(act_rows, modulation_weight[0], preferred_element_type=F32)
    share = share.reshape(2, n_dp, cols)
    share = lax.psum_scatter(share, "dp", scatter_dimension=1, tiled=False)
    share = share + modulation_bias[0].astype(F32)
    full = lax.all_gather(share, ("section", "mh", "ml")).reshape(2, n_mp, 2, cols)
    full = lax.dynamic_index_in_dim(full, high, 2, keepdims=False)
    modul = full.reshape(2, 6, width)

    packed = jnp.concatenate(
        [query_value_bias[0].reshape(-1), first_dense_bias[0], output_proj_bias[0], second_dense_bias[0]]
    )
    packed = lax.all_gather(packed, ("section", "mh", "ml")).reshape(2, n_mp, -1)
    packed = lax.dynamic_index_in_dim(packed, member, 1, keepdims=False).astype(F32)
    bounds = [0, 2 * part_width, 2 * part_width + units, 2 * part_width + units + width]
    bqv = packed[:, : bounds[1]].reshape(2, 2, 1, part_width)
    bqkv = jnp.stack([bqv[:, 0], jnp.zeros_like(bqv[:, 0]), bqv[:, 1]], axis=1)
    b1 = packed[:, None, bounds[1] : bounds[2]]
    bproj = packed[:, None, bounds[2] : bounds[3]]
    b2 = packed[:, None, bounds[3] :]

    w_att = jnp.concatenate(
        [query_key_value_weight[0].transpose(1, 0, 2), output_proj_weight[0].T[None]], axis=0
    )
    w_one = first_dense_weight[0]
    w_two = second_dense_weight[0].T

    def collect(block):
        out = lax.all_gather(swap(block), OTHERS)
        return out.reshape((2, n_dp) + block.shape)

    w_att, w_one, w_two = collect(w_att), collect(w_one), collect(w_two)

    saved = []
    hidden = latent
    for layer in range(2):
        middle, normed, proj, att, branch = att_fwd(
            hidden, modul[layer], bqkv[layer], bproj[layer], w_att[layer]
        )
        out, normed2, pre, gelu, branch2 = mlp_fwd(
            middle, modul[layer], b1[layer], b2[layer], w_one[layer], w_two[layer]
        )
        saved.append((hidden, middle, normed, proj, att, branch, normed2, pre, gelu, branch2))
        hidden = out
    acts = [saved[1][0], hidden]

    grad = cot
    grad_in, d_att, d_one, d_two, d_bias, d_mod = {}, {}, {}, {}, {}, {}
    for layer in (1, 0):
        hidden, middle, normed, proj, att, branch, normed2, pre, gelu, branch2 = saved[layer]
        gmid, dw1, dw2, db1, db2, dmod2 = mlp_bwd(
            grad, middle, modul[layer], branch2, normed2, pre, gelu, w_one[layer], w_two[layer]
        )
        gin, dw, dbqkv, dbproj, dmod1 = att_bwd(
            gmid, hidden, modul[layer], branch, normed, proj, att, w_att[layer]
        )
        grad_in[layer] = gin
        d_att[layer], d_one[layer], d_two[layer] = dw, dw1, dw2
        d_bias[layer] = (
            jnp.concatenate([dbqkv[0, 0], dbqkv[2, 0], db1[0]]),
            jnp.concatenate([dbproj[0], db2[0]]),
        )
        d_mod[layer] = jnp.concatenate([dmod1.reshape(-1), dmod2.reshape(-1)])
        grad = gin.astype(BF16)

    def disperse(pair):
        block = jnp.stack([pair[0], pair[1]])
        return block

    def reduce_rows(first, second, axis):
        block = jnp.stack([first, second])
        axis += 1
        shape = block.shape
        block = block.reshape(shape[:axis] + (n_dp, rows) + shape[axis + 1 :])
        block = jnp.moveaxis(block, axis, 1).reshape((2 * n_dp,) + shape[1:axis] + (rows,) + shape[axis + 1 :])
        out = lax.psum_scatter(block, OTHERS, scatter_dimension=0, tiled=False)
        return swap(out).astype(F32)

    g_att = reduce_rows(d_att[0], d_att[1], 1)
    g_one = reduce_rows(d_one[0], d_one[1], 0)
    g_two = reduce_rows(d_two[0], d_two[1], 0)

    per_unit = lax.psum(jnp.stack([d_bias[0][0], d_bias[1][0]]), OTHERS)
    shared = lax.psum(jnp.stack([d_bias[0][1], d_bias[1][1]]), OTHERS)
    per_unit = lax.all_gather(per_unit, "section")
    per_unit = lax.dynamic_index_in_dim(per_unit, high, 0, keepdims=False)
    per_unit = lax.dynamic_index_in_dim(per_unit, section, 0, keepdims=False)
    shared = lax.dynamic_index_in_dim(shared, section, 0, keepdims=False)

    def dp_part(vec):
        size = vec.shape[-1] // n_dp
        return lax.dynamic_slice_in_dim(vec, dp * size, size, vec.ndim - 1)

    g_bqv = dp_part(per_unit[: 2 * part_width].reshape(2, part_width))
    g_b1 = dp_part(per_unit[2 * part_width :])
    g_bproj = dp_part(shared[:width])
    g_b2 = dp_part(shared[width:])

    dmod = lax.psum(jnp.stack([d_mod[0], d_mod[1]]), GROUP).astype(BF16)
    dmod = lax.all_gather(dmod, OTHERS)
    dmod = lax.dynamic_index_in_dim(dmod, section, 1, keepdims=False)
    dmod = lax.dynamic_slice_in_dim(dmod, mp * cols, cols, 1)
    g_bada = dp_part(jnp.sum(dmod, axis=0, dtype=F32))
    g_wada = jnp.dot(act_rows.T, dmod, preferred_element_type=F32)
    g_act = jnp.dot(dmod, modulation_weight[0].T, preferred_element_type=F32)
    g_act = lax.psum(g_act, ("section", "mh", "ml"))
    g_act = lax.all_gather(g_act, "dp", axis=1, tiled=True).reshape(2, n_dp, width)
    g_act = lax.dynamic_index_in_dim(g_act, dp, 1, keepdims=False)
    _, silu_back = jax.vjp(jax.nn.silu, condition[:, 0].astype(F32))
    g_cond = silu_back(g_act)[0][:, None]

    def deliver(first, second):
        block = jnp.stack([first, second])
        block = lax.all_to_all(block, "section", 0, 0, tiled=True)
        return lax.all_to_all(block, "mh", 0, 0, tiled=True)[None, :, None]

    acts_out = deliver(*acts)
    grad_input = deliver(grad_in[0], grad_in[1])
    return (
        acts_out,
        grad_input,
        g_cond,
        g_wada[None],
        g_bada[None],
        g_att[:3].transpose(1, 0, 2)[None],
        g_bqv[None],
        g_att[3].T[None],
        g_bproj[None],
        g_one[None],
        g_b1[None],
        g_two.T[None],
        g_b2[None],
    )


def solution(mesh):
    sizes = mesh.shape
    grid = mesh.devices.reshape(sizes["section"], sizes["dp"], 2, sizes["mp"] // 2)
    fine = Mesh(grid, ("section", "dp", "mh", "ml"))
    mp = ("mh", "ml")
    in_specs = (
        P(None, "dp", mp, None),
        P(None, "dp", None),
        P(None, "dp", mp, None),
        P("section", "dp", mp),
        P("section", mp),
        P("section", "dp", None, mp),
        P("section", None, mp),
        P("section", mp, "dp"),
        P("section", None),
        P("section", "dp", mp),
        P("section", mp),
        P("section", mp, "dp"),
        P("section", None),
    )
    mpdp = ("mh", "ml", "dp")
    out_specs = (
        P("section", None, "dp", mp, None),
        P("section", None, "dp", mp, None),
        P(None, "dp", None),
        P("section", "dp", mp),
        P("section", mpdp),
        P("section", "dp", None, mp),
        P("section", None, mpdp),
        P("section", mp, "dp"),
        P("section", "dp"),
        P("section", "dp", mp),
        P("section", mpdp),
        P("section", mp, "dp"),
        P("section", "dp"),
    )
    return jax.shard_map(
        per_device, mesh=fine, in_specs=in_specs, out_specs=out_specs, check_vma=False
    )
```

```python
import jax
import jax.numpy as jnp
from jax import lax
from jax.experimental import pallas as pl
from jax.experimental.pallas import tpu as pltpu
from jax.sharding import Mesh
from jax.sharding import PartitionSpec as P

HEAD_SIZE = 72
EPS = 1e-06
MESH = pl.DeviceIdType.MESH
BF16 = jnp.bfloat16
F32 = jnp.float32
GELU_C = 0.7978845608028654
GELU_A = 0.044715
NT = (((1,), (1,)), ((), ()))
TN = (((0,), (0,)), ((), ()))
VMEM_LIMIT = 60 * 1024 * 1024


def dot_nn(a, b):
    return jnp.dot(a, b, preferred_element_type=F32)


def dot_nt(a, b):
    return lax.dot_general(a, b, NT, preferred_element_type=F32)


def dot_tn(a, b):
    return lax.dot_general(a, b, TN, preferred_element_type=F32)


def norm_parts(values):
    center = values - jnp.mean(values, axis=-1, keepdims=True)
    spread = jnp.mean(center * center, axis=-1, keepdims=True)
    rstd = lax.rsqrt(spread + EPS)
    return center * rstd, rstd


def norm_back(grad, normed, rstd, scale):
    dn = grad * (1.0 + scale)
    first = jnp.mean(dn, axis=-1, keepdims=True)
    second = jnp.mean(dn * normed, axis=-1, keepdims=True)
    return (dn - first - normed * second) * rstd


def col_sum(values):
    return jnp.sum(values, axis=0, keepdims=True)


class Group:
    def __init__(self):
        self.low = lax.axis_size("ml")
        self.size = lax.axis_size("section") * self.low
        self.me = lax.axis_index("section") * self.low + lax.axis_index("ml")

    def device(self, member):
        return (
            lax.div(member, self.low),
            lax.axis_index("dp"),
            lax.axis_index("mh"),
            lax.rem(member, self.low),
        )

    def peer(self, step):
        return lax.rem(self.me + step, self.size)

    def copy(self, src, dst, send_sem, recv_sem, member):
        return pltpu.make_async_remote_copy(
            src_ref=src,
            dst_ref=dst,
            send_sem=send_sem,
            recv_sem=recv_sem,
            device_id=self.device(member),
            device_id_type=MESH,
        )

    def spread(self, buf, send_sem, recv_sem):
        me = self.me
        for step in range(1, self.size):
            self.copy(
                buf.at[me], buf.at[me], send_sem.at[step], recv_sem.at[me], self.peer(step)
            ).start()

    def spread_wait(self, buf, send_sem, recv_sem, member):
        self.copy(buf.at[member], buf.at[member], send_sem.at[1], recv_sem.at[member], member).wait_recv()

    def spread_sent(self, buf, send_sem, recv_sem):
        me = self.me
        for step in range(1, self.size):
            self.copy(
                buf.at[me], buf.at[me], send_sem.at[step], recv_sem.at[me], self.peer(step)
            ).wait_send()

    def reduce_copy(self, stage, landing, send_sem, recv_sem, member):
        return self.copy(
            stage.at[member], landing.at[self.me], send_sem.at[member], recv_sem.at[self.me], member
        )

    def reduce_wait(self, landing, send_sem, recv_sem, member):
        self.copy(
            landing.at[member], landing.at[member], send_sem.at[member], recv_sem.at[member], member
        ).wait_recv()

    def landed_sum(self, own, stage, landing, send_sem, recv_sem):
        total = own
        for step in range(1, self.size):
            member = self.peer(step)
            self.reduce_wait(landing, send_sem, recv_sem, member)
            total = total + landing[member].astype(F32)
        for step in range(1, self.size):
            self.reduce_copy(stage, landing, send_sem, recv_sem, self.peer(step)).wait_send()
        return total


def load(src, dst, sem):
    copy = pltpu.make_async_copy(src, dst, sem)
    copy.start()
    return [copy]


def lane_mask(shape, head):
    lanes = lax.broadcasted_iota(jnp.int32, shape, len(shape) - 1)
    return (lanes >= head * HEAD_SIZE) & (lanes < (head + 1) * HEAD_SIZE)


def row_mask(shape, head):
    rows = lax.broadcasted_iota(jnp.int32, shape, 0)
    return (rows >= head * HEAD_SIZE) & (rows < (head + 1) * HEAD_SIZE)


def stack_heads(block):
    heads = block.shape[-1] // HEAD_SIZE
    zero = jnp.zeros_like(block)
    return jnp.concatenate(
        [jnp.where(lane_mask(block.shape, head), block, zero) for head in range(heads)], axis=0
    )


def identity(size):
    rows = lax.broadcasted_iota(jnp.int32, (size, size), 0)
    cols = lax.broadcasted_iota(jnp.int32, (size, size), 1)
    return jnp.where(rows == cols, 1.0, 0.0).astype(BF16)


def att_fwd_kernel(
    bg,
    hidden_ref, mod_ref, bias_ref, bproj_ref, w_ref,
    middle_ref, normed_ref, proj_ref, att_ref, branch_ref,
    w_buf, wo_buf, stage, landing, w_sem, ag_send, ag_recv, rs_send, rs_recv,
):
    group = Group()
    me, size = group.me, group.size
    tokens, width = hidden_ref.shape
    part_width = att_ref.shape[-1]
    heads = part_width // HEAD_SIZE
    loads = load(w_ref, w_buf, w_sem.at[0])
    hidden = hidden_ref[...].astype(F32)
    normed, _ = norm_parts(hidden)
    normed_ref[me] = (normed * (1.0 + mod_ref[1:2]) + mod_ref[0:1]).astype(BF16)
    Place().greet()
    group.spread(normed_ref, ag_send, ag_recv)
    bg(0)
    for copy in loads:
        copy.wait()

    def project(step, carry):
        member = group.peer(step)

        @pl.when(step > 0)
        def _():
            group.spread_wait(normed_ref, ag_send, ag_recv, member)

        out = dot_nn(normed_ref[member], w_buf[:, : 3 * part_width]) + bias_ref[...]
        for part in range(3):
            cols = slice(part * part_width, (part + 1) * part_width)
            proj_ref[part, member] = out[:, cols].astype(BF16)
        return carry

    wo_buf[...] = w_buf[:, 3 * part_width :]
    lax.fori_loop(0, size, project, 0)
    bg(1)
    seq = size * tokens
    keys = proj_ref[1].reshape(seq, -1)
    values = proj_ref[2].reshape(seq, -1)

    def attend(member):
        stacked = stack_heads(proj_ref[0, member])
        powered = jnp.exp(dot_nt(stacked, keys) * HEAD_SIZE**-0.5)
        probs = powered * (1.0 / jnp.sum(powered, axis=-1, keepdims=True))
        mixed = dot_nn(probs.astype(BF16), values)
        out = mixed[:tokens]
        for head in range(1, heads):
            part = mixed[head * tokens : (head + 1) * tokens]
            out = jnp.where(lane_mask(part.shape, head), part, out)
        low = out.astype(BF16)
        att_ref[member] = low
        return dot_nt(low, wo_buf[...])

    def send(step, carry):
        member = group.peer(step)
        stage[member] = attend(member).astype(BF16)
        group.reduce_copy(stage, landing, rs_send, rs_recv, member).start()
        return carry

    lax.fori_loop(1, size, send, 0)
    bg(2)
    own = attend(me)
    group.spread_sent(normed_ref, ag_send, ag_recv)
    bg(3)
    branch = group.landed_sum(own, stage, landing, rs_send, rs_recv) + bproj_ref[...]
    branch_ref[...] = branch
    middle_ref[...] = hidden_ref[...].astype(F32) + mod_ref[2:3] * branch
    bg(4)


def mlp_fwd_kernel(
    bg,
    middle_ref, mod_ref, b1_ref, b2_ref, w1_ref, w2_ref,
    out_ref, normed_ref, pre_ref, gelu_ref, branch_ref,
    w1_buf, w2_buf, stage, landing, w_sem, ag_send, ag_recv, rs_send, rs_recv,
):
    group = Group()
    me, size = group.me, group.size
    loads = load(w1_ref, w1_buf, w_sem.at[0]) + load(w2_ref, w2_buf, w_sem.at[1])
    normed, _ = norm_parts(middle_ref[...])
    normed_ref[me] = (normed * (1.0 + mod_ref[4:5]) + mod_ref[3:4]).astype(BF16)
    Place().greet()
    group.spread(normed_ref, ag_send, ag_recv)
    bg(0)
    for copy in loads:
        copy.wait()

    def dense(member):
        pre = dot_nn(normed_ref[member], w1_buf[...]) + b1_ref[...]
        pre_ref[member] = pre
        bent = jnp.tanh(GELU_C * (pre + GELU_A * pre * pre * pre))
        low = (0.5 * pre * (1.0 + bent)).astype(BF16)
        gelu_ref[member] = low
        return dot_nt(low, w2_buf[...])

    own = dense(me)

    def send(step, carry):
        member = group.peer(step)
        group.spread_wait(normed_ref, ag_send, ag_recv, member)
        stage[member] = dense(member).astype(BF16)
        group.reduce_copy(stage, landing, rs_send, rs_recv, member).start()
        return carry

    stage[me] = own.astype(BF16)
    bg(1)
    lax.fori_loop(1, size, send, 0)
    bg(2)
    group.spread_sent(normed_ref, ag_send, ag_recv)
    bg(3)
    own = stage[me].astype(F32)
    branch = group.landed_sum(own, stage, landing, rs_send, rs_recv) + b2_ref[...]
    branch_ref[...] = branch
    out_ref[...] = (middle_ref[...] + mod_ref[5:6] * branch).astype(BF16)
    bg(4)


def weight_grad(lhs_ref, rhs, out_ref, tile):
    def body(index, carry):
        cols = pl.ds(pl.multiple_of(index * tile, tile), tile)
        out_ref[cols, :] = dot_tn(lhs_ref[:, cols], rhs).astype(BF16)
        return carry

    lax.fori_loop(0, lhs_ref.shape[-1] // tile, body, 0)


def mlp_bwd_kernel(
    bg,
    grad_ref, middle_ref, mod_ref, branch_ref, normed_ref, pre_ref, gelu_ref, w1_ref, w2_ref,
    gmid_ref, dw1_ref, dw2_ref, db1_ref, db2_ref, dmod_ref,
    w1_buf, w2_buf, dbr, dpre, stage, landing, w_sem, ag_send, ag_recv, rs_send, rs_recv,
):
    group = Group()
    me, size = group.me, group.size
    tokens, width = grad_ref.shape
    loads = load(w1_ref, w1_buf, w_sem.at[0]) + load(w2_ref, w2_buf, w_sem.at[1])
    grad = grad_ref[...].astype(F32)
    dbr[me] = (grad * mod_ref[5:6]).astype(BF16)
    Place().greet()
    group.spread(dbr, ag_send, ag_recv)
    bg(0)
    dmod_ref[2:3] = col_sum(grad * branch_ref[...])
    for copy in loads:
        copy.wait()

    def back(member):
        dgelu = dot_nn(dbr[member], w2_buf[...])
        pre = pre_ref[member]
        bent = jnp.tanh(GELU_C * (pre + GELU_A * pre * pre * pre))
        slope = 0.5 * (1.0 + bent) + 0.5 * pre * (1.0 - bent * bent) * (
            GELU_C * (1.0 + 3.0 * GELU_A * pre * pre)
        )
        low = (dgelu * slope).astype(BF16)
        dpre[member] = low
        return dot_nt(low, w1_buf[...])

    stage[me] = back(me).astype(BF16)
    bg(1)

    def send(step, carry):
        member = group.peer(step)
        group.spread_wait(dbr, ag_send, ag_recv, member)
        stage[member] = back(member).astype(BF16)
        group.reduce_copy(stage, landing, rs_send, rs_recv, member).start()
        return carry

    lax.fori_loop(1, size, send, 0)
    bg(2)
    seq = size * tokens
    dpre_all = dpre[...].reshape(seq, -1)
    gelu_all = gelu_ref[...].reshape(seq, -1)
    db1_ref[...] = col_sum(dpre_all.astype(F32))
    db2_ref[...] = col_sum(dbr[...].reshape(seq, -1).astype(F32))
    weight_grad(normed_ref.reshape(seq, width), dpre_all, dw1_ref, 128)
    weight_grad(dbr.reshape(seq, width), gelu_all, dw2_ref, 128)
    group.spread_sent(dbr, ag_send, ag_recv)
    bg(3)
    total = group.landed_sum(stage[me].astype(F32), stage, landing, rs_send, rs_recv)
    normed, rstd = norm_parts(middle_ref[...])
    dmod_ref[0:1] = col_sum(total)
    dmod_ref[1:2] = col_sum(total * normed)
    gmid_ref[...] = norm_back(total, normed, rstd, mod_ref[4:5]) + grad_ref[...].astype(F32)
    bg(4)


def att_bwd_kernel(
    bg,
    gmid_ref, hidden_ref, mod_ref, branch_ref, normed_ref, proj_ref, att_ref, w_ref,
    gin_ref, dw_ref, dbqkv_ref, dbproj_ref, dmod_ref,
    w_buf, wo_buf, dba, dproj, dkey, dval, stage, landing, w_sem, ag_send, ag_recv, rs_send, rs_recv,
):
    group = Group()
    me, size = group.me, group.size
    tokens, width = gmid_ref.shape
    seq = size * tokens
    part_width = att_ref.shape[-1]
    heads = part_width // HEAD_SIZE
    loads = load(w_ref, w_buf, w_sem.at[0])
    gmid = gmid_ref[...]
    dba[me] = (gmid * mod_ref[2:3]).astype(BF16)
    Place().greet()
    group.spread(dba, ag_send, ag_recv)
    bg(0)
    dmod_ref[2:3] = col_sum(gmid * branch_ref[...])
    keys = proj_ref[1].reshape(seq, part_width)
    values = proj_ref[2].reshape(seq, part_width)
    keys_t = dot_nt(identity(part_width), keys).astype(BF16)
    dkey[...] = jnp.zeros_like(dkey)
    dval[...] = jnp.zeros_like(dval)
    for copy in loads:
        copy.wait()
    wo_buf[...] = w_buf[:, 3 * part_width :]

    def back(step, carry):
        member = group.peer(step)

        if not isinstance(step, int):
            group.spread_wait(dba, ag_send, ag_recv, member)
        datt = dot_nn(dba[member], wo_buf[...]).astype(BF16)
        datt_st = stack_heads(datt)
        query_st = stack_heads(proj_ref[0, member])
        powered = jnp.exp(dot_nt(keys, query_st) * HEAD_SIZE**-0.5)
        probs = powered * (1.0 / jnp.sum(powered, axis=0, keepdims=True))
        dval[...] += dot_nn(probs.astype(BF16), datt_st)
        dprobs = dot_nt(values, datt_st)
        dscore = (probs * (dprobs - jnp.sum(probs * dprobs, axis=0, keepdims=True))).astype(BF16)
        dkey[...] += dot_nn(dscore, query_st)
        dq_t = dot_nn(keys_t, dscore)
        picked = dq_t[:, :tokens]
        for head in range(1, heads):
            part = dq_t[:, head * tokens : (head + 1) * tokens]
            picked = jnp.where(row_mask(part.shape, head), part, picked)
        low = (picked * HEAD_SIZE**-0.5).astype(BF16)
        dproj[member, :, :part_width] = dot_nt(identity(tokens), low).astype(BF16)
        return carry

    back(0, 0)
    bg(1)
    lax.fori_loop(1, size, back, 0)
    for member in range(size):
        rows = slice(member * tokens, (member + 1) * tokens)
        dproj[member, :, part_width : 2 * part_width] = (dkey[rows] * HEAD_SIZE**-0.5).astype(BF16)
        dproj[member, :, 2 * part_width :] = dval[rows].astype(BF16)

    def partial_rows(member):
        return dot_nt(dproj[member], w_buf[:, : 3 * part_width])

    def send(step, carry):
        member = group.peer(step)
        stage[member] = partial_rows(member).astype(BF16)
        group.reduce_copy(stage, landing, rs_send, rs_recv, member).start()
        return carry

    lax.fori_loop(1, size, send, 0)
    stage[me] = partial_rows(me).astype(BF16)
    bg(2)
    grads = dproj[...].reshape(seq, -1)
    dbqkv_ref[...] = col_sum(grads.astype(F32))
    dbproj_ref[...] = col_sum(dba[...].reshape(seq, width).astype(F32))
    mixed = att_ref[...].reshape(seq, part_width)
    normed_rows, dba_rows = normed_ref.reshape(seq, width), dba.reshape(seq, width)

    def weights(index, carry):
        cols = pl.ds(pl.multiple_of(index * 128, 128), 128)
        dw_ref[cols, : 3 * part_width] = dot_tn(normed_rows[:, cols], grads).astype(BF16)
        dw_ref[cols, 3 * part_width :] = dot_tn(dba_rows[:, cols], mixed).astype(BF16)
        return carry

    lax.fori_loop(0, width // 128, weights, 0)
    group.spread_sent(dba, ag_send, ag_recv)
    bg(3)
    total = group.landed_sum(stage[me].astype(F32), stage, landing, rs_send, rs_recv)
    hidden = hidden_ref[...].astype(F32)
    normed, rstd = norm_parts(hidden)
    dmod_ref[0:1] = col_sum(total)
    dmod_ref[1:2] = col_sum(total * normed)
    gin = norm_back(total, normed, rstd, mod_ref[1:2]) + gmid_ref[...]
    gin_ref[...] = gin.astype(BF16)
    bg(4)


class Place:
    def __init__(self):
        self.section, self.dp = lax.axis_index("section"), lax.axis_index("dp")
        self.high, self.low = lax.axis_index("mh"), lax.axis_index("ml")
        self.n_dp, self.n_low = lax.axis_size("dp"), lax.axis_size("ml")
        self.total = 4 * self.n_dp * self.n_low
        self.me = ((self.section * self.n_dp + self.dp) * 2 + self.high) * self.n_low + self.low

    def unflatten(self, number):
        low = lax.rem(number, self.n_low)
        rest = lax.div(number, self.n_low)
        high, rest = lax.rem(rest, 2), lax.div(rest, 2)
        return lax.div(rest, self.n_dp), lax.rem(rest, self.n_dp), high, low

    def greet(self):
        barrier = pltpu.get_barrier_semaphore()
        others = []
        for sec in range(2):
            for step in range(self.n_low):
                if sec or step:
                    section = lax.rem(self.section + sec, 2)
                    others.append((section, self.dp, self.high, lax.rem(self.low + step, self.n_low)))
        for sec in range(2):
            others.append(self.plane(sec, 1 - self.high))
        for step in range(1, self.n_dp // 2):
            others.append((self.section, self.same_core(step), self.high, self.low))
        others.append(self.core_mate())
        for device in others:
            pl.semaphore_signal(barrier, inc=1, device_id=device, device_id_type=MESH)
        pl.semaphore_wait(barrier, len(others))

    def role(self, layer, number):
        same = (self.section == layer) if number < 2 else (self.section != layer)
        return same & ((self.high == layer) if number % 2 == 0 else (self.high != layer))

    def role_device(self, layer, number):
        section = layer if number < 2 else 1 - layer
        return self.plane(section, layer if number % 2 == 0 else 1 - layer)

    def greet_all(self):
        barrier = pltpu.get_barrier_semaphore()

        def body(step, carry):
            pl.semaphore_signal(
                barrier,
                inc=1,
                device_id=self.unflatten(lax.rem(self.me + step, self.total)),
                device_id_type=MESH,
            )
            return carry

        lax.fori_loop(1, self.total, body, 0)
        pl.semaphore_wait(barrier, self.total - 1)

    def copy(self, src, dst, send_sem, recv_sem, device):
        return pltpu.make_async_remote_copy(
            src_ref=src,
            dst_ref=dst,
            send_sem=send_sem,
            recv_sem=recv_sem,
            device_id=device,
            device_id_type=MESH,
        )

    def core_mate(self):
        return (self.section, self.dp + 1 - 2 * lax.rem(self.dp, 2), self.high, self.low)

    def same_core(self, step):
        return lax.rem(self.dp + 2 * step, self.n_dp)

    def plane(self, section, high):
        return (section, self.dp, high, self.low)

    def exchange(self, pick, landing, send_sem, recv_sem):
        landing[self.me] = pick((self.section, self.dp, self.high, self.low))[...]

        def copy(number):
            device = self.unflatten(number)
            return self.copy(
                pick(device), landing.at[self.me], send_sem.at[number], recv_sem.at[self.me], device
            )

        def start(step, carry):
            copy(lax.rem(self.me + step, self.total)).start()
            return carry

        def finish(step, carry):
            number = lax.rem(self.me + step, self.total)
            device = self.unflatten(number)
            self.copy(
                landing.at[number], landing.at[number], send_sem.at[number], recv_sem.at[number], device
            ).wait_recv()
            copy(number).wait_send()
            return carry

        lax.fori_loop(1, self.total, start, 0)
        return lambda: lax.fori_loop(1, self.total, finish, 0)


VM = pl.BlockSpec(memory_space=pltpu.VMEM)
ANY = pl.BlockSpec(memory_space=pl.ANY)
DMA = pltpu.SemaphoreType.DMA


class Handle:
    def __init__(self, shape, dtype):
        self.shape, self.dtype = shape, dtype
        self.array = None
        self.ref = None


class Task:
    inputs = ()
    outs = ()
    scratch = ()
    handles = ()


class Collect(Task):
    def __init__(self, item, tensor, layer, handle):
        self.tensor, self.layer, self.handle = tensor, layer, handle
        self.inputs = ((item, VM),)
        self.handles = (handle,)
        self.chunk = item.shape[1]
        self.scratch = (DMA((2,)), DMA, DMA)

    def run(self, phase, refs):
        (item,), _, (send, recv, own) = refs
        place = Place()
        source = item.at[self.tensor]
        rows = self.handle.ref.at[pl.ds(pl.multiple_of(place.dp * self.chunk, 16), self.chunk)]

        def to(number, role):
            return place.copy(
                source, rows, send.at[number], recv, place.role_device(self.layer, role)
            )

        targets = {0: (1,), 1: (2, 3), 2: (), 3: ()}
        for role in range(4):

            @pl.when(place.role(self.layer, role))
            def _():
                if phase == "a":
                    for number, target in enumerate(targets[role]):
                        to(number, target).start()
                    if role == 0:
                        pltpu.make_async_copy(source, rows, own).start()
                if phase == "b":
                    if role == 0:
                        pltpu.make_async_copy(source, rows, own).wait()
                    else:
                        place.copy(
                            rows, rows, send.at[0], recv, place.role_device(self.layer, 0)
                        ).wait_recv()
                if phase == "c":
                    for number, target in enumerate(targets[role]):
                        to(number, target).wait_send()


class Widen(Task):
    def __init__(self, handle):
        self.handle = handle
        self.handles = (handle,)
        chips = lax.axis_size("dp") // 2
        self.scratch = (DMA((chips,)),) * 4

    def rows(self, index):
        chunk = self.handle.shape[0] // lax.axis_size("dp")
        return self.handle.ref.at[pl.ds(pl.multiple_of(index * chunk, 16), chunk)]

    def run(self, phase, refs):
        _, _, (x_send, x_recv, c_send, c_recv) = refs
        place = Place()
        chips = place.n_dp // 2

        def across(step):
            return place.copy(
                self.rows(place.dp), self.rows(place.dp), x_send.at[step], x_recv.at[step],
                (place.section, place.same_core(step), place.high, place.low),
            )

        def landed(step):
            held = self.rows(place.same_core(chips - step))
            return place.copy(
                held, held, x_send.at[step], x_recv.at[step],
                (place.section, place.same_core(step), place.high, place.low),
            )

        def to_mate(step):
            held = self.rows(place.same_core(step))
            return place.copy(held, held, c_send.at[step], c_recv.at[step], place.core_mate())

        def from_mate(step):
            held = self.rows(lax.rem(place.core_mate()[1] + 2 * step, place.n_dp))
            return place.copy(held, held, c_send.at[step], c_recv.at[step], place.core_mate())

        if phase == "a":
            for step in range(1, chips):
                across(step).start()
            to_mate(0).start()
        if phase == "b":
            for step in range(1, chips):
                landed(step).wait_recv()
                to_mate(chips - step).start()
        if phase == "c":
            for step in range(chips):
                from_mate(step).wait_recv()
                to_mate(step).wait_send()
                if step:
                    across(step).wait_send()


class Narrow(Task):
    def __init__(self, grad):
        n_dp = lax.axis_size("dp")
        chips = n_dp // 2
        self.chunk = grad.shape[0] // n_dp
        block = (chips, self.chunk, grad.shape[1])
        self.inputs = ((grad, ANY),)
        self.outs = (((self.chunk, grad.shape[1]), BF16, VM),)
        self.scratch = (pltpu.VMEM(block, BF16),) * 3 + (DMA((chips,)),) * 5

    def run(self, phase, refs):
        (grad,), (out,), scratch = refs
        own, near, far, own_sem, c_send, c_recv, x_send, x_recv = scratch
        place = Place()
        chips = place.n_dp // 2

        def rows(index):
            return grad.at[pl.ds(pl.multiple_of(index * self.chunk, 16), self.chunk)]

        def to_mate(step):
            other = lax.rem(place.core_mate()[1] + 2 * step, place.n_dp)
            return place.copy(
                rows(other), near.at[step], c_send.at[step], c_recv.at[step], place.core_mate()
            )

        def load_own(step):
            return pltpu.make_async_copy(
                rows(place.same_core(step)), own.at[step], own_sem.at[step]
            )

        def across(step):
            return place.copy(
                own.at[step], far.at[step], x_send.at[step], x_recv.at[step],
                (place.section, place.same_core(step), place.high, place.low),
            )

        order = list(range(1, chips)) + [0]
        if phase == "a":
            for step in order:
                to_mate(step).start()
                load_own(step).start()
        if phase == "b":
            for step in order:
                load_own(step).wait()
                to_mate(step).wait_recv()
                own[step] = (own[step].astype(F32) + near[step].astype(F32)).astype(BF16)
                if step:
                    across(step).start()
        if phase == "c":
            total = own[0].astype(F32)
            for step in range(1, chips):
                across(step).wait_recv()
                total = total + far[step].astype(F32)
            out[...] = total.astype(BF16)
            for step in range(chips):
                to_mate(step).wait_send()
                if step:
                    across(step).wait_send()


class Settle(Task):
    def __init__(self, part, layer, held=None):
        self.layer = layer
        self.held = held
        self.inputs = () if held else ((part, ANY),)
        self.outs = ((part.shape, F32, VM),)
        self.scratch = (
            pltpu.VMEM((2,) + part.shape, BF16), pltpu.VMEM(part.shape, BF16),
            DMA((2,)), DMA((3,)), DMA,
        )

    def run(self, phase, refs):
        ins, (out,), (land, temp, send, recv, own_sem) = refs
        part = self.held() if self.held else ins[0]
        place = Place()
        layer = self.layer

        def to(src, dst, s, r, role):
            return place.copy(src, dst, send.at[s], recv.at[r], place.role_device(layer, role))

        def direct(role):
            if role == 2:
                return to(part, temp, 0, 2, 0)
            return to(part, land.at[0], 0, 0, 0 if role == 1 else 1)

        def relay():
            return to(temp, land.at[1], 1, 1, 1)

        for role in range(4):

            @pl.when(place.role(layer, role))
            def _():
                if phase == "a":
                    if role:
                        direct(role).start()
                    else:
                        pltpu.make_async_copy(part, land.at[1], own_sem).start()
                if phase == "b":
                    if role == 0:
                        to(temp, temp, 0, 2, 0).wait_recv()
                        relay().start()
                    else:
                        direct(role).wait_send()
                if phase == "c":
                    if role == 0:
                        pltpu.make_async_copy(part, land.at[1], own_sem).wait()
                        relay().wait_send()
                    if role < 2:
                        to(land.at[0], land.at[0], 0, 0, role).wait_recv()
                    if role == 1:
                        to(land.at[1], land.at[1], 0, 1, 1).wait_recv()
                    if role < 2:
                        out[...] = land[0].astype(F32) + land[1].astype(F32)


class Deliver(Task):
    def __init__(self, rows, layer):
        self.layer = layer
        self.inputs = ((rows, VM),)
        self.outs = (((2,) + rows.shape, rows.dtype, VM),)
        self.scratch = (pltpu.VMEM(rows.shape, rows.dtype), DMA((2,)), DMA((3,)))

    def run(self, phase, refs):
        (rows,), (out,), (temp, send, recv) = refs
        place = Place()
        layer = self.layer

        def to(src, dst, s, r, role):
            return place.copy(src, dst, send.at[s], recv.at[r], place.role_device(layer, role))

        def direct(role):
            if role == 2:
                return to(rows, temp, 0, 2, 0)
            return to(rows, out.at[1 - layer], 0, 0, 0 if role == 1 else 1)

        def relay():
            return to(temp, out.at[layer], 1, 1, 1)

        for role in range(4):

            @pl.when(place.role(layer, role))
            def _():
                if phase == "a":
                    if role:
                        direct(role).start()
                    else:
                        out[layer] = rows[...]
                if phase == "b" and role == 0:
                    to(temp, temp, 0, 2, 0).wait_recv()
                    relay().start()
                if phase == "c":
                    if role == 0:
                        relay().wait_send()
                    else:
                        direct(role).wait_send()
                    if role < 2:
                        to(out.at[1 - layer], out.at[1 - layer], 0, 0, role).wait_recv()
                    if role == 1:
                        to(out.at[layer], out.at[layer], 0, 1, 1).wait_recv()


class Tokens(Task):
    def __init__(self, rows):
        self.inputs = ((rows, VM),)
        self.outs = ((rows.shape[1:], rows.dtype, VM),)
        self.scratch = (DMA, DMA)

    def run(self, phase, refs):
        (rows,), (out,), (send, recv) = refs
        place = Place()
        local = place.section == place.high
        copy = place.copy(
            rows.at[1 - place.high], out, send, recv, place.plane(place.section, 1 - place.high)
        )

        @pl.when(local)
        def _():
            if phase == "a":
                copy.start()
                out[...] = rows[place.high]
            if phase == "c":
                copy.wait_send()

        @pl.when(jnp.logical_not(local))
        def _():
            if phase == "c":
                copy.wait_recv()


def launch(kernel, operands, outs, scratch, schedule, cid, name):
    tasks = []
    for point in schedule:
        for task, _ in point:
            if task not in tasks:
                tasks.append(task)
    operands, outs, scratch = list(operands), list(outs), list(scratch)
    n_in, n_out, n_scratch = len(operands), len(outs), len(scratch)
    spans = []
    for task in tasks:
        spans.append((len(operands), len(outs), len(scratch)))
        operands += task.inputs
        outs += task.outs
        scratch += task.scratch
    handles = []
    for task in tasks:
        for handle in task.handles:
            if handle not in handles:
                handles.append(handle)
    aliases = {}
    first_handle = len(outs)
    for handle in handles:
        if handle.array is not None:
            aliases[len(operands)] = len(outs)
            operands.append((handle.array, ANY))
        outs.append((handle.shape, handle.dtype, ANY))

    def body(*refs):
        ins = refs[: len(operands)]
        results = refs[len(operands) : len(operands) + len(outs)]
        rest = refs[len(operands) + len(outs) :]
        for number, handle in enumerate(handles):
            handle.ref = results[first_handle + number]
        views = []
        for task, (a, b, c) in zip(tasks, spans):
            views.append(
                (
                    ins[a : a + len(task.inputs)],
                    results[b : b + len(task.outs)],
                    rest[c : c + len(task.scratch)],
                )
            )
            task.refs = views[-1]

        def bg(point):
            for task, phase in schedule[point]:
                task.run(phase, task.refs)

        kernel(bg, *ins[:n_in], *results[:n_out], *rest[:n_scratch])

    done = pl.pallas_call(
        body,
        out_shape=tuple(jax.ShapeDtypeStruct(shape, dtype) for shape, dtype, _ in outs),
        in_specs=[spec for _, spec in operands],
        out_specs=tuple(spec for _, _, spec in outs),
        scratch_shapes=scratch,
        input_output_aliases=aliases,
        compiler_params=pltpu.CompilerParams(
            collective_id=cid, has_side_effects=True, vmem_limit_bytes=VMEM_LIMIT
        ),
        name=name,
    )(*[array for array, _ in operands])
    for number, handle in enumerate(handles):
        handle.array = done[first_handle + number]
        handle.ref = None
    for task, (_, b, _) in zip(tasks, spans):
        task.results = done[b : b + len(task.outs)]
    return done[:n_out]


def group_size():
    return lax.axis_size("section") * lax.axis_size("ml")


def comm_scratch(tokens, width):
    size = group_size()
    return [pltpu.VMEM((size, tokens, width), BF16)] * 2, [DMA((size,))] * 4


def att_fwd(hidden, mod, bias, bproj, w, schedule, cid):
    tokens, width = hidden.shape
    size = group_size()
    part_width = width // size
    bufs, sems = comm_scratch(tokens, width)
    return launch(
        att_fwd_kernel,
        [(hidden, VM), (mod, VM), (bias, VM), (bproj, VM), (w.array, ANY)],
        [
            ((tokens, width), F32, VM),
            ((size, tokens, width), BF16, VM),
            ((3, size, tokens, part_width), BF16, VM),
            ((size, tokens, part_width), BF16, VM),
            ((tokens, width), F32, VM),
        ],
        [pltpu.VMEM(w.shape, BF16), pltpu.VMEM((width, part_width), BF16)]
        + bufs
        + [DMA((1,))]
        + sems,
        schedule,
        cid,
        "att_fwd",
    )


def mlp_fwd(middle, mod, b1, b2, w1, w2, schedule, cid):
    tokens, width = middle.shape
    size = group_size()
    units = w1.shape[1]
    bufs, sems = comm_scratch(tokens, width)
    return launch(
        mlp_fwd_kernel,
        [(middle, VM), (mod, VM), (b1, VM), (b2, VM), (w1.array, ANY), (w2.array, ANY)],
        [
            ((tokens, width), BF16, VM),
            ((size, tokens, width), BF16, VM),
            ((size, tokens, units), F32, VM),
            ((size, tokens, units), BF16, VM),
            ((tokens, width), F32, VM),
        ],
        [pltpu.VMEM(w1.shape, BF16)] * 2 + bufs + [DMA((2,))] + sems,
        schedule,
        cid,
        "mlp_fwd",
    )


def mlp_bwd(grad, middle, mod, branch, normed, pre, gelu, w1, w2, schedule, cid):
    tokens, width = middle.shape
    size = group_size()
    units = w1.shape[1]
    bufs, sems = comm_scratch(tokens, width)
    ins = (grad, middle, mod, branch, normed, pre, gelu)
    return launch(
        mlp_bwd_kernel,
        [(array, VM) for array in ins] + [(w1.array, ANY), (w2.array, ANY)],
        [
            ((tokens, width), F32, VM),
            (w1.shape, BF16, VM),
            (w2.shape, BF16, VM),
            ((1, units), F32, VM),
            ((1, width), F32, VM),
            ((3, width), F32, VM),
        ],
        [pltpu.VMEM(w1.shape, BF16)] * 2
        + [pltpu.VMEM((size, tokens, width), BF16), pltpu.VMEM((size, tokens, units), BF16)]
        + bufs
        + [DMA((2,))]
        + sems,
        schedule,
        cid,
        "mlp_bwd",
    )


def att_bwd(gmid, hidden, mod, branch, normed, proj, att, w, schedule, cid):
    tokens, width = gmid.shape
    size = group_size()
    part_width = width // size
    bufs, sems = comm_scratch(tokens, width)
    seq = size * tokens
    ins = (gmid, hidden, mod, branch, normed, proj, att)
    return launch(
        att_bwd_kernel,
        [(array, VM) for array in ins] + [(w.array, ANY)],
        [
            ((tokens, width), BF16, VM),
            (w.shape, BF16, VM),
            ((1, 3 * part_width), F32, VM),
            ((1, width), F32, VM),
            ((3, width), F32, VM),
        ],
        [
            pltpu.VMEM(w.shape, BF16),
            pltpu.VMEM((width, part_width), BF16),
            pltpu.VMEM((size, tokens, width), BF16),
            pltpu.VMEM((size, tokens, 3 * part_width), BF16),
            pltpu.VMEM((seq, part_width), F32),
            pltpu.VMEM((seq, part_width), F32),
        ]
        + bufs
        + [DMA((1,))]
        + sems,
        schedule,
        cid,
        "att_bwd",
    )


def prologue_kernel(
    bg,
    cond_ref, wada_ref, bada_ref, bias_ref,
    modul_ref, act_ref, bias_out,
    cond_land, share, land, cond_send, cond_recv, mod_send, mod_recv, b_send, b_recv,
):
    place = Place()
    section, dp, high = place.section, place.dp, place.high
    place.greet_all()

    def spread(step):
        other = lax.rem(dp + step, place.n_dp)
        return place.copy(
            cond_ref.at[other], cond_land.at[dp], cond_send.at[step], cond_recv.at[dp],
            (section, other, high, place.low),
        )

    def spread_wait(step):
        other = lax.rem(dp + step, place.n_dp)
        return place.copy(
            cond_land.at[other], cond_land.at[other], cond_send.at[step], cond_recv.at[other],
            (section, other, high, place.low),
        )

    cond_land[dp] = cond_ref[dp]
    for step in range(1, place.n_dp):
        spread(step).start()

    def bias_copy(target):
        return place.copy(
            bias_ref, bias_out.at[section], b_send.at[target], b_recv.at[section],
            place.plane(high, target),
        )

    here = section == high
    for target in range(2):

        @pl.when(jnp.logical_not(here & (high == target)))
        def _():
            bias_copy(target).start()

    @pl.when(here)
    def _():
        bias_out[section] = bias_ref[...]

    bg(0)
    for step in range(1, place.n_dp):
        spread_wait(step).wait_recv()
    parts = [cond_land[index] for index in range(place.n_dp)]
    act = jax.nn.silu(jnp.concatenate(parts, axis=0)).astype(BF16)
    act_ref[...] = act
    bias = jnp.where(dp == 0, bada_ref[...], 0.0)
    product = dot_nn(act, wada_ref[...])
    for row in range(2 * place.n_dp):
        share[row] = product[row : row + 1] + bias
    finish = place.exchange(
        lambda device: share.at[device[1] * 2 + device[2]], land, mod_send, mod_recv
    )
    bg(1)
    bg(2)
    finish()
    for layer in range(2):
        for part in range(2 * place.n_low):
            total = land[layer * place.n_dp * 2 * place.n_low + part]
            for index in range(1, place.n_dp):
                total = total + land[(layer * place.n_dp + index) * 2 * place.n_low + part]
            modul_ref[layer * 2 * place.n_low + part] = total
    bg(3)
    for step in range(1, place.n_dp):
        spread(step).wait_send()
    for target in range(2):

        @pl.when(jnp.logical_not(here & (high == target)))
        def _():
            bias_copy(target).wait_send()

        @pl.when(jnp.logical_not(here & (section == target)))
        def _():
            place.copy(
                bias_out.at[target], bias_out.at[target], b_send.at[0], b_recv.at[target],
                place.plane(section, 1 - high),
            ).wait_recv()

    bg(4)


def prologue(cond, wada, bada, bias, schedule, cid):
    n_dp, _, chunk = cond.shape
    n_mp = 2 * lax.axis_size("ml")
    total = 2 * n_dp * n_mp
    share = wada.shape[1]
    return launch(
        prologue_kernel,
        [(cond, VM), (wada, VM), (bada, VM), (bias, VM)],
        [
            ((2 * n_mp, 1, share), F32, VM),
            ((2 * n_dp, chunk), BF16, VM),
            ((2,) + bias.shape, F32, VM),
        ],
        [
            pltpu.VMEM((n_dp, 2, chunk), F32),
            pltpu.VMEM((2 * n_dp, 1, share), F32),
            pltpu.VMEM((total, 1, share), F32),
            DMA((n_dp,)),
            DMA((n_dp,)),
            DMA((total,)),
            DMA((total,)),
            DMA((2,)),
            DMA((2,)),
        ],
        schedule,
        cid,
        "prologue",
    )


def epilogue_kernel(
    bg,
    dmod_ref, act_ref, wada_ref, dbias_ref,
    gada_ref, gbada_ref, gact_ref, gbias_ref,
    mod_land, act_stage, act_land, bias_land, bias_stage, bias_final,
    mod_send, mod_recv, act_send, act_recv, d_send, d_recv, b_send, b_recv,
):
    place = Place()
    section, dp, high = place.section, place.dp, place.high
    place.greet_all()
    finish_mod = place.exchange(
        lambda device: dmod_ref.at[(device[0] * 2 + device[2]) * place.n_low + device[3]],
        mod_land, mod_send, mod_recv,
    )

    def spread(step):
        other = lax.rem(dp + step, place.n_dp)
        return place.copy(
            dbias_ref, bias_land.at[dp], d_send.at[step], d_recv.at[dp],
            (section, other, high, place.low),
        )

    for step in range(1, place.n_dp):
        spread(step).start()
    bg(0)
    finish_mod()
    parts = 2 * place.n_low
    latents = []
    for index in range(place.n_dp):
        for micro in range(2):
            total = 0.0
            for sec in range(2):
                for low in range(place.n_low):
                    number = ((sec * place.n_dp + index) * 2 + micro) * place.n_low + low
                    total = total + mod_land[number]
            latents.append(total)
    dmod = jnp.concatenate(latents, axis=0).astype(BF16)
    back = dot_nt(dmod, wada_ref[...])
    for index in range(place.n_dp):
        act_stage[index] = back[2 * index : 2 * index + 2]
    finish_act = place.exchange(lambda device: act_stage.at[device[1]], act_land, act_send, act_recv)
    bias_sum = dbias_ref[...]
    for step in range(1, place.n_dp):
        other = lax.rem(dp + step, place.n_dp)
        place.copy(
            bias_land.at[other], bias_land.at[other], d_send.at[step], d_recv.at[other],
            (section, other, high, place.low),
        ).wait_recv()
        bias_sum = bias_sum + bias_land[other]
    bias_stage[...] = bias_sum

    def settle(layer):
        return place.copy(
            bias_stage.at[layer], bias_final.at[high], b_send.at[layer], b_recv.at[high],
            place.plane(layer, section),
        )

    for layer in range(2):
        here = (section == layer) & (high == section)

        @pl.when(here)
        def _():
            bias_final[high] = bias_stage[layer]

        @pl.when(jnp.logical_not(here))
        def _():
            settle(layer).start()

    bg(1)
    gbada_ref[...] = col_sum(dmod.astype(F32))
    gada_ref[...] = dot_tn(act_ref[...], dmod)
    bg(2)
    finish_act()
    for index in range(place.n_dp):
        total = 0.0
        for sec in range(2):
            for part in range(parts):
                total = total + act_land[(sec * place.n_dp + index) * parts + part]
        gact_ref[index] = total
    bg(3)
    for half in range(2):
        here = (section == high) & (high == half)

        @pl.when(jnp.logical_not(here))
        def _():
            place.copy(
                bias_final.at[half], bias_final.at[half], b_send.at[0], b_recv.at[half],
                place.plane(high, half),
            ).wait_recv()

    gbias_ref[...] = bias_final[0] + bias_final[1]
    for layer in range(2):

        @pl.when(jnp.logical_not((section == layer) & (high == section)))
        def _():
            settle(layer).wait_send()

    for step in range(1, place.n_dp):
        spread(step).wait_send()
    bg(4)


def epilogue(dmod, act, wada, dbias, schedule, cid):
    n_dp, n_mp = lax.axis_size("dp"), 2 * lax.axis_size("ml")
    total = 2 * n_dp * n_mp
    chunk, share = wada.shape
    row = dbias.shape[1:]
    return launch(
        epilogue_kernel,
        [(dmod, VM), (act, VM), (wada, VM), (dbias, VM)],
        [
            ((chunk, share), F32, VM),
            ((1, share), F32, VM),
            ((n_dp, 2, chunk), F32, VM),
            (row, F32, VM),
        ],
        [
            pltpu.VMEM((total, 1, share), F32),
            pltpu.VMEM((n_dp, 2, chunk), F32),
            pltpu.VMEM((total, 2, chunk), F32),
            pltpu.VMEM((n_dp,) + dbias.shape, F32),
            pltpu.VMEM(dbias.shape, F32),
            pltpu.VMEM((2,) + row, F32),
            DMA((total,)),
            DMA((total,)),
            DMA((total,)),
            DMA((total,)),
            DMA((n_dp,)),
            DMA((n_dp,)),
            DMA((2,)),
            DMA((2,)),
        ],
        schedule,
        cid,
        "epilogue",
    )


def per_device(
    latents_in, condition, cotangent,
    modulation_weight, modulation_bias, query_key_value_weight, query_value_bias,
    output_proj_weight, output_proj_bias, first_dense_weight, first_dense_bias,
    second_dense_weight, second_dense_bias,
):
    section, dp = lax.axis_index("section"), lax.axis_index("dp")
    n_dp, n_low = lax.axis_size("dp"), lax.axis_size("ml")
    n_mp = 2 * n_low
    width = latents_in.shape[-1]
    rows = modulation_weight.shape[1]
    cols = modulation_weight.shape[2]
    part_width = query_key_value_weight.shape[3]
    units = first_dense_weight.shape[2]

    item = jnp.stack(
        [
            jnp.concatenate(
                [query_key_value_weight[0].reshape(rows, -1), output_proj_weight[0].T], axis=1
            ),
            first_dense_weight[0],
            second_dense_weight[0].T,
        ]
    )
    cond = condition[:, 0].astype(F32)
    packed = jnp.concatenate(
        [
            query_value_bias[0, 0], query_value_bias[0, 1], first_dense_bias[0],
            output_proj_bias[0], second_dense_bias[0],
        ]
    ).astype(F32)[None]
    w = [[Handle((width, units), BF16) for _ in range(3)] for _ in range(2)]
    collect = [[Collect(item, t, l, w[l][t]) for t in range(3)] for l in range(2)]
    widen = [[Widen(w[l][t]) for t in range(3)] for l in range(2)]
    tokens_in = Tokens(latents_in[:, 0])
    tokens_cot = Tokens(cotangent[:, 0])

    def plan(*points):
        out = []
        for point in points:
            out.append([(task, phase) for task, phases in point for phase in phases])
        return out

    c, x = collect, widen
    modul, act_rows, biases = prologue(
        cond.reshape(2, n_dp, rows).transpose(1, 0, 2),
        modulation_weight[0],
        modulation_bias.astype(F32),
        packed,
        plan(
            [(tokens_in, "a"), (c[0][0], "a"), (c[1][0], "a")],
            [(c[0][0], "c"), (c[1][0], "c"), (c[0][1], "a"), (c[1][1], "a")]
            + [(c[0][0], "b"), (x[0][0], "a"), (c[1][0], "b")],
            [(c[0][1], "c"), (c[1][1], "c"), (c[0][2], "a"), (c[1][2], "a")]
            + [(x[0][0], "b"), (c[0][1], "b"), (x[0][1], "a"), (c[1][1], "b")],
            [],
            [(c[0][2], "c"), (c[1][2], "c"), (c[0][2], "b"), (c[1][2], "b"), (x[0][1], "b")]
            + [(tokens_in, "c"), (x[0][0], "c"), (x[0][1], "c")],
        ),
        1,
    )
    modul = modul.reshape(2, 6, width)
    bounds = [0, part_width, 2 * part_width, 2 * part_width + units, 2 * part_width + units + width]
    bqkv = jnp.concatenate(
        [
            biases[..., : bounds[1]], jnp.zeros((2, 1, part_width), F32),
            biases[..., bounds[1] : bounds[2]],
        ],
        axis=-1,
    )
    b1 = biases[..., bounds[2] : bounds[3]]
    bproj = biases[..., bounds[3] : bounds[4]]
    b2 = biases[..., bounds[4] :]

    hidden = [tokens_in.results[0]]
    att_plan = [
        plan(
            [(x[0][2], "a")],
            [],
            [],
            [(x[0][2], "b")],
            [(x[0][2], "c")],
        ),
        plan(
            [(x[1][1], "a"), (x[1][2], "a"), (tokens_cot, "a")],
            [],
            [],
            [(x[1][1], "b"), (x[1][2], "b")],
            [(x[1][1], "c"), (x[1][2], "c"), (tokens_cot, "c")],
        ),
    ]
    saved = []
    for layer in range(2):
        middle, normed, proj, att, branch = att_fwd(
            hidden[layer], modul[layer], bqkv[layer], bproj[layer], w[layer][0], att_plan[layer],
            2 + 2 * layer,
        )
        if layer == 0:
            mlp_plan = plan(
                [(x[1][0], "a")],
                [],
                [],
                [(x[1][0], "b")],
                [(x[1][0], "c")],
            )
        else:
            acts_first = Deliver(hidden[1], 0)
            mlp_plan = plan([], [], [], [], [])
        out, normed2, pre, gelu, branch2 = mlp_fwd(
            middle, modul[layer], b1[layer], b2[layer], w[layer][1], w[layer][2], mlp_plan,
            3 + 2 * layer,
        )
        saved.append((middle, normed, proj, att, branch, normed2, pre, gelu, branch2))
        hidden.append(out)

    grad = tokens_cot.results[0]
    narrow = [[None] * 3 for _ in range(2)]
    settle = [[None] * 3 for _ in range(2)]
    d_bias, d_mod, gins = {}, {}, {}
    acts_second = Deliver(hidden[2], 1)
    for layer in (1, 0):
        middle, normed, proj, att, branch, normed2, pre, gelu, branch2 = saved[layer]
        if layer == 1:
            mlp_plan = plan(
                [(acts_first, "a"), (acts_second, "a")],
                [],
                [(acts_first, "b"), (acts_second, "b")],
                [],
                [(acts_first, "c"), (acts_second, "c")],
            )
        else:
            third = narrow[1][0]
            mlp_plan = plan([(third, "a")], [(third, "b")], [], [], [(third, "c")])
        gmid, dw1, dw2, db1, db2, dmod2 = mlp_bwd(
            grad, middle, modul[layer], branch2, normed2, pre, gelu, w[layer][1], w[layer][2],
            mlp_plan, 6 + 2 * (1 - layer),
        )
        narrow[layer][1], narrow[layer][2] = Narrow(dw1), Narrow(dw2)
        one, two = narrow[layer][1], narrow[layer][2]
        if layer == 0:
            settle[1][0] = Settle(narrow[1][0].results[0], 1)
            gin_second = Deliver(gins[1], 1)
        att_plan = plan(
            [(two, "a"), (one, "a")], [(two, "b"), (one, "b")], [], [], [(two, "c"), (one, "c")]
        )
        gin, dw, dbqkv, dbproj, dmod1 = att_bwd(
            gmid, hidden[layer], modul[layer], branch, normed, proj, att, w[layer][0],
            att_plan, 7 + 2 * (1 - layer),
        )
        for tensor in (1, 2):
            settle[layer][tensor] = Settle(narrow[layer][tensor].results[0], layer)
        narrow[layer][0] = Narrow(dw)
        gins[layer] = grad = gin
        d_bias[layer] = jnp.concatenate(
            [dbqkv[:, :part_width], dbqkv[:, 2 * part_width :], db1, dbproj, db2], axis=1
        )
        d_mod[layer] = jnp.concatenate([dmod1.reshape(-1), dmod2.reshape(-1)])

    last = narrow[0][0]
    final = Settle(jax.ShapeDtypeStruct((rows, units), BF16), 0, held=lambda: last.refs[1][0])
    settle[0][0] = final
    gin_first = Deliver(gins[0], 0)
    dmod = jnp.stack([d_mod[0], d_mod[1]]).reshape(2 * n_mp, 1, cols)
    g_wada, g_bada, g_act, g_bias = epilogue(
        dmod,
        act_rows,
        modulation_weight[0],
        jnp.stack([d_bias[0], d_bias[1]]),
        plan(
            [(last, "a"), (gin_first, "a"), (gin_second, "a")]
            + [(settle[0][2], "a"), (settle[1][2], "a")],
            [(last, "b"), (gin_first, "b"), (gin_second, "b"), (settle[0][2], "b"), (settle[1][2], "b")]
            + [(settle[0][1], "a"), (settle[1][1], "a")],
            [(last, "c"), (settle[0][1], "b"), (settle[1][1], "b"), (final, "a"), (settle[1][0], "a")],
            [(final, "b"), (settle[1][0], "b"), (settle[0][2], "c"), (settle[1][2], "c")],
            [(settle[0][1], "c"), (settle[1][1], "c"), (gin_first, "c"), (gin_second, "c")]
            + [(settle[1][0], "c"), (final, "c")],
        ),
        10,
    )
    g_act = g_act.transpose(1, 0, 2).reshape(2, width)
    low_section = section == 0

    def own_block(first, second):
        return jnp.where(low_section, first.results[0], second.results[0])

    g_att, g_one, g_two = [own_block(settle[0][t], settle[1][t]) for t in range(3)]
    g_qkv = g_att[:, : 3 * part_width].reshape(rows, 3, part_width)
    g_proj = g_att[:, 3 * part_width :].T

    def dp_part(vec):
        size = vec.shape[-1] // n_dp
        return lax.dynamic_slice_in_dim(vec, dp * size, size, vec.ndim - 1)

    g_bias = g_bias[0]
    g_bqv = dp_part(g_bias[: bounds[2]].reshape(2, part_width))
    g_b1 = dp_part(g_bias[bounds[2] : bounds[3]])
    g_bproj = dp_part(g_bias[bounds[3] : bounds[4]])
    g_b2 = dp_part(g_bias[bounds[4] :])
    g_bada = dp_part(g_bada[0])
    _, silu_back = jax.vjp(jax.nn.silu, cond)
    g_cond = silu_back(g_act)[0][:, None]
    acts_out = own_block(acts_first, acts_second)[None, :, None]
    grad_input = own_block(gin_first, gin_second).astype(F32)[None, :, None]
    return (
        acts_out,
        grad_input,
        g_cond,
        g_wada[None],
        g_bada[None],
        g_qkv[None],
        g_bqv[None],
        g_proj[None],
        g_bproj[None],
        g_one[None],
        g_b1[None],
        g_two.T[None],
        g_b2[None],
    )


def solution(mesh):
    sizes = mesh.shape
    grid = mesh.devices.reshape(sizes["section"], sizes["dp"], 2, sizes["mp"] // 2)
    fine = Mesh(grid, ("section", "dp", "mh", "ml"))
    mp = ("mh", "ml")
    in_specs = (
        P(None, "dp", mp, None),
        P(None, "dp", None),
        P(None, "dp", mp, None),
        P("section", "dp", mp),
        P("section", mp),
        P("section", "dp", None, mp),
        P("section", None, mp),
        P("section", mp, "dp"),
        P("section", None),
        P("section", "dp", mp),
        P("section", mp),
        P("section", mp, "dp"),
        P("section", None),
    )
    mpdp = ("mh", "ml", "dp")
    out_specs = (
        P("section", None, "dp", mp, None),
        P("section", None, "dp", mp, None),
        P(None, "dp", None),
        P("section", "dp", mp),
        P("section", mpdp),
        P("section", "dp", None, mp),
        P("section", None, mpdp),
        P("section", mp, "dp"),
        P("section", "dp"),
        P("section", "dp", mp),
        P("section", mpdp),
        P("section", mp, "dp"),
        P("section", "dp"),
    )
    return jax.shard_map(
        per_device, mesh=fine, in_specs=in_specs, out_specs=out_specs, check_vma=False
    )
```

```python
import jax
import jax.numpy as jnp
from jax import lax
from jax.experimental import pallas as pl
from jax.experimental.pallas import tpu as pltpu
from jax.sharding import Mesh
from jax.sharding import PartitionSpec as P

HEAD_SIZE = 72
EPS = 1e-06
MESH = pl.DeviceIdType.MESH
BF16 = jnp.bfloat16
F32 = jnp.float32
GELU_C = 0.7978845608028654
GELU_A = 0.044715
NT = (((1,), (1,)), ((), ()))
TN = (((0,), (0,)), ((), ()))
VMEM_LIMIT = 50 * 1024 * 1024


def dot_nn(a, b):
    return jnp.dot(a, b, preferred_element_type=F32)


def dot_nt(a, b):
    return lax.dot_general(a, b, NT, preferred_element_type=F32)


def dot_tn(a, b):
    return lax.dot_general(a, b, TN, preferred_element_type=F32)


def norm_parts(values):
    center = values - jnp.mean(values, axis=-1, keepdims=True)
    spread = jnp.mean(center * center, axis=-1, keepdims=True)
    rstd = lax.rsqrt(spread + EPS)
    return center * rstd, rstd


def norm_back(grad, normed, rstd, scale):
    dn = grad * (1.0 + scale)
    first = jnp.mean(dn, axis=-1, keepdims=True)
    second = jnp.mean(dn * normed, axis=-1, keepdims=True)
    return (dn - first - normed * second) * rstd


def col_sum(values):
    return jnp.sum(values, axis=0, keepdims=True)


class Group:
    def __init__(self, tokens):
        self.low = lax.axis_size("ml")
        self.size = lax.axis_size("section") * self.low
        self.me = lax.axis_index("section") * self.low + lax.axis_index("ml")
        self.square = self.size == 4
        self.half = (slice(0, tokens // 2), slice(tokens // 2, tokens))

    def device(self, member):
        return (
            lax.div(member, self.low),
            lax.axis_index("dp"),
            lax.axis_index("mh"),
            lax.rem(member, self.low),
        )

    def member(self, step):
        if not self.square:
            return lax.rem(self.me + step, self.size)
        section = lax.rem(lax.axis_index("section") + lax.rem(step, 2), 2)
        low = lax.rem(lax.axis_index("ml") + lax.div(step, 2), 2)
        return section * 2 + low

    def copy(self, src, dst, send_sem, recv_sem, member):
        return pltpu.make_async_remote_copy(
            src_ref=src,
            dst_ref=dst,
            send_sem=send_sem,
            recv_sem=recv_sem,
            device_id=self.device(member),
            device_id_type=MESH,
        )

    def first_copies(self, buf, send_sem, recv_sem):
        steps = (1, 2) if self.square else range(1, self.size)
        mine = buf.at[self.me]
        return [
            self.copy(mine, mine, send_sem.at[step], recv_sem.at[self.me], self.member(step))
            for step in steps
        ]

    def relay_copy(self, buf, send_sem, recv_sem, step):
        rows = buf.at[self.member(step), self.half[step - 1]]
        return self.copy(
            rows, rows, send_sem.at[2 + step], recv_sem.at[3 + step], self.member(3 - step)
        )

    def spread(self, buf, send_sem, recv_sem):
        for copy in self.first_copies(buf, send_sem, recv_sem):
            copy.start()

    def arrive(self, buf, send_sem, recv_sem, step):
        def landed(rows, sem):
            self.copy(rows, rows, send_sem.at[1], sem, self.member(1)).wait_recv()

        if not self.square:
            landed(buf.at[self.member(step)], recv_sem.at[self.member(step)])
            return

        @pl.when(step == 1)
        def _():
            for near in (1, 2):
                landed(buf.at[self.member(near)], recv_sem.at[self.member(near)])
                self.relay_copy(buf, send_sem, recv_sem, near).start()

        @pl.when(step == 3)
        def _():
            for near in (1, 2):
                landed(buf.at[self.member(3), self.half[near - 1]], recv_sem.at[3 + near])

    def spread_sent(self, buf, send_sem, recv_sem):
        for copy in self.first_copies(buf, send_sem, recv_sem):
            copy.wait_send()
        if self.square:
            for step in (1, 2):
                self.relay_copy(buf, send_sem, recv_sem, step).wait_send()

    def straight(self, stage, landing, send_sem, recv_sem, step):
        rows = self.half[step - 1]
        return self.copy(
            stage.at[self.member(step), rows], landing.at[step - 1, rows],
            send_sem.at[step - 1], recv_sem.at[step - 1], self.member(step),
        )

    def corner(self, stage, landing, send_sem, recv_sem, step):
        rows = self.half[step - 1]
        return self.copy(
            stage.at[self.member(3), rows], landing.at[2, rows],
            send_sem.at[1 + step], recv_sem.at[1 + step], self.member(step),
        )

    def summed(self, landing, send_sem, recv_sem, step):
        rows = self.half[2 - step]
        return self.copy(
            landing.at[3, rows], landing.at[step - 1, rows],
            send_sem.at[3 + step], recv_sem.at[3 + step], self.member(step),
        )

    def reduce_copy(self, stage, landing, send_sem, recv_sem, member):
        return self.copy(
            stage.at[member], landing.at[self.me], send_sem.at[member], recv_sem.at[self.me], member
        )

    def give(self, stage, landing, send_sem, recv_sem, step):
        args = (stage, landing, send_sem, recv_sem)
        if not self.square:
            self.reduce_copy(*args, self.member(step)).start()
            return
        for near in (1, 2):

            @pl.when(step == near)
            def _():
                self.straight(*args, near).start()

        @pl.when(step == 3)
        def _():
            for near in (1, 2):
                self.corner(*args, near).start()

    def combine(self, stage, landing, send_sem, recv_sem):
        if not self.square:
            return
        for step in (1, 2):
            rows = self.half[2 - step]
            self.copy(
                landing.at[2, rows], landing.at[2, rows], send_sem.at[0], recv_sem.at[4 - step],
                self.member(1),
            ).wait_recv()
            total = stage[self.member(step), rows].astype(F32) + landing[2, rows].astype(F32)
            landing[3, rows] = total.astype(BF16)
            self.summed(landing, send_sem, recv_sem, step).start()

    def landed_sum(self, own, stage, landing, send_sem, recv_sem):
        args = (stage, landing, send_sem, recv_sem)
        total = own

        def landed(rows, sem):
            self.copy(rows, rows, send_sem.at[0], sem, self.member(1)).wait_recv()

        if self.square:
            for step in (1, 2):
                first, second = self.half[step - 1], self.half[2 - step]
                landed(landing.at[step - 1, first], recv_sem.at[step - 1])
                landed(landing.at[step - 1, second], recv_sem.at[3 + step])
                total = total + landing[step - 1].astype(F32)
            for step in (1, 2):
                self.straight(*args, step).wait_send()
                self.corner(*args, step).wait_send()
                self.summed(landing, send_sem, recv_sem, step).wait_send()
            return total
        for step in range(1, self.size):
            member = self.member(step)
            landed(landing.at[member], recv_sem.at[member])
            total = total + landing[member].astype(F32)
        for step in range(1, self.size):
            self.reduce_copy(*args, self.member(step)).wait_send()
        return total


def load(src, dst, sem):
    copy = pltpu.make_async_copy(src, dst, sem)
    copy.start()
    return [copy]


def lane_mask(shape, head):
    lanes = lax.broadcasted_iota(jnp.int32, shape, len(shape) - 1)
    return (lanes >= head * HEAD_SIZE) & (lanes < (head + 1) * HEAD_SIZE)


def row_mask(shape, head):
    rows = lax.broadcasted_iota(jnp.int32, shape, 0)
    return (rows >= head * HEAD_SIZE) & (rows < (head + 1) * HEAD_SIZE)


def stack_heads(block):
    heads = block.shape[-1] // HEAD_SIZE
    zero = jnp.zeros_like(block)
    return jnp.concatenate(
        [jnp.where(lane_mask(block.shape, head), block, zero) for head in range(heads)], axis=0
    )


def identity(size):
    rows = lax.broadcasted_iota(jnp.int32, (size, size), 0)
    cols = lax.broadcasted_iota(jnp.int32, (size, size), 1)
    return jnp.where(rows == cols, 1.0, 0.0).astype(BF16)


def att_fwd_kernel(
    bg,
    hidden_ref, mod_ref, bias_ref, bproj_ref, w_ref,
    middle_ref, normed_ref, proj_ref, att_ref, branch_ref,
    w_buf, wo_buf, stage, landing, w_sem, ag_send, ag_recv, rs_send, rs_recv,
):
    tokens, width = hidden_ref.shape
    group = Group(tokens)
    me, size = group.me, group.size
    part_width = att_ref.shape[-1]
    heads = part_width // HEAD_SIZE
    loads = load(w_ref, w_buf, w_sem.at[0])
    hidden = hidden_ref[...].astype(F32)
    normed, _ = norm_parts(hidden)
    normed_ref[me] = (normed * (1.0 + mod_ref[1:2]) + mod_ref[0:1]).astype(BF16)
    Place().greet()
    group.spread(normed_ref, ag_send, ag_recv)
    bg(0)
    for copy in loads:
        copy.wait()

    def project(step, carry):
        member = group.member(step)
        if not isinstance(step, int):
            group.arrive(normed_ref, ag_send, ag_recv, step)
        out = dot_nn(normed_ref[member], w_buf[:, : 3 * part_width]) + bias_ref[...]
        for part in range(3):
            cols = slice(part * part_width, (part + 1) * part_width)
            proj_ref[part, member] = out[:, cols].astype(BF16)
        return carry

    wo_buf[...] = w_buf[:, 3 * part_width :]
    project(0, 0)
    lax.fori_loop(1, size, project, 0)
    bg(1)
    seq = size * tokens
    keys = proj_ref[1].reshape(seq, -1)
    values = proj_ref[2].reshape(seq, -1)

    def attend(member):
        stacked = stack_heads(proj_ref[0, member])
        powered = jnp.exp(dot_nt(stacked, keys) * HEAD_SIZE**-0.5)
        probs = powered * (1.0 / jnp.sum(powered, axis=-1, keepdims=True))
        mixed = dot_nn(probs.astype(BF16), values)
        out = mixed[:tokens]
        for head in range(1, heads):
            part = mixed[head * tokens : (head + 1) * tokens]
            out = jnp.where(lane_mask(part.shape, head), part, out)
        low = out.astype(BF16)
        att_ref[member] = low
        return dot_nt(low, wo_buf[...])

    def send(step, carry):
        member = group.member(size - step)
        stage[member] = attend(member).astype(BF16)
        group.give(stage, landing, rs_send, rs_recv, size - step)
        return carry

    lax.fori_loop(1, size, send, 0)
    group.combine(stage, landing, rs_send, rs_recv)
    bg(2)
    own = attend(me)
    group.spread_sent(normed_ref, ag_send, ag_recv)
    bg(3)
    branch = group.landed_sum(own, stage, landing, rs_send, rs_recv) + bproj_ref[...]
    branch_ref[...] = branch
    middle_ref[...] = hidden_ref[...].astype(F32) + mod_ref[2:3] * branch
    bg(4)


def mlp_fwd_kernel(
    bg,
    middle_ref, mod_ref, b1_ref, b2_ref, w1_ref, w2_ref,
    out_ref, normed_ref, pre_ref, gelu_ref, branch_ref,
    w1_buf, w2_buf, stage, landing, w_sem, ag_send, ag_recv, rs_send, rs_recv,
):
    group = Group(middle_ref.shape[0])
    me, size = group.me, group.size
    loads = load(w1_ref, w1_buf, w_sem.at[0]) + load(w2_ref, w2_buf, w_sem.at[1])
    normed, _ = norm_parts(middle_ref[...])
    normed_ref[me] = (normed * (1.0 + mod_ref[4:5]) + mod_ref[3:4]).astype(BF16)
    Place().greet()
    group.spread(normed_ref, ag_send, ag_recv)
    bg(0)
    for copy in loads:
        copy.wait()

    def dense(member):
        pre = dot_nn(normed_ref[member], w1_buf[...]) + b1_ref[...]
        pre_ref[member] = pre
        bent = jnp.tanh(GELU_C * (pre + GELU_A * pre * pre * pre))
        low = (0.5 * pre * (1.0 + bent)).astype(BF16)
        gelu_ref[member] = low
        return dot_nt(low, w2_buf[...])

    own = dense(me)

    def send(step, carry):
        member = group.member(step)
        group.arrive(normed_ref, ag_send, ag_recv, step)
        stage[member] = dense(member).astype(BF16)
        group.give(stage, landing, rs_send, rs_recv, step)
        return carry

    stage[me] = own.astype(BF16)
    bg(1)
    lax.fori_loop(1, size, send, 0)
    group.combine(stage, landing, rs_send, rs_recv)
    bg(2)
    group.spread_sent(normed_ref, ag_send, ag_recv)
    bg(3)
    own = stage[me].astype(F32)
    branch = group.landed_sum(own, stage, landing, rs_send, rs_recv) + b2_ref[...]
    branch_ref[...] = branch
    out_ref[...] = (middle_ref[...] + mod_ref[5:6] * branch).astype(BF16)
    bg(4)


def weight_grad(lhs_ref, rhs, out_ref, tile):
    def body(index, carry):
        cols = pl.ds(pl.multiple_of(index * tile, tile), tile)
        out_ref[cols, :] = dot_tn(lhs_ref[:, cols], rhs).astype(BF16)
        return carry

    lax.fori_loop(0, lhs_ref.shape[-1] // tile, body, 0)


def mlp_bwd_kernel(
    bg,
    grad_ref, middle_ref, mod_ref, branch_ref, normed_ref, pre_ref, gelu_ref, w1_ref, w2_ref,
    gmid_ref, dw1_ref, dw2_ref, db1_ref, db2_ref, dmod_ref,
    w1_buf, w2_buf, dbr, dpre, stage, landing, w_sem, ag_send, ag_recv, rs_send, rs_recv,
):
    tokens, width = grad_ref.shape
    group = Group(tokens)
    me, size = group.me, group.size
    loads = load(w1_ref, w1_buf, w_sem.at[0]) + load(w2_ref, w2_buf, w_sem.at[1])
    grad = grad_ref[...].astype(F32)
    dbr[me] = (grad * mod_ref[5:6]).astype(BF16)
    Place().greet()
    group.spread(dbr, ag_send, ag_recv)
    bg(0)
    dmod_ref[2:3] = col_sum(grad * branch_ref[...])
    for copy in loads:
        copy.wait()

    def back(member):
        dgelu = dot_nn(dbr[member], w2_buf[...])
        pre = pre_ref[member]
        bent = jnp.tanh(GELU_C * (pre + GELU_A * pre * pre * pre))
        slope = 0.5 * (1.0 + bent) + 0.5 * pre * (1.0 - bent * bent) * (
            GELU_C * (1.0 + 3.0 * GELU_A * pre * pre)
        )
        low = (dgelu * slope).astype(BF16)
        dpre[member] = low
        return dot_nt(low, w1_buf[...])

    stage[me] = back(me).astype(BF16)
    bg(1)

    def send(step, carry):
        member = group.member(step)
        group.arrive(dbr, ag_send, ag_recv, step)
        stage[member] = back(member).astype(BF16)
        group.give(stage, landing, rs_send, rs_recv, step)
        return carry

    lax.fori_loop(1, size, send, 0)
    group.combine(stage, landing, rs_send, rs_recv)
    bg(2)
    seq = size * tokens
    dpre_all = dpre[...].reshape(seq, -1)
    gelu_all = gelu_ref[...].reshape(seq, -1)
    db1_ref[...] = col_sum(dpre_all.astype(F32))
    db2_ref[...] = col_sum(dbr[...].reshape(seq, -1).astype(F32))
    weight_grad(normed_ref.reshape(seq, width), dpre_all, dw1_ref, 128)
    weight_grad(dbr.reshape(seq, width), gelu_all, dw2_ref, 128)
    group.spread_sent(dbr, ag_send, ag_recv)
    bg(3)
    total = group.landed_sum(stage[me].astype(F32), stage, landing, rs_send, rs_recv)
    normed, rstd = norm_parts(middle_ref[...])
    dmod_ref[0:1] = col_sum(total)
    dmod_ref[1:2] = col_sum(total * normed)
    gmid_ref[...] = norm_back(total, normed, rstd, mod_ref[4:5]) + grad_ref[...].astype(F32)
    bg(4)


def att_bwd_kernel(
    bg,
    gmid_ref, hidden_ref, mod_ref, branch_ref, normed_ref, proj_ref, att_ref, w_ref,
    gin_ref, dw_ref, dbqkv_ref, dbproj_ref, dmod_ref,
    w_buf, wo_buf, dba, dproj, dkey, dval, stage, landing, w_sem, ag_send, ag_recv, rs_send, rs_recv,
):
    tokens, width = gmid_ref.shape
    group = Group(tokens)
    me, size = group.me, group.size
    seq = size * tokens
    part_width = att_ref.shape[-1]
    heads = part_width // HEAD_SIZE
    loads = load(w_ref, w_buf, w_sem.at[0])
    gmid = gmid_ref[...]
    dba[me] = (gmid * mod_ref[2:3]).astype(BF16)
    Place().greet()
    group.spread(dba, ag_send, ag_recv)
    bg(0)
    dmod_ref[2:3] = col_sum(gmid * branch_ref[...])
    keys = proj_ref[1].reshape(seq, part_width)
    values = proj_ref[2].reshape(seq, part_width)
    keys_t = dot_nt(identity(part_width), keys).astype(BF16)
    dkey[...] = jnp.zeros_like(dkey)
    dval[...] = jnp.zeros_like(dval)
    for copy in loads:
        copy.wait()
    wo_buf[...] = w_buf[:, 3 * part_width :]

    def back(step, carry):
        member = group.member(step)
        if not isinstance(step, int):
            group.arrive(dba, ag_send, ag_recv, step)
        datt = dot_nn(dba[member], wo_buf[...]).astype(BF16)
        datt_st = stack_heads(datt)
        query_st = stack_heads(proj_ref[0, member])
        powered = jnp.exp(dot_nt(keys, query_st) * HEAD_SIZE**-0.5)
        probs = powered * (1.0 / jnp.sum(powered, axis=0, keepdims=True))
        dval[...] += dot_nn(probs.astype(BF16), datt_st)
        dprobs = dot_nt(values, datt_st)
        dscore = (probs * (dprobs - jnp.sum(probs * dprobs, axis=0, keepdims=True))).astype(BF16)
        dkey[...] += dot_nn(dscore, query_st)
        dq_t = dot_nn(keys_t, dscore)
        picked = dq_t[:, :tokens]
        for head in range(1, heads):
            part = dq_t[:, head * tokens : (head + 1) * tokens]
            picked = jnp.where(row_mask(part.shape, head), part, picked)
        low = (picked * HEAD_SIZE**-0.5).astype(BF16)
        dproj[member, :, :part_width] = dot_nt(identity(tokens), low).astype(BF16)
        return carry

    back(0, 0)
    bg(1)
    lax.fori_loop(1, size, back, 0)
    for member in range(size):
        rows = slice(member * tokens, (member + 1) * tokens)
        dproj[member, :, part_width : 2 * part_width] = (dkey[rows] * HEAD_SIZE**-0.5).astype(BF16)
        dproj[member, :, 2 * part_width :] = dval[rows].astype(BF16)

    def partial_rows(member):
        return dot_nt(dproj[member], w_buf[:, : 3 * part_width])

    def send(step, carry):
        member = group.member(size - step)
        stage[member] = partial_rows(member).astype(BF16)
        group.give(stage, landing, rs_send, rs_recv, size - step)
        return carry

    lax.fori_loop(1, size, send, 0)
    stage[me] = partial_rows(me).astype(BF16)
    group.combine(stage, landing, rs_send, rs_recv)
    bg(2)
    grads = dproj[...].reshape(seq, -1)
    dbqkv_ref[...] = col_sum(grads.astype(F32))
    dbproj_ref[...] = col_sum(dba[...].reshape(seq, width).astype(F32))
    mixed = att_ref[...].reshape(seq, part_width)
    normed_rows, dba_rows = normed_ref.reshape(seq, width), dba.reshape(seq, width)

    def weights(index, carry):
        cols = pl.ds(pl.multiple_of(index * 128, 128), 128)
        dw_ref[cols, : 3 * part_width] = dot_tn(normed_rows[:, cols], grads).astype(BF16)
        dw_ref[cols, 3 * part_width :] = dot_tn(dba_rows[:, cols], mixed).astype(BF16)
        return carry

    lax.fori_loop(0, width // 128, weights, 0)
    group.spread_sent(dba, ag_send, ag_recv)
    bg(3)
    total = group.landed_sum(stage[me].astype(F32), stage, landing, rs_send, rs_recv)
    hidden = hidden_ref[...].astype(F32)
    normed, rstd = norm_parts(hidden)
    dmod_ref[0:1] = col_sum(total)
    dmod_ref[1:2] = col_sum(total * normed)
    gin = norm_back(total, normed, rstd, mod_ref[1:2]) + gmid_ref[...]
    gin_ref[...] = gin.astype(BF16)
    bg(4)


class Place:
    def __init__(self):
        self.section, self.dp = lax.axis_index("section"), lax.axis_index("dp")
        self.high, self.low = lax.axis_index("mh"), lax.axis_index("ml")
        self.n_dp, self.n_low = lax.axis_size("dp"), lax.axis_size("ml")
        self.total = 4 * self.n_dp * self.n_low
        self.me = ((self.section * self.n_dp + self.dp) * 2 + self.high) * self.n_low + self.low

    def unflatten(self, number):
        low = lax.rem(number, self.n_low)
        rest = lax.div(number, self.n_low)
        high, rest = lax.rem(rest, 2), lax.div(rest, 2)
        return lax.div(rest, self.n_dp), lax.rem(rest, self.n_dp), high, low

    def greet(self):
        barrier = pltpu.get_barrier_semaphore()
        others = []
        for sec in range(2):
            for step in range(self.n_low):
                if sec or step:
                    section = lax.rem(self.section + sec, 2)
                    others.append((section, self.dp, self.high, lax.rem(self.low + step, self.n_low)))
        for sec in range(2):
            others.append(self.plane(sec, 1 - self.high))
        for step in range(1, self.n_dp // 2):
            others.append((self.section, self.same_core(step), self.high, self.low))
        others.append(self.core_mate())
        for device in others:
            pl.semaphore_signal(barrier, inc=1, device_id=device, device_id_type=MESH)
        pl.semaphore_wait(barrier, len(others))

    def role(self, layer, number):
        same = (self.section == layer) if number < 2 else (self.section != layer)
        return same & ((self.high == layer) if number % 2 == 0 else (self.high != layer))

    def role_device(self, layer, number):
        section = layer if number < 2 else 1 - layer
        return self.plane(section, layer if number % 2 == 0 else 1 - layer)

    def greet_all(self):
        barrier = pltpu.get_barrier_semaphore()

        def body(step, carry):
            pl.semaphore_signal(
                barrier,
                inc=1,
                device_id=self.unflatten(lax.rem(self.me + step, self.total)),
                device_id_type=MESH,
            )
            return carry

        lax.fori_loop(1, self.total, body, 0)
        pl.semaphore_wait(barrier, self.total - 1)

    def copy(self, src, dst, send_sem, recv_sem, device):
        return pltpu.make_async_remote_copy(
            src_ref=src,
            dst_ref=dst,
            send_sem=send_sem,
            recv_sem=recv_sem,
            device_id=device,
            device_id_type=MESH,
        )

    def core_mate(self):
        return (self.section, self.dp + 1 - 2 * lax.rem(self.dp, 2), self.high, self.low)

    def same_core(self, step):
        return lax.rem(self.dp + 2 * step, self.n_dp)

    def plane(self, section, high):
        return (section, self.dp, high, self.low)

    def exchange(self, pick, landing, send_sem, recv_sem):
        landing[self.me] = pick((self.section, self.dp, self.high, self.low))[...]

        def copy(number):
            device = self.unflatten(number)
            return self.copy(
                pick(device), landing.at[self.me], send_sem.at[number], recv_sem.at[self.me], device
            )

        def start(step, carry):
            copy(lax.rem(self.me + step, self.total)).start()
            return carry

        def finish(step, carry):
            number = lax.rem(self.me + step, self.total)
            device = self.unflatten(number)
            self.copy(
                landing.at[number], landing.at[number], send_sem.at[number], recv_sem.at[number], device
            ).wait_recv()
            copy(number).wait_send()
            return carry

        lax.fori_loop(1, self.total, start, 0)
        return lambda: lax.fori_loop(1, self.total, finish, 0)


VM = pl.BlockSpec(memory_space=pltpu.VMEM)
ANY = pl.BlockSpec(memory_space=pltpu.HBM)
DMA = pltpu.SemaphoreType.DMA


class Handle:
    def __init__(self, shape, dtype):
        self.shape, self.dtype = shape, dtype
        self.array = None
        self.ref = None


class Task:
    inputs = ()
    outs = ()
    scratch = ()
    handles = ()


class Collect(Task):
    def __init__(self, item, tensor, layer, handle):
        self.tensor, self.layer, self.handle = tensor, layer, handle
        self.inputs = ((item, VM),)
        self.handles = (handle,)
        self.chunk = item.shape[1]
        self.scratch = (DMA((2,)), DMA, DMA)

    def run(self, phase, refs):
        (item,), _, (send, recv, own) = refs
        place = Place()
        source = item.at[self.tensor]
        rows = self.handle.ref.at[pl.ds(pl.multiple_of(place.dp * self.chunk, 16), self.chunk)]

        def to(number, role):
            return place.copy(
                source, rows, send.at[number], recv, place.role_device(self.layer, role)
            )

        targets = {0: (1,), 1: (2, 3), 2: (), 3: ()}
        for role in range(4):

            @pl.when(place.role(self.layer, role))
            def _():
                if phase == "a":
                    for number, target in enumerate(targets[role]):
                        to(number, target).start()
                    if role == 0:
                        pltpu.make_async_copy(source, rows, own).start()
                if phase == "b":
                    if role == 0:
                        pltpu.make_async_copy(source, rows, own).wait()
                    else:
                        place.copy(
                            rows, rows, send.at[0], recv, place.role_device(self.layer, 0)
                        ).wait_recv()
                if phase == "c":
                    for number, target in enumerate(targets[role]):
                        to(number, target).wait_send()


class Widen(Task):
    def __init__(self, handle):
        self.handle = handle
        self.handles = (handle,)
        chips = lax.axis_size("dp") // 2
        self.scratch = (DMA((chips,)),) * 4

    def rows(self, index):
        chunk = self.handle.shape[0] // lax.axis_size("dp")
        return self.handle.ref.at[pl.ds(pl.multiple_of(index * chunk, 16), chunk)]

    def run(self, phase, refs):
        _, _, (x_send, x_recv, c_send, c_recv) = refs
        place = Place()
        chips = place.n_dp // 2

        def across(step):
            return place.copy(
                self.rows(place.dp), self.rows(place.dp), x_send.at[step], x_recv.at[step],
                (place.section, place.same_core(step), place.high, place.low),
            )

        def landed(step):
            held = self.rows(place.same_core(chips - step))
            return place.copy(
                held, held, x_send.at[step], x_recv.at[step],
                (place.section, place.same_core(step), place.high, place.low),
            )

        def to_mate(step):
            held = self.rows(place.same_core(step))
            return place.copy(held, held, c_send.at[step], c_recv.at[step], place.core_mate())

        def from_mate(step):
            held = self.rows(lax.rem(place.core_mate()[1] + 2 * step, place.n_dp))
            return place.copy(held, held, c_send.at[step], c_recv.at[step], place.core_mate())

        if phase == "a":
            for step in range(1, chips):
                across(step).start()
            to_mate(0).start()
        if phase == "b":
            for step in range(1, chips):
                landed(step).wait_recv()
                to_mate(chips - step).start()
        if phase == "c":
            for step in range(chips):
                from_mate(step).wait_recv()
                to_mate(step).wait_send()
                if step:
                    across(step).wait_send()


class Narrow(Task):
    def __init__(self, grad):
        n_dp = lax.axis_size("dp")
        chips = n_dp // 2
        self.chunk = grad.shape[0] // n_dp
        block = (chips, self.chunk, grad.shape[1])
        self.inputs = ((grad, ANY),)
        self.outs = (((self.chunk, grad.shape[1]), BF16, VM),)
        self.scratch = (pltpu.VMEM(block, BF16),) * 3 + (DMA((chips,)),) * 5

    def run(self, phase, refs):
        (grad,), (out,), scratch = refs
        own, near, far, own_sem, c_send, c_recv, x_send, x_recv = scratch
        place = Place()
        chips = place.n_dp // 2

        def rows(index):
            return grad.at[pl.ds(pl.multiple_of(index * self.chunk, 16), self.chunk)]

        def to_mate(step):
            other = lax.rem(place.core_mate()[1] + 2 * step, place.n_dp)
            return place.copy(
                rows(other), near.at[step], c_send.at[step], c_recv.at[step], place.core_mate()
            )

        def load_own(step):
            return pltpu.make_async_copy(
                rows(place.same_core(step)), own.at[step], own_sem.at[step]
            )

        def across(step):
            return place.copy(
                own.at[step], far.at[step], x_send.at[step], x_recv.at[step],
                (place.section, place.same_core(step), place.high, place.low),
            )

        order = list(range(1, chips)) + [0]
        if phase == "a":
            for step in order:
                to_mate(step).start()
                load_own(step).start()
        if phase == "b":
            for step in order:
                load_own(step).wait()
                to_mate(step).wait_recv()
                own[step] = (own[step].astype(F32) + near[step].astype(F32)).astype(BF16)
                if step:
                    across(step).start()
        if phase == "c":
            total = own[0].astype(F32)
            for step in range(1, chips):
                across(step).wait_recv()
                total = total + far[step].astype(F32)
            out[...] = total.astype(BF16)
            for step in range(chips):
                to_mate(step).wait_send()
                if step:
                    across(step).wait_send()


class Settle(Task):
    def __init__(self, part, layer, held=None):
        self.layer = layer
        self.held = held
        self.inputs = () if held else ((part, ANY),)
        self.outs = ((part.shape, F32, VM),)
        self.scratch = (
            pltpu.VMEM((2,) + part.shape, BF16), pltpu.VMEM(part.shape, BF16),
            DMA((2,)), DMA((3,)), DMA,
        )

    def run(self, phase, refs):
        ins, (out,), (land, temp, send, recv, own_sem) = refs
        part = self.held() if self.held else ins[0]
        place = Place()
        layer = self.layer

        def to(src, dst, s, r, role):
            return place.copy(src, dst, send.at[s], recv.at[r], place.role_device(layer, role))

        def direct(role):
            if role == 2:
                return to(part, temp, 0, 2, 0)
            return to(part, land.at[0], 0, 0, 0 if role == 1 else 1)

        def relay():
            return to(temp, land.at[1], 1, 1, 1)

        for role in range(4):

            @pl.when(place.role(layer, role))
            def _():
                if phase == "z" and role == 1:
                    direct(role).start()
                if phase == "a":
                    if role > 1:
                        direct(role).start()
                    if role == 0:
                        pltpu.make_async_copy(part, land.at[1], own_sem).start()
                if phase == "b":
                    if role == 0:
                        to(temp, temp, 0, 2, 0).wait_recv()
                        relay().start()
                    if role > 1:
                        direct(role).wait_send()
                if phase == "c":
                    if role == 1:
                        direct(role).wait_send()
                    if role == 0:
                        pltpu.make_async_copy(part, land.at[1], own_sem).wait()
                        relay().wait_send()
                    if role < 2:
                        to(land.at[0], land.at[0], 0, 0, role).wait_recv()
                    if role == 1:
                        to(land.at[1], land.at[1], 0, 1, 1).wait_recv()
                    if role < 2:
                        out[...] = land[0].astype(F32) + land[1].astype(F32)


class Deliver(Task):
    def __init__(self, rows, layer):
        self.layer = layer
        self.inputs = ((rows, VM),)
        self.outs = (((2,) + rows.shape, rows.dtype, VM),)
        self.scratch = (pltpu.VMEM(rows.shape, rows.dtype), DMA((2,)), DMA((3,)))

    def run(self, phase, refs):
        (rows,), (out,), (temp, send, recv) = refs
        place = Place()
        layer = self.layer

        def to(src, dst, s, r, role):
            return place.copy(src, dst, send.at[s], recv.at[r], place.role_device(layer, role))

        def direct(role):
            if role == 2:
                return to(rows, temp, 0, 2, 0)
            return to(rows, out.at[1 - layer], 0, 0, 0 if role == 1 else 1)

        def relay():
            return to(temp, out.at[layer], 1, 1, 1)

        for role in range(4):

            @pl.when(place.role(layer, role))
            def _():
                if phase == "z" and role == 1:
                    direct(role).start()
                if phase == "a":
                    if role > 1:
                        direct(role).start()
                    if role == 0:
                        out[layer] = rows[...]
                if phase == "b" and role == 0:
                    to(temp, temp, 0, 2, 0).wait_recv()
                    relay().start()
                if phase == "c":
                    if role == 0:
                        relay().wait_send()
                    else:
                        direct(role).wait_send()
                    if role < 2:
                        to(out.at[1 - layer], out.at[1 - layer], 0, 0, role).wait_recv()
                    if role == 1:
                        to(out.at[layer], out.at[layer], 0, 1, 1).wait_recv()


class Tokens(Task):
    def __init__(self, rows):
        self.inputs = ((rows, VM),)
        self.outs = ((rows.shape[1:], rows.dtype, VM),)
        self.scratch = (DMA, DMA((2,)))

    def run(self, phase, refs):
        (rows,), (out,), (send, recv) = refs
        place = Place()
        half = rows.shape[1] // 2
        parts = (slice(0, half), slice(half, 2 * half))

        def copy(part, section):
            return place.copy(
                rows.at[1 - place.high, parts[part]], out.at[parts[part]], send, recv.at[part],
                place.plane(section, 1 - place.high),
            )

        @pl.when(place.section == place.high)
        def _():
            if phase == "a":
                copy(0, place.section).start()
                out[...] = rows[place.high]
            if phase == "c":
                copy(0, place.section).wait_send()

        @pl.when(place.section != place.high)
        def _():
            if phase == "a":
                copy(1, 1 - place.section).start()
            if phase == "c":
                copy(1, 1 - place.section).wait_send()
                copy(0, place.section).wait_recv()
                copy(1, place.section).wait_recv()


def launch(kernel, operands, outs, scratch, schedule, cid, name):
    tasks = []
    for point in schedule:
        for task, _ in point:
            if task not in tasks:
                tasks.append(task)
    operands, outs, scratch = list(operands), list(outs), list(scratch)
    n_in, n_out, n_scratch = len(operands), len(outs), len(scratch)
    spans = []
    for task in tasks:
        spans.append((len(operands), len(outs), len(scratch)))
        operands += task.inputs
        outs += task.outs
        scratch += task.scratch
    handles = []
    for task in tasks:
        for handle in task.handles:
            if handle not in handles:
                handles.append(handle)
    aliases = {}
    first_handle = len(outs)
    for handle in handles:
        if handle.array is not None:
            aliases[len(operands)] = len(outs)
            operands.append((handle.array, ANY))
        outs.append((handle.shape, handle.dtype, ANY))

    def body(*refs):
        ins = refs[: len(operands)]
        results = refs[len(operands) : len(operands) + len(outs)]
        rest = refs[len(operands) + len(outs) :]
        for number, handle in enumerate(handles):
            handle.ref = results[first_handle + number]
        views = []
        for task, (a, b, c) in zip(tasks, spans):
            views.append(
                (
                    ins[a : a + len(task.inputs)],
                    results[b : b + len(task.outs)],
                    rest[c : c + len(task.scratch)],
                )
            )
            task.refs = views[-1]

        def bg(point):
            for task, phase in schedule[point]:
                task.run(phase, task.refs)

        kernel(bg, *ins[:n_in], *results[:n_out], *rest[:n_scratch])

    done = pl.pallas_call(
        body,
        out_shape=tuple(jax.ShapeDtypeStruct(shape, dtype) for shape, dtype, _ in outs),
        in_specs=[spec for _, spec in operands],
        out_specs=tuple(spec for _, _, spec in outs),
        scratch_shapes=scratch,
        input_output_aliases=aliases,
        compiler_params=pltpu.CompilerParams(
            collective_id=cid, has_side_effects=True, vmem_limit_bytes=VMEM_LIMIT
        ),
        name=name,
    )(*[array for array, _ in operands])
    for number, handle in enumerate(handles):
        handle.array = done[first_handle + number]
        handle.ref = None
    for task, (_, b, _) in zip(tasks, spans):
        task.results = done[b : b + len(task.outs)]
    return done[:n_out]


def group_size():
    return lax.axis_size("section") * lax.axis_size("ml")


def comm_scratch(tokens, width):
    size = group_size()
    return [pltpu.VMEM((size, tokens, width), BF16)] * 2, [DMA((max(size, 6),))] * 4


def att_fwd(hidden, mod, bias, bproj, w, schedule, cid):
    tokens, width = hidden.shape
    size = group_size()
    part_width = width // size
    bufs, sems = comm_scratch(tokens, width)
    return launch(
        att_fwd_kernel,
        [(hidden, VM), (mod, VM), (bias, VM), (bproj, VM), (w.array, ANY)],
        [
            ((tokens, width), F32, VM),
            ((size, tokens, width), BF16, VM),
            ((3, size, tokens, part_width), BF16, VM),
            ((size, tokens, part_width), BF16, VM),
            ((tokens, width), F32, VM),
        ],
        [pltpu.VMEM(w.shape, BF16), pltpu.VMEM((width, part_width), BF16)]
        + bufs
        + [DMA((1,))]
        + sems,
        schedule,
        cid,
        "att_fwd",
    )


def mlp_fwd(middle, mod, b1, b2, w1, w2, schedule, cid):
    tokens, width = middle.shape
    size = group_size()
    units = w1.shape[1]
    bufs, sems = comm_scratch(tokens, width)
    return launch(
        mlp_fwd_kernel,
        [(middle, VM), (mod, VM), (b1, VM), (b2, VM), (w1.array, ANY), (w2.array, ANY)],
        [
            ((tokens, width), BF16, VM),
            ((size, tokens, width), BF16, VM),
            ((size, tokens, units), F32, VM),
            ((size, tokens, units), BF16, VM),
            ((tokens, width), F32, VM),
        ],
        [pltpu.VMEM(w1.shape, BF16)] * 2 + bufs + [DMA((2,))] + sems,
        schedule,
        cid,
        "mlp_fwd",
    )


def mlp_bwd(grad, middle, mod, branch, normed, pre, gelu, w1, w2, schedule, cid):
    tokens, width = middle.shape
    size = group_size()
    units = w1.shape[1]
    bufs, sems = comm_scratch(tokens, width)
    ins = (grad, middle, mod, branch, normed, pre, gelu)
    return launch(
        mlp_bwd_kernel,
        [(array, VM) for array in ins] + [(w1.array, ANY), (w2.array, ANY)],
        [
            ((tokens, width), F32, VM),
            (w1.shape, BF16, VM),
            (w2.shape, BF16, VM),
            ((1, units), F32, VM),
            ((1, width), F32, VM),
            ((3, width), F32, VM),
        ],
        [pltpu.VMEM(w1.shape, BF16)] * 2
        + [pltpu.VMEM((size, tokens, width), BF16), pltpu.VMEM((size, tokens, units), BF16)]
        + bufs
        + [DMA((2,))]
        + sems,
        schedule,
        cid,
        "mlp_bwd",
    )


def att_bwd(gmid, hidden, mod, branch, normed, proj, att, w, schedule, cid):
    tokens, width = gmid.shape
    size = group_size()
    part_width = width // size
    bufs, sems = comm_scratch(tokens, width)
    seq = size * tokens
    ins = (gmid, hidden, mod, branch, normed, proj, att)
    return launch(
        att_bwd_kernel,
        [(array, VM) for array in ins] + [(w.array, ANY)],
        [
            ((tokens, width), BF16, VM),
            (w.shape, BF16, VM),
            ((1, 3 * part_width), F32, VM),
            ((1, width), F32, VM),
            ((3, width), F32, VM),
        ],
        [
            pltpu.VMEM(w.shape, BF16),
            pltpu.VMEM((width, part_width), BF16),
            pltpu.VMEM((size, tokens, width), BF16),
            pltpu.VMEM((size, tokens, 3 * part_width), BF16),
            pltpu.VMEM((seq, part_width), F32),
            pltpu.VMEM((seq, part_width), F32),
        ]
        + bufs
        + [DMA((1,))]
        + sems,
        schedule,
        cid,
        "att_bwd",
    )


def prologue_kernel(
    bg,
    cond_ref, wada_ref, bada_ref, bias_ref,
    modul_ref, act_ref, bias_out,
    cond_land, share, land, cond_send, cond_recv, mod_send, mod_recv, b_send, b_recv,
):
    place = Place()
    section, dp, high = place.section, place.dp, place.high
    place.greet_all()

    def spread(step):
        other = lax.rem(dp + step, place.n_dp)
        return place.copy(
            cond_ref.at[other], cond_land.at[dp], cond_send.at[step], cond_recv.at[dp],
            (section, other, high, place.low),
        )

    def spread_wait(step):
        other = lax.rem(dp + step, place.n_dp)
        return place.copy(
            cond_land.at[other], cond_land.at[other], cond_send.at[step], cond_recv.at[other],
            (section, other, high, place.low),
        )

    cond_land[dp] = cond_ref[dp]
    for step in range(1, place.n_dp):
        spread(step).start()

    def bias_copy(target):
        return place.copy(
            bias_ref, bias_out.at[section], b_send.at[target], b_recv.at[section],
            place.plane(high, target),
        )

    here = section == high
    for target in range(2):

        @pl.when(jnp.logical_not(here & (high == target)))
        def _():
            bias_copy(target).start()

    @pl.when(here)
    def _():
        bias_out[section] = bias_ref[...]

    bg(0)
    for step in range(1, place.n_dp):
        spread_wait(step).wait_recv()
    parts = [cond_land[index] for index in range(place.n_dp)]
    act = jax.nn.silu(jnp.concatenate(parts, axis=0)).astype(BF16)
    act_ref[...] = act
    bias = jnp.where(dp == 0, bada_ref[...], 0.0)
    product = dot_nn(act, wada_ref[...])
    for row in range(2 * place.n_dp):
        share[row] = product[row : row + 1] + bias
    finish = place.exchange(
        lambda device: share.at[device[1] * 2 + device[2]], land, mod_send, mod_recv
    )
    bg(1)
    bg(2)
    finish()
    for layer in range(2):
        for part in range(2 * place.n_low):
            total = land[layer * place.n_dp * 2 * place.n_low + part]
            for index in range(1, place.n_dp):
                total = total + land[(layer * place.n_dp + index) * 2 * place.n_low + part]
            modul_ref[layer * 2 * place.n_low + part] = total
    bg(3)
    for step in range(1, place.n_dp):
        spread(step).wait_send()
    for target in range(2):

        @pl.when(jnp.logical_not(here & (high == target)))
        def _():
            bias_copy(target).wait_send()

        @pl.when(jnp.logical_not(here & (section == target)))
        def _():
            place.copy(
                bias_out.at[target], bias_out.at[target], b_send.at[0], b_recv.at[target],
                place.plane(section, 1 - high),
            ).wait_recv()

    bg(4)


def prologue(cond, wada, bada, bias, schedule, cid):
    n_dp, _, chunk = cond.shape
    n_mp = 2 * lax.axis_size("ml")
    total = 2 * n_dp * n_mp
    share = wada.shape[1]
    return launch(
        prologue_kernel,
        [(cond, VM), (wada, VM), (bada, VM), (bias, VM)],
        [
            ((2 * n_mp, 1, share), F32, VM),
            ((2 * n_dp, chunk), BF16, VM),
            ((2,) + bias.shape, F32, VM),
        ],
        [
            pltpu.VMEM((n_dp, 2, chunk), F32),
            pltpu.VMEM((2 * n_dp, 1, share), F32),
            pltpu.VMEM((total, 1, share), F32),
            DMA((n_dp,)),
            DMA((n_dp,)),
            DMA((total,)),
            DMA((total,)),
            DMA((2,)),
            DMA((2,)),
        ],
        schedule,
        cid,
        "prologue",
    )


def epilogue_kernel(
    bg,
    dmod_ref, act_ref, wada_ref, dbias_ref,
    gada_ref, gbada_ref, gact_ref, gbias_ref,
    mod_land, act_stage, act_land, bias_land, bias_stage, bias_final,
    mod_send, mod_recv, act_send, act_recv, d_send, d_recv, b_send, b_recv,
):
    place = Place()
    section, dp, high = place.section, place.dp, place.high
    place.greet_all()
    finish_mod = place.exchange(
        lambda device: dmod_ref.at[(device[0] * 2 + device[2]) * place.n_low + device[3]],
        mod_land, mod_send, mod_recv,
    )

    def spread(step):
        other = lax.rem(dp + step, place.n_dp)
        return place.copy(
            dbias_ref, bias_land.at[dp], d_send.at[step], d_recv.at[dp],
            (section, other, high, place.low),
        )

    for step in range(1, place.n_dp):
        spread(step).start()
    bg(0)
    finish_mod()
    parts = 2 * place.n_low
    latents = []
    for index in range(place.n_dp):
        for micro in range(2):
            total = 0.0
            for sec in range(2):
                for low in range(place.n_low):
                    number = ((sec * place.n_dp + index) * 2 + micro) * place.n_low + low
                    total = total + mod_land[number]
            latents.append(total)
    dmod = jnp.concatenate(latents, axis=0).astype(BF16)
    back = dot_nt(dmod, wada_ref[...])
    for index in range(place.n_dp):
        act_stage[index] = back[2 * index : 2 * index + 2]
    finish_act = place.exchange(lambda device: act_stage.at[device[1]], act_land, act_send, act_recv)
    bias_sum = dbias_ref[...]
    for step in range(1, place.n_dp):
        other = lax.rem(dp + step, place.n_dp)
        place.copy(
            bias_land.at[other], bias_land.at[other], d_send.at[step], d_recv.at[other],
            (section, other, high, place.low),
        ).wait_recv()
        bias_sum = bias_sum + bias_land[other]
    bias_stage[...] = bias_sum

    def settle(layer):
        return place.copy(
            bias_stage.at[layer], bias_final.at[high], b_send.at[layer], b_recv.at[high],
            place.plane(layer, section),
        )

    for layer in range(2):
        here = (section == layer) & (high == section)

        @pl.when(here)
        def _():
            bias_final[high] = bias_stage[layer]

        @pl.when(jnp.logical_not(here))
        def _():
            settle(layer).start()

    bg(1)
    gbada_ref[...] = col_sum(dmod.astype(F32))
    gada_ref[...] = dot_tn(act_ref[...], dmod)
    bg(2)
    finish_act()
    for index in range(place.n_dp):
        total = 0.0
        for sec in range(2):
            for part in range(parts):
                total = total + act_land[(sec * place.n_dp + index) * parts + part]
        gact_ref[index] = total
    bg(3)
    for half in range(2):
        here = (section == high) & (high == half)

        @pl.when(jnp.logical_not(here))
        def _():
            place.copy(
                bias_final.at[half], bias_final.at[half], b_send.at[0], b_recv.at[half],
                place.plane(high, half),
            ).wait_recv()

    gbias_ref[...] = bias_final[0] + bias_final[1]
    for layer in range(2):

        @pl.when(jnp.logical_not((section == layer) & (high == section)))
        def _():
            settle(layer).wait_send()

    for step in range(1, place.n_dp):
        spread(step).wait_send()
    bg(4)


def epilogue(dmod, act, wada, dbias, schedule, cid):
    n_dp, n_mp = lax.axis_size("dp"), 2 * lax.axis_size("ml")
    total = 2 * n_dp * n_mp
    chunk, share = wada.shape
    row = dbias.shape[1:]
    return launch(
        epilogue_kernel,
        [(dmod, VM), (act, VM), (wada, VM), (dbias, VM)],
        [
            ((chunk, share), F32, VM),
            ((1, share), F32, VM),
            ((n_dp, 2, chunk), F32, VM),
            (row, F32, VM),
        ],
        [
            pltpu.VMEM((total, 1, share), F32),
            pltpu.VMEM((n_dp, 2, chunk), F32),
            pltpu.VMEM((total, 2, chunk), F32),
            pltpu.VMEM((n_dp,) + dbias.shape, F32),
            pltpu.VMEM(dbias.shape, F32),
            pltpu.VMEM((2,) + row, F32),
            DMA((total,)),
            DMA((total,)),
            DMA((total,)),
            DMA((total,)),
            DMA((n_dp,)),
            DMA((n_dp,)),
            DMA((2,)),
            DMA((2,)),
        ],
        schedule,
        cid,
        "epilogue",
    )


def per_device(
    latents_in, condition, cotangent,
    modulation_weight, modulation_bias, query_key_value_weight, query_value_bias,
    output_proj_weight, output_proj_bias, first_dense_weight, first_dense_bias,
    second_dense_weight, second_dense_bias,
):
    section, dp = lax.axis_index("section"), lax.axis_index("dp")
    n_dp, n_low = lax.axis_size("dp"), lax.axis_size("ml")
    n_mp = 2 * n_low
    width = latents_in.shape[-1]
    rows = modulation_weight.shape[1]
    cols = modulation_weight.shape[2]
    part_width = query_key_value_weight.shape[3]
    units = first_dense_weight.shape[2]

    item = jnp.stack(
        [
            jnp.concatenate(
                [query_key_value_weight[0].reshape(rows, -1), output_proj_weight[0].T], axis=1
            ),
            first_dense_weight[0],
            second_dense_weight[0].T,
        ]
    )
    cond = condition[:, 0].astype(F32)
    packed = jnp.concatenate(
        [
            query_value_bias[0, 0], query_value_bias[0, 1], first_dense_bias[0],
            output_proj_bias[0], second_dense_bias[0],
        ]
    ).astype(F32)[None]
    w = [[Handle((width, units), BF16) for _ in range(3)] for _ in range(2)]
    collect = [[Collect(item, t, l, w[l][t]) for t in range(3)] for l in range(2)]
    widen = [[Widen(w[l][t]) for t in range(3)] for l in range(2)]
    tokens_in = Tokens(latents_in[:, 0])
    tokens_cot = Tokens(cotangent[:, 0])

    def plan(*points):
        out = []
        for point in points:
            out.append([(task, phase) for task, phases in point for phase in phases])
        return out

    c, x = collect, widen
    modul, act_rows, biases = prologue(
        cond.reshape(2, n_dp, rows).transpose(1, 0, 2),
        modulation_weight[0],
        modulation_bias.astype(F32),
        packed,
        plan(
            [(tokens_in, "a"), (c[0][0], "a"), (c[1][0], "a")],
            [(c[0][0], "c"), (c[1][0], "c"), (c[0][1], "a"), (c[1][1], "a")]
            + [(c[0][0], "b"), (x[0][0], "a"), (c[1][0], "b")],
            [(c[0][1], "c"), (c[1][1], "c"), (c[0][2], "a"), (c[1][2], "a")]
            + [(x[0][0], "b"), (c[0][1], "b"), (x[0][1], "a"), (c[1][1], "b")],
            [],
            [(c[0][2], "c"), (c[1][2], "c"), (c[0][2], "b"), (c[1][2], "b"), (x[0][1], "b")]
            + [(tokens_in, "c"), (x[0][0], "c"), (x[0][1], "c")],
        ),
        1,
    )
    modul = modul.reshape(2, 6, width)
    bounds = [0, part_width, 2 * part_width, 2 * part_width + units, 2 * part_width + units + width]
    bqkv = jnp.concatenate(
        [
            biases[..., : bounds[1]], jnp.zeros((2, 1, part_width), F32),
            biases[..., bounds[1] : bounds[2]],
        ],
        axis=-1,
    )
    b1 = biases[..., bounds[2] : bounds[3]]
    bproj = biases[..., bounds[3] : bounds[4]]
    b2 = biases[..., bounds[4] :]

    hidden = [tokens_in.results[0]]
    att_plan = [
        plan(
            [(x[0][2], "a")],
            [],
            [],
            [(x[0][2], "b")],
            [(x[0][2], "c")],
        ),
        plan(
            [(x[1][1], "a"), (x[1][2], "a"), (tokens_cot, "a")],
            [],
            [],
            [(x[1][1], "b"), (x[1][2], "b")],
            [(x[1][1], "c"), (x[1][2], "c"), (tokens_cot, "c")],
        ),
    ]
    saved = []
    for layer in range(2):
        middle, normed, proj, att, branch = att_fwd(
            hidden[layer], modul[layer], bqkv[layer], bproj[layer], w[layer][0], att_plan[layer],
            2 + 2 * layer,
        )
        if layer == 0:
            mlp_plan = plan(
                [(x[1][0], "a")],
                [],
                [],
                [(x[1][0], "b")],
                [(x[1][0], "c")],
            )
        else:
            acts_first = Deliver(hidden[1], 0)
            mlp_plan = plan([], [], [], [], [])
        out, normed2, pre, gelu, branch2 = mlp_fwd(
            middle, modul[layer], b1[layer], b2[layer], w[layer][1], w[layer][2], mlp_plan,
            3 + 2 * layer,
        )
        saved.append((middle, normed, proj, att, branch, normed2, pre, gelu, branch2))
        hidden.append(out)

    grad = tokens_cot.results[0]
    narrow = [[None] * 3 for _ in range(2)]
    settle = [[None] * 3 for _ in range(2)]
    d_bias, d_mod, gins = {}, {}, {}
    acts_second = Deliver(hidden[2], 1)
    for layer in (1, 0):
        middle, normed, proj, att, branch, normed2, pre, gelu, branch2 = saved[layer]
        if layer == 1:
            mlp_plan = plan(
                [(acts_first, "az"), (acts_second, "az")],
                [],
                [(acts_first, "b"), (acts_second, "b")],
                [],
                [(acts_first, "c"), (acts_second, "c")],
            )
        else:
            third = narrow[1][0]
            mlp_plan = plan([(third, "a")], [(third, "b")], [], [], [(third, "c")])
        gmid, dw1, dw2, db1, db2, dmod2 = mlp_bwd(
            grad, middle, modul[layer], branch2, normed2, pre, gelu, w[layer][1], w[layer][2],
            mlp_plan, 6 + 2 * (1 - layer),
        )
        narrow[layer][1], narrow[layer][2] = Narrow(dw1), Narrow(dw2)
        one, two = narrow[layer][1], narrow[layer][2]
        if layer == 0:
            settle[1][0] = Settle(narrow[1][0].results[0], 1)
            gin_second = Deliver(gins[1], 1)
        att_plan = plan(
            [(two, "a"), (one, "a")], [(two, "b"), (one, "b")], [], [], [(two, "c"), (one, "c")]
        )
        gin, dw, dbqkv, dbproj, dmod1 = att_bwd(
            gmid, hidden[layer], modul[layer], branch, normed, proj, att, w[layer][0],
            att_plan, 7 + 2 * (1 - layer),
        )
        for tensor in (1, 2):
            settle[layer][tensor] = Settle(narrow[layer][tensor].results[0], layer)
        narrow[layer][0] = Narrow(dw)
        gins[layer] = grad = gin
        d_bias[layer] = jnp.concatenate(
            [dbqkv[:, :part_width], dbqkv[:, 2 * part_width :], db1, dbproj, db2], axis=1
        )
        d_mod[layer] = jnp.concatenate([dmod1.reshape(-1), dmod2.reshape(-1)])

    last = narrow[0][0]
    final = Settle(jax.ShapeDtypeStruct((rows, units), BF16), 0, held=lambda: last.refs[1][0])
    settle[0][0] = final
    gin_first = Deliver(gins[0], 0)
    dmod = jnp.stack([d_mod[0], d_mod[1]]).reshape(2 * n_mp, 1, cols)
    g_wada, g_bada, g_act, g_bias = epilogue(
        dmod,
        act_rows,
        modulation_weight[0],
        jnp.stack([d_bias[0], d_bias[1]]),
        plan(
            [(last, "a"), (settle[0][2], "az"), (settle[1][2], "az")],
            [(settle[0][2], "b"), (settle[1][2], "b"), (settle[0][1], "az"), (settle[1][1], "az")]
            + [(last, "b"), (gin_first, "az"), (gin_second, "az")],
            [(settle[0][1], "b"), (settle[1][1], "b"), (settle[1][0], "az"), (last, "c"), (final, "az")]
            + [(gin_first, "b"), (gin_second, "b")],
            [(settle[1][0], "b"), (final, "b"), (settle[0][2], "c"), (settle[1][2], "c")],
            [(settle[0][1], "c"), (settle[1][1], "c"), (gin_first, "c"), (gin_second, "c")]
            + [(settle[1][0], "c"), (final, "c")],
        ),
        10,
    )
    g_act = g_act.transpose(1, 0, 2).reshape(2, width)
    low_section = section == 0

    def own_block(first, second):
        return jnp.where(low_section, first.results[0], second.results[0])

    g_att, g_one, g_two = [own_block(settle[0][t], settle[1][t]) for t in range(3)]
    g_qkv = g_att[:, : 3 * part_width].reshape(rows, 3, part_width)
    g_proj = g_att[:, 3 * part_width :].T

    def dp_part(vec):
        size = vec.shape[-1] // n_dp
        return lax.dynamic_slice_in_dim(vec, dp * size, size, vec.ndim - 1)

    g_bias = g_bias[0]
    g_bqv = dp_part(g_bias[: bounds[2]].reshape(2, part_width))
    g_b1 = dp_part(g_bias[bounds[2] : bounds[3]])
    g_bproj = dp_part(g_bias[bounds[3] : bounds[4]])
    g_b2 = dp_part(g_bias[bounds[4] :])
    g_bada = dp_part(g_bada[0])
    _, silu_back = jax.vjp(jax.nn.silu, cond)
    g_cond = silu_back(g_act)[0][:, None]
    acts_out = own_block(acts_first, acts_second)[None, :, None]
    grad_input = own_block(gin_first, gin_second).astype(F32)[None, :, None]
    return (
        acts_out,
        grad_input,
        g_cond,
        g_wada[None],
        g_bada[None],
        g_qkv[None],
        g_bqv[None],
        g_proj[None],
        g_bproj[None],
        g_one[None],
        g_b1[None],
        g_two.T[None],
        g_b2[None],
    )


def solution(mesh):
    sizes = mesh.shape
    grid = mesh.devices.reshape(sizes["section"], sizes["dp"], 2, sizes["mp"] // 2)
    fine = Mesh(grid, ("section", "dp", "mh", "ml"))
    mp = ("mh", "ml")
    in_specs = (
        P(None, "dp", mp, None),
        P(None, "dp", None),
        P(None, "dp", mp, None),
        P("section", "dp", mp),
        P("section", mp),
        P("section", "dp", None, mp),
        P("section", None, mp),
        P("section", mp, "dp"),
        P("section", None),
        P("section", "dp", mp),
        P("section", mp),
        P("section", mp, "dp"),
        P("section", None),
    )
    mpdp = ("mh", "ml", "dp")
    out_specs = (
        P("section", None, "dp", mp, None),
        P("section", None, "dp", mp, None),
        P(None, "dp", None),
        P("section", "dp", mp),
        P("section", mpdp),
        P("section", "dp", None, mp),
        P("section", None, mpdp),
        P("section", mp, "dp"),
        P("section", "dp"),
        P("section", "dp", mp),
        P("section", mpdp),
        P("section", mp, "dp"),
        P("section", "dp"),
    )
    return jax.shard_map(
        per_device, mesh=fine, in_specs=in_specs, out_specs=out_specs, check_vma=False
    )
```

```python
import jax
import jax.numpy as jnp
from jax import lax
from jax.experimental import pallas as pl
from jax.experimental.pallas import tpu as pltpu
from jax.sharding import Mesh
from jax.sharding import PartitionSpec as P

HEAD_SIZE = 72
EPS = 1e-06
MESH = pl.DeviceIdType.MESH
BF16 = jnp.bfloat16
F32 = jnp.float32
GELU_C = 0.7978845608028654
GELU_A = 0.044715
NT = (((1,), (1,)), ((), ()))
TN = (((0,), (0,)), ((), ()))
VMEM_LIMIT = 50 * 1024 * 1024


def dot_nn(a, b):
    return jnp.dot(a, b, preferred_element_type=F32)


def dot_nt(a, b):
    return lax.dot_general(a, b, NT, preferred_element_type=F32)


def dot_tn(a, b):
    return lax.dot_general(a, b, TN, preferred_element_type=F32)


def norm_parts(values):
    center = values - jnp.mean(values, axis=-1, keepdims=True)
    spread = jnp.mean(center * center, axis=-1, keepdims=True)
    rstd = lax.rsqrt(spread + EPS)
    return center * rstd, rstd


def norm_back(grad, normed, rstd, scale):
    dn = grad * (1.0 + scale)
    first = jnp.mean(dn, axis=-1, keepdims=True)
    second = jnp.mean(dn * normed, axis=-1, keepdims=True)
    return (dn - first - normed * second) * rstd


def col_sum(values):
    return jnp.sum(values, axis=0, keepdims=True)


class Group:
    def __init__(self, tokens):
        self.low = lax.axis_size("ml")
        self.size = lax.axis_size("section") * self.low
        self.me = lax.axis_index("section") * self.low + lax.axis_index("ml")
        self.square = self.size == 4
        self.half = (slice(0, tokens // 2), slice(tokens // 2, tokens))

    def device(self, member):
        return (
            lax.div(member, self.low),
            lax.axis_index("dp"),
            lax.axis_index("mh"),
            lax.rem(member, self.low),
        )

    def member(self, step):
        if not self.square:
            return lax.rem(self.me + step, self.size)
        section = lax.rem(lax.axis_index("section") + lax.rem(step, 2), 2)
        low = lax.rem(lax.axis_index("ml") + lax.div(step, 2), 2)
        return section * 2 + low

    def copy(self, src, dst, send_sem, recv_sem, member):
        return pltpu.make_async_remote_copy(
            src_ref=src,
            dst_ref=dst,
            send_sem=send_sem,
            recv_sem=recv_sem,
            device_id=self.device(member),
            device_id_type=MESH,
        )

    def first_copies(self, buf, send_sem, recv_sem):
        steps = (1, 2) if self.square else range(1, self.size)
        mine = buf.at[self.me]
        return [
            self.copy(mine, mine, send_sem.at[step], recv_sem.at[self.me], self.member(step))
            for step in steps
        ]

    def relay_copy(self, buf, send_sem, recv_sem, step):
        rows = buf.at[self.member(step), self.half[step - 1]]
        return self.copy(
            rows, rows, send_sem.at[2 + step], recv_sem.at[3 + step], self.member(3 - step)
        )

    def spread(self, buf, send_sem, recv_sem):
        for copy in self.first_copies(buf, send_sem, recv_sem):
            copy.start()

    def arrive(self, buf, send_sem, recv_sem, step):
        def landed(rows, sem):
            self.copy(rows, rows, send_sem.at[1], sem, self.member(1)).wait_recv()

        if not self.square:

            @pl.when(step > 0)
            def _():
                landed(buf.at[self.member(step)], recv_sem.at[self.member(step)])

            return

        @pl.when(step == 1)
        def _():
            for near in (1, 2):
                landed(buf.at[self.member(near)], recv_sem.at[self.member(near)])
                self.relay_copy(buf, send_sem, recv_sem, near).start()

        @pl.when(step == 3)
        def _():
            for near in (1, 2):
                landed(buf.at[self.member(3), self.half[near - 1]], recv_sem.at[3 + near])

    def spread_sent(self, buf, send_sem, recv_sem):
        for copy in self.first_copies(buf, send_sem, recv_sem):
            copy.wait_send()
        if self.square:
            for step in (1, 2):
                self.relay_copy(buf, send_sem, recv_sem, step).wait_send()

    def straight(self, stage, landing, send_sem, recv_sem, step):
        rows = self.half[step - 1]
        return self.copy(
            stage.at[self.member(step), rows], landing.at[step - 1, rows],
            send_sem.at[step - 1], recv_sem.at[step - 1], self.member(step),
        )

    def corner(self, stage, landing, send_sem, recv_sem, step):
        rows = self.half[step - 1]
        return self.copy(
            stage.at[self.member(3), rows], landing.at[2, rows],
            send_sem.at[1 + step], recv_sem.at[1 + step], self.member(step),
        )

    def summed(self, landing, send_sem, recv_sem, step):
        rows = self.half[2 - step]
        return self.copy(
            landing.at[3, rows], landing.at[step - 1, rows],
            send_sem.at[3 + step], recv_sem.at[3 + step], self.member(step),
        )

    def reduce_copy(self, stage, landing, send_sem, recv_sem, member):
        return self.copy(
            stage.at[member], landing.at[self.me], send_sem.at[member], recv_sem.at[self.me], member
        )

    def give(self, stage, landing, send_sem, recv_sem, step):
        args = (stage, landing, send_sem, recv_sem)
        if not self.square:

            @pl.when(step > 0)
            def _():
                self.reduce_copy(*args, self.member(step)).start()

            return
        for near in (1, 2):

            @pl.when(step == near)
            def _():
                self.straight(*args, near).start()

        @pl.when(step == 3)
        def _():
            for near in (1, 2):
                self.corner(*args, near).start()

    def combine(self, stage, landing, send_sem, recv_sem):
        if not self.square:
            return
        for step in (1, 2):
            rows = self.half[2 - step]
            self.copy(
                landing.at[2, rows], landing.at[2, rows], send_sem.at[0], recv_sem.at[4 - step],
                self.member(1),
            ).wait_recv()
            total = stage[self.member(step), rows].astype(F32) + landing[2, rows].astype(F32)
            landing[3, rows] = total.astype(BF16)
            self.summed(landing, send_sem, recv_sem, step).start()

    def landed_sum(self, own, stage, landing, send_sem, recv_sem):
        args = (stage, landing, send_sem, recv_sem)
        total = own

        def landed(rows, sem):
            self.copy(rows, rows, send_sem.at[0], sem, self.member(1)).wait_recv()

        if self.square:
            for step in (1, 2):
                first, second = self.half[step - 1], self.half[2 - step]
                landed(landing.at[step - 1, first], recv_sem.at[step - 1])
                landed(landing.at[step - 1, second], recv_sem.at[3 + step])
                total = total + landing[step - 1].astype(F32)
            for step in (1, 2):
                self.straight(*args, step).wait_send()
                self.corner(*args, step).wait_send()
                self.summed(landing, send_sem, recv_sem, step).wait_send()
            return total
        for step in range(1, self.size):
            member = self.member(step)
            landed(landing.at[member], recv_sem.at[member])
            total = total + landing[member].astype(F32)
        for step in range(1, self.size):
            self.reduce_copy(*args, self.member(step)).wait_send()
        return total


def load(src, dst, sem):
    copy = pltpu.make_async_copy(src, dst, sem)
    copy.start()
    return [copy]


def lane_mask(shape, head):
    lanes = lax.broadcasted_iota(jnp.int32, shape, len(shape) - 1)
    return (lanes >= head * HEAD_SIZE) & (lanes < (head + 1) * HEAD_SIZE)


def row_mask(shape, head):
    rows = lax.broadcasted_iota(jnp.int32, shape, 0)
    return (rows >= head * HEAD_SIZE) & (rows < (head + 1) * HEAD_SIZE)


def stack_heads(block):
    heads = block.shape[-1] // HEAD_SIZE
    zero = jnp.zeros_like(block)
    return jnp.concatenate(
        [jnp.where(lane_mask(block.shape, head), block, zero) for head in range(heads)], axis=0
    )


def identity(size):
    rows = lax.broadcasted_iota(jnp.int32, (size, size), 0)
    cols = lax.broadcasted_iota(jnp.int32, (size, size), 1)
    return jnp.where(rows == cols, 1.0, 0.0).astype(BF16)


def att_fwd_kernel(
    bg,
    hidden_ref, mod_ref, bias_ref, bproj_ref, w_ref,
    middle_ref, normed_ref, proj_ref, att_ref, branch_ref,
    w_buf, wo_buf, stage, landing, w_sem, ag_send, ag_recv, rs_send, rs_recv,
):
    tokens, width = hidden_ref.shape
    group = Group(tokens)
    me, size = group.me, group.size
    part_width = att_ref.shape[-1]
    heads = part_width // HEAD_SIZE
    loads = load(w_ref, w_buf, w_sem.at[0])
    hidden = hidden_ref[...].astype(F32)
    normed, _ = norm_parts(hidden)
    normed_ref[me] = (normed * (1.0 + mod_ref[1:2]) + mod_ref[0:1]).astype(BF16)
    Place().greet()
    group.spread(normed_ref, ag_send, ag_recv)
    bg(0)
    for copy in loads:
        copy.wait()

    def project(step, carry):
        member = group.member(step)
        group.arrive(normed_ref, ag_send, ag_recv, step)
        out = dot_nn(normed_ref[member], w_buf[:, : 3 * part_width]) + bias_ref[...]
        for part in range(3):
            cols = slice(part * part_width, (part + 1) * part_width)
            proj_ref[part, member] = out[:, cols].astype(BF16)
        return carry

    wo_buf[...] = w_buf[:, 3 * part_width :]
    lax.fori_loop(0, size, project, 0)
    bg(1)
    seq = size * tokens
    keys = proj_ref[1].reshape(seq, -1)
    values = proj_ref[2].reshape(seq, -1)

    def attend(member):
        stacked = stack_heads(proj_ref[0, member])
        powered = jnp.exp(dot_nt(stacked, keys) * HEAD_SIZE**-0.5)
        probs = powered * (1.0 / jnp.sum(powered, axis=-1, keepdims=True))
        mixed = dot_nn(probs.astype(BF16), values)
        out = mixed[:tokens]
        for head in range(1, heads):
            part = mixed[head * tokens : (head + 1) * tokens]
            out = jnp.where(lane_mask(part.shape, head), part, out)
        low = out.astype(BF16)
        att_ref[member] = low
        return dot_nt(low, wo_buf[...])

    def send(step, carry):
        @pl.when(step == size)
        def _():
            group.combine(stage, landing, rs_send, rs_recv)
            bg(2)

        member = group.member(size - step)
        stage[member] = attend(member).astype(BF16)
        group.give(stage, landing, rs_send, rs_recv, size - step)
        return carry

    lax.fori_loop(1, size + 1, send, 0)
    group.spread_sent(normed_ref, ag_send, ag_recv)
    bg(3)
    own = stage[me].astype(F32)
    branch = group.landed_sum(own, stage, landing, rs_send, rs_recv) + bproj_ref[...]
    branch_ref[...] = branch
    middle_ref[...] = hidden_ref[...].astype(F32) + mod_ref[2:3] * branch
    bg(4)


def mlp_fwd_kernel(
    bg,
    middle_ref, mod_ref, b1_ref, b2_ref, w1_ref, w2_ref,
    out_ref, normed_ref, pre_ref, gelu_ref, branch_ref,
    w1_buf, w2_buf, stage, landing, w_sem, ag_send, ag_recv, rs_send, rs_recv,
):
    group = Group(middle_ref.shape[0])
    me, size = group.me, group.size
    loads = load(w1_ref, w1_buf, w_sem.at[0]) + load(w2_ref, w2_buf, w_sem.at[1])
    normed, _ = norm_parts(middle_ref[...])
    normed_ref[me] = (normed * (1.0 + mod_ref[4:5]) + mod_ref[3:4]).astype(BF16)
    Place().greet()
    group.spread(normed_ref, ag_send, ag_recv)
    bg(0)
    for copy in loads:
        copy.wait()

    def dense(member):
        pre = dot_nn(normed_ref[member], w1_buf[...]) + b1_ref[...]
        pre_ref[member] = pre
        bent = jnp.tanh(GELU_C * (pre + GELU_A * pre * pre * pre))
        low = (0.5 * pre * (1.0 + bent)).astype(BF16)
        gelu_ref[member] = low
        return dot_nt(low, w2_buf[...])

    def send(step, carry):
        @pl.when(step == 1)
        def _():
            bg(1)

        member = group.member(step)
        group.arrive(normed_ref, ag_send, ag_recv, step)
        stage[member] = dense(member).astype(BF16)
        group.give(stage, landing, rs_send, rs_recv, step)
        return carry

    lax.fori_loop(0, size, send, 0)
    group.combine(stage, landing, rs_send, rs_recv)
    bg(2)
    group.spread_sent(normed_ref, ag_send, ag_recv)
    bg(3)
    own = stage[me].astype(F32)
    branch = group.landed_sum(own, stage, landing, rs_send, rs_recv) + b2_ref[...]
    branch_ref[...] = branch
    out_ref[...] = (middle_ref[...] + mod_ref[5:6] * branch).astype(BF16)
    bg(4)


def weight_grad(lhs_ref, rhs, out_ref, tile):
    def body(index, carry):
        cols = pl.ds(pl.multiple_of(index * tile, tile), tile)
        out_ref[cols, :] = dot_tn(lhs_ref[:, cols], rhs).astype(BF16)
        return carry

    lax.fori_loop(0, lhs_ref.shape[-1] // tile, body, 0)


def mlp_bwd_kernel(
    bg,
    grad_ref, middle_ref, mod_ref, branch_ref, normed_ref, pre_ref, gelu_ref, w1_ref, w2_ref,
    gmid_ref, dw1_ref, dw2_ref, db1_ref, db2_ref, dmod_ref,
    w1_buf, w2_buf, dbr, dpre, stage, landing, w_sem, ag_send, ag_recv, rs_send, rs_recv,
):
    tokens, width = grad_ref.shape
    group = Group(tokens)
    me, size = group.me, group.size
    loads = load(w1_ref, w1_buf, w_sem.at[0]) + load(w2_ref, w2_buf, w_sem.at[1])
    grad = grad_ref[...].astype(F32)
    dbr[me] = (grad * mod_ref[5:6]).astype(BF16)
    Place().greet()
    group.spread(dbr, ag_send, ag_recv)
    bg(0)
    dmod_ref[2:3] = col_sum(grad * branch_ref[...])
    for copy in loads:
        copy.wait()

    def back(member):
        dgelu = dot_nn(dbr[member], w2_buf[...])
        pre = pre_ref[member]
        bent = jnp.tanh(GELU_C * (pre + GELU_A * pre * pre * pre))
        slope = 0.5 * (1.0 + bent) + 0.5 * pre * (1.0 - bent * bent) * (
            GELU_C * (1.0 + 3.0 * GELU_A * pre * pre)
        )
        low = (dgelu * slope).astype(BF16)
        dpre[member] = low
        return dot_nt(low, w1_buf[...])

    stage[me] = back(me).astype(BF16)
    bg(1)

    def send(step, carry):
        member = group.member(step)
        group.arrive(dbr, ag_send, ag_recv, step)
        stage[member] = back(member).astype(BF16)
        group.give(stage, landing, rs_send, rs_recv, step)
        return carry

    lax.fori_loop(1, size, send, 0)
    group.combine(stage, landing, rs_send, rs_recv)
    bg(2)
    seq = size * tokens
    dpre_all = dpre[...].reshape(seq, -1)
    gelu_all = gelu_ref[...].reshape(seq, -1)
    db1_ref[...] = col_sum(dpre_all.astype(F32))
    db2_ref[...] = col_sum(dbr[...].reshape(seq, -1).astype(F32))
    weight_grad(normed_ref.reshape(seq, width), dpre_all, dw1_ref, 128)
    weight_grad(dbr.reshape(seq, width), gelu_all, dw2_ref, 128)
    group.spread_sent(dbr, ag_send, ag_recv)
    bg(3)
    total = group.landed_sum(stage[me].astype(F32), stage, landing, rs_send, rs_recv)
    normed, rstd = norm_parts(middle_ref[...])
    dmod_ref[0:1] = col_sum(total)
    dmod_ref[1:2] = col_sum(total * normed)
    gmid_ref[...] = norm_back(total, normed, rstd, mod_ref[4:5]) + grad_ref[...].astype(F32)
    bg(4)


def att_bwd_kernel(
    bg,
    gmid_ref, hidden_ref, mod_ref, branch_ref, normed_ref, proj_ref, att_ref, w_ref,
    gin_ref, dw_ref, dbqkv_ref, dbproj_ref, dmod_ref,
    w_buf, wo_buf, dba, dproj, dkey, dval, stage, landing, w_sem, ag_send, ag_recv, rs_send, rs_recv,
):
    tokens, width = gmid_ref.shape
    group = Group(tokens)
    me, size = group.me, group.size
    seq = size * tokens
    part_width = att_ref.shape[-1]
    heads = part_width // HEAD_SIZE
    loads = load(w_ref, w_buf, w_sem.at[0])
    gmid = gmid_ref[...]
    dba[me] = (gmid * mod_ref[2:3]).astype(BF16)
    Place().greet()
    group.spread(dba, ag_send, ag_recv)
    bg(0)
    dmod_ref[2:3] = col_sum(gmid * branch_ref[...])
    keys = proj_ref[1].reshape(seq, part_width)
    values = proj_ref[2].reshape(seq, part_width)
    keys_t = dot_nt(identity(part_width), keys).astype(BF16)
    dkey[...] = jnp.zeros_like(dkey)
    dval[...] = jnp.zeros_like(dval)
    for copy in loads:
        copy.wait()
    wo_buf[...] = w_buf[:, 3 * part_width :]

    def back(step, carry):
        @pl.when(step == 1)
        def _():
            bg(1)

        member = group.member(step)
        group.arrive(dba, ag_send, ag_recv, step)
        datt = dot_nn(dba[member], wo_buf[...]).astype(BF16)
        datt_st = stack_heads(datt)
        query_st = stack_heads(proj_ref[0, member])
        powered = jnp.exp(dot_nt(keys, query_st) * HEAD_SIZE**-0.5)
        probs = powered * (1.0 / jnp.sum(powered, axis=0, keepdims=True))
        dval[...] += dot_nn(probs.astype(BF16), datt_st)
        dprobs = dot_nt(values, datt_st)
        dscore = (probs * (dprobs - jnp.sum(probs * dprobs, axis=0, keepdims=True))).astype(BF16)
        dkey[...] += dot_nn(dscore, query_st)
        dq_t = dot_nn(keys_t, dscore)
        picked = dq_t[:, :tokens]
        for head in range(1, heads):
            part = dq_t[:, head * tokens : (head + 1) * tokens]
            picked = jnp.where(row_mask(part.shape, head), part, picked)
        low = (picked * HEAD_SIZE**-0.5).astype(BF16)
        dproj[member, :, :part_width] = dot_nt(identity(tokens), low).astype(BF16)
        return carry

    lax.fori_loop(0, size, back, 0)
    for member in range(size):
        rows = slice(member * tokens, (member + 1) * tokens)
        dproj[member, :, part_width : 2 * part_width] = (dkey[rows] * HEAD_SIZE**-0.5).astype(BF16)
        dproj[member, :, 2 * part_width :] = dval[rows].astype(BF16)

    def partial_rows(member):
        return dot_nt(dproj[member], w_buf[:, : 3 * part_width])

    def send(step, carry):
        member = group.member(size - step)
        stage[member] = partial_rows(member).astype(BF16)
        group.give(stage, landing, rs_send, rs_recv, size - step)
        return carry

    lax.fori_loop(1, size + 1, send, 0)
    group.combine(stage, landing, rs_send, rs_recv)
    bg(2)
    grads = dproj[...].reshape(seq, -1)
    dbqkv_ref[...] = col_sum(grads.astype(F32))
    dbproj_ref[...] = col_sum(dba[...].reshape(seq, width).astype(F32))
    mixed = att_ref[...].reshape(seq, part_width)
    normed_rows, dba_rows = normed_ref.reshape(seq, width), dba.reshape(seq, width)

    def weights(index, carry):
        cols = pl.ds(pl.multiple_of(index * 128, 128), 128)
        dw_ref[cols, : 3 * part_width] = dot_tn(normed_rows[:, cols], grads).astype(BF16)
        dw_ref[cols, 3 * part_width :] = dot_tn(dba_rows[:, cols], mixed).astype(BF16)
        return carry

    lax.fori_loop(0, width // 128, weights, 0)
    group.spread_sent(dba, ag_send, ag_recv)
    bg(3)
    total = group.landed_sum(stage[me].astype(F32), stage, landing, rs_send, rs_recv)
    hidden = hidden_ref[...].astype(F32)
    normed, rstd = norm_parts(hidden)
    dmod_ref[0:1] = col_sum(total)
    dmod_ref[1:2] = col_sum(total * normed)
    gin = norm_back(total, normed, rstd, mod_ref[1:2]) + gmid_ref[...]
    gin_ref[...] = gin.astype(BF16)
    bg(4)


class Place:
    def __init__(self):
        self.section, self.dp = lax.axis_index("section"), lax.axis_index("dp")
        self.high, self.low = lax.axis_index("mh"), lax.axis_index("ml")
        self.n_dp, self.n_low = lax.axis_size("dp"), lax.axis_size("ml")
        self.total = 4 * self.n_dp * self.n_low
        self.me = ((self.section * self.n_dp + self.dp) * 2 + self.high) * self.n_low + self.low

    def unflatten(self, number):
        low = lax.rem(number, self.n_low)
        rest = lax.div(number, self.n_low)
        high, rest = lax.rem(rest, 2), lax.div(rest, 2)
        return lax.div(rest, self.n_dp), lax.rem(rest, self.n_dp), high, low

    def greet(self):
        barrier = pltpu.get_barrier_semaphore()
        others = []
        for sec in range(2):
            for step in range(self.n_low):
                if sec or step:
                    section = lax.rem(self.section + sec, 2)
                    others.append((section, self.dp, self.high, lax.rem(self.low + step, self.n_low)))
        for sec in range(2):
            others.append(self.plane(sec, 1 - self.high))
        for step in range(1, self.n_dp // 2):
            others.append((self.section, self.same_core(step), self.high, self.low))
        others.append(self.core_mate())
        for device in others:
            pl.semaphore_signal(barrier, inc=1, device_id=device, device_id_type=MESH)
        pl.semaphore_wait(barrier, len(others))

    def role(self, layer, number):
        same = (self.section == layer) if number < 2 else (self.section != layer)
        return same & ((self.high == layer) if number % 2 == 0 else (self.high != layer))

    def role_device(self, layer, number):
        section = layer if number < 2 else 1 - layer
        return self.plane(section, layer if number % 2 == 0 else 1 - layer)

    def greet_all(self):
        barrier = pltpu.get_barrier_semaphore()

        def body(step, carry):
            pl.semaphore_signal(
                barrier,
                inc=1,
                device_id=self.unflatten(lax.rem(self.me + step, self.total)),
                device_id_type=MESH,
            )
            return carry

        lax.fori_loop(1, self.total, body, 0)
        pl.semaphore_wait(barrier, self.total - 1)

    def copy(self, src, dst, send_sem, recv_sem, device):
        return pltpu.make_async_remote_copy(
            src_ref=src,
            dst_ref=dst,
            send_sem=send_sem,
            recv_sem=recv_sem,
            device_id=device,
            device_id_type=MESH,
        )

    def core_mate(self):
        return (self.section, self.dp + 1 - 2 * lax.rem(self.dp, 2), self.high, self.low)

    def same_core(self, step):
        return lax.rem(self.dp + 2 * step, self.n_dp)

    def plane(self, section, high):
        return (section, self.dp, high, self.low)

    def exchange(self, pick, landing, send_sem, recv_sem):
        landing[self.me] = pick((self.section, self.dp, self.high, self.low))[...]

        def copy(number):
            device = self.unflatten(number)
            return self.copy(
                pick(device), landing.at[self.me], send_sem.at[number], recv_sem.at[self.me], device
            )

        def start(step, carry):
            copy(lax.rem(self.me + step, self.total)).start()
            return carry

        def finish(step, carry):
            number = lax.rem(self.me + step, self.total)
            device = self.unflatten(number)
            self.copy(
                landing.at[number], landing.at[number], send_sem.at[number], recv_sem.at[number], device
            ).wait_recv()
            copy(number).wait_send()
            return carry

        lax.fori_loop(1, self.total, start, 0)
        return lambda: lax.fori_loop(1, self.total, finish, 0)


VM = pl.BlockSpec(memory_space=pltpu.VMEM)
ANY = pl.BlockSpec(memory_space=pltpu.HBM)
DMA = pltpu.SemaphoreType.DMA


class Handle:
    def __init__(self, shape, dtype):
        self.shape, self.dtype = shape, dtype
        self.array = None
        self.ref = None


class Task:
    inputs = ()
    outs = ()
    scratch = ()
    handles = ()


class Collect(Task):
    def __init__(self, item, tensor, layer, handle):
        self.tensor, self.layer, self.handle = tensor, layer, handle
        self.inputs = ((item, VM),)
        self.handles = (handle,)
        self.chunk = item.shape[1]
        self.scratch = (DMA((2,)), DMA, DMA)

    def run(self, phase, refs):
        (item,), _, (send, recv, own) = refs
        place = Place()
        source = item.at[self.tensor]
        rows = self.handle.ref.at[pl.ds(pl.multiple_of(place.dp * self.chunk, 16), self.chunk)]

        def to(number, role):
            return place.copy(
                source, rows, send.at[number], recv, place.role_device(self.layer, role)
            )

        targets = {0: (1,), 1: (2, 3), 2: (), 3: ()}
        for role in range(4):

            @pl.when(place.role(self.layer, role))
            def _():
                if phase == "a":
                    for number, target in enumerate(targets[role]):
                        to(number, target).start()
                    if role == 0:
                        pltpu.make_async_copy(source, rows, own).start()
                if phase == "b":
                    if role == 0:
                        pltpu.make_async_copy(source, rows, own).wait()
                    else:
                        place.copy(
                            rows, rows, send.at[0], recv, place.role_device(self.layer, 0)
                        ).wait_recv()
                if phase == "c":
                    for number, target in enumerate(targets[role]):
                        to(number, target).wait_send()


class Widen(Task):
    def __init__(self, handle):
        self.handle = handle
        self.handles = (handle,)
        chips = lax.axis_size("dp") // 2
        self.scratch = (DMA((chips,)),) * 4

    def rows(self, index):
        chunk = self.handle.shape[0] // lax.axis_size("dp")
        return self.handle.ref.at[pl.ds(pl.multiple_of(index * chunk, 16), chunk)]

    def run(self, phase, refs):
        _, _, (x_send, x_recv, c_send, c_recv) = refs
        place = Place()
        chips = place.n_dp // 2

        def across(step):
            return place.copy(
                self.rows(place.dp), self.rows(place.dp), x_send.at[step], x_recv.at[step],
                (place.section, place.same_core(step), place.high, place.low),
            )

        def landed(step):
            held = self.rows(place.same_core(chips - step))
            return place.copy(
                held, held, x_send.at[step], x_recv.at[step],
                (place.section, place.same_core(step), place.high, place.low),
            )

        def to_mate(step):
            held = self.rows(place.same_core(step))
            return place.copy(held, held, c_send.at[step], c_recv.at[step], place.core_mate())

        def from_mate(step):
            held = self.rows(lax.rem(place.core_mate()[1] + 2 * step, place.n_dp))
            return place.copy(held, held, c_send.at[step], c_recv.at[step], place.core_mate())

        if phase == "a":
            for step in range(1, chips):
                across(step).start()
            to_mate(0).start()
        if phase == "b":
            for step in range(1, chips):
                landed(step).wait_recv()
                to_mate(chips - step).start()
        if phase == "c":
            for step in range(chips):
                from_mate(step).wait_recv()
                to_mate(step).wait_send()
                if step:
                    across(step).wait_send()


class Narrow(Task):
    def __init__(self, grad):
        n_dp = lax.axis_size("dp")
        chips = n_dp // 2
        self.chunk = grad.shape[0] // n_dp
        block = (chips, self.chunk, grad.shape[1])
        self.inputs = ((grad, ANY),)
        self.outs = (((self.chunk, grad.shape[1]), BF16, VM),)
        self.scratch = (pltpu.VMEM(block, BF16),) * 3 + (DMA((chips,)),) * 5

    def run(self, phase, refs):
        (grad,), (out,), scratch = refs
        own, near, far, own_sem, c_send, c_recv, x_send, x_recv = scratch
        place = Place()
        chips = place.n_dp // 2

        def rows(index):
            return grad.at[pl.ds(pl.multiple_of(index * self.chunk, 16), self.chunk)]

        def to_mate(step):
            other = lax.rem(place.core_mate()[1] + 2 * step, place.n_dp)
            return place.copy(
                rows(other), near.at[step], c_send.at[step], c_recv.at[step], place.core_mate()
            )

        def load_own(step):
            return pltpu.make_async_copy(
                rows(place.same_core(step)), own.at[step], own_sem.at[step]
            )

        def across(step):
            return place.copy(
                own.at[step], far.at[step], x_send.at[step], x_recv.at[step],
                (place.section, place.same_core(step), place.high, place.low),
            )

        order = list(range(1, chips)) + [0]
        if phase == "a":
            for step in order:
                to_mate(step).start()
                load_own(step).start()
        if phase == "b":
            for step in order:
                load_own(step).wait()
                to_mate(step).wait_recv()
                own[step] = (own[step].astype(F32) + near[step].astype(F32)).astype(BF16)
                if step:
                    across(step).start()
        if phase == "c":
            total = own[0].astype(F32)
            for step in range(1, chips):
                across(step).wait_recv()
                total = total + far[step].astype(F32)
            out[...] = total.astype(BF16)
            for step in range(chips):
                to_mate(step).wait_send()
                if step:
                    across(step).wait_send()


class Settle(Task):
    def __init__(self, part, layer, held=None, into=None):
        self.layer = layer
        self.held = held
        self.into = into
        self.inputs = () if held else ((part, ANY),)
        self.outs = () if into else ((part.shape, F32, VM),)
        self.scratch = (
            pltpu.VMEM((2,) + part.shape, BF16), pltpu.VMEM(part.shape, BF16),
            DMA((2,)), DMA((3,)), DMA,
        )

    def run(self, phase, refs):
        ins, outs, (land, temp, send, recv, own_sem) = refs
        (out,) = self.into.refs[1] if self.into else outs
        part = self.held() if self.held else ins[0]
        place = Place()
        layer = self.layer

        def to(src, dst, s, r, role):
            return place.copy(src, dst, send.at[s], recv.at[r], place.role_device(layer, role))

        def direct(role):
            if role == 2:
                return to(part, temp, 0, 2, 0)
            return to(part, land.at[0], 0, 0, 0 if role == 1 else 1)

        def relay():
            return to(temp, land.at[1], 1, 1, 1)

        for role in range(4):

            @pl.when(place.role(layer, role))
            def _():
                if phase == "z" and role == 1:
                    direct(role).start()
                if phase == "a":
                    if role > 1:
                        direct(role).start()
                    if role == 0:
                        pltpu.make_async_copy(part, land.at[1], own_sem).start()
                if phase == "b":
                    if role == 0:
                        to(temp, temp, 0, 2, 0).wait_recv()
                        relay().start()
                    if role > 1:
                        direct(role).wait_send()
                if phase == "s":
                    if role == 0:
                        relay().wait_send()
                    if role == 1:
                        direct(role).wait_send()
                if phase == "c":
                    if role == 0:
                        pltpu.make_async_copy(part, land.at[1], own_sem).wait()
                    if role < 2:
                        to(land.at[0], land.at[0], 0, 0, role).wait_recv()
                    if role == 1:
                        to(land.at[1], land.at[1], 0, 1, 1).wait_recv()
                    if role < 2:
                        out[...] = land[0].astype(F32) + land[1].astype(F32)


class Deliver(Task):
    def __init__(self, rows, layer, into=None):
        self.layer = layer
        self.into = into
        self.inputs = ((rows, VM),)
        self.outs = () if into else (((2,) + rows.shape, rows.dtype, VM),)
        self.scratch = (pltpu.VMEM(rows.shape, rows.dtype), DMA((2,)), DMA((3,)))

    def run(self, phase, refs):
        (rows,), outs, (temp, send, recv) = refs
        (out,) = self.into.refs[1] if self.into else outs
        place = Place()
        layer = self.layer

        def to(src, dst, s, r, role):
            return place.copy(src, dst, send.at[s], recv.at[r], place.role_device(layer, role))

        def direct(role):
            if role == 2:
                return to(rows, temp, 0, 2, 0)
            return to(rows, out.at[1 - layer], 0, 0, 0 if role == 1 else 1)

        def relay():
            return to(temp, out.at[layer], 1, 1, 1)

        for role in range(4):

            @pl.when(place.role(layer, role))
            def _():
                if phase == "z" and role == 1:
                    direct(role).start()
                if phase == "a":
                    if role > 1:
                        direct(role).start()
                    if role == 0:
                        out[layer] = rows[...]
                if phase == "b" and role == 0:
                    to(temp, temp, 0, 2, 0).wait_recv()
                    relay().start()
                if phase == "c":
                    if role == 0:
                        relay().wait_send()
                    else:
                        direct(role).wait_send()
                    if role < 2:
                        to(out.at[1 - layer], out.at[1 - layer], 0, 0, role).wait_recv()
                    if role == 1:
                        to(out.at[layer], out.at[layer], 0, 1, 1).wait_recv()


class Tokens(Task):
    def __init__(self, rows):
        self.inputs = ((rows, VM),)
        self.outs = ((rows.shape[1:], rows.dtype, VM),)
        self.scratch = (DMA, DMA((2,)))

    def run(self, phase, refs):
        (rows,), (out,), (send, recv) = refs
        place = Place()
        half = rows.shape[1] // 2
        parts = (slice(0, half), slice(half, 2 * half))

        def copy(part, section):
            return place.copy(
                rows.at[1 - place.high, parts[part]], out.at[parts[part]], send, recv.at[part],
                place.plane(section, 1 - place.high),
            )

        @pl.when(place.section == place.high)
        def _():
            if phase == "a":
                copy(0, place.section).start()
                out[...] = rows[place.high]
            if phase == "c":
                copy(0, place.section).wait_send()

        @pl.when(place.section != place.high)
        def _():
            if phase == "a":
                copy(1, 1 - place.section).start()
            if phase == "c":
                copy(1, 1 - place.section).wait_send()
                copy(0, place.section).wait_recv()
                copy(1, place.section).wait_recv()


def launch(kernel, operands, outs, scratch, schedule, cid, name):
    tasks = []
    for point in schedule:
        for task, _ in point:
            if task not in tasks:
                tasks.append(task)
    operands, outs, scratch = list(operands), list(outs), list(scratch)
    n_in, n_out, n_scratch = len(operands), len(outs), len(scratch)
    spans = []
    for task in tasks:
        spans.append((len(operands), len(outs), len(scratch)))
        operands += task.inputs
        outs += task.outs
        scratch += task.scratch
    handles = []
    for task in tasks:
        for handle in task.handles:
            if handle not in handles:
                handles.append(handle)
    aliases = {}
    first_handle = len(outs)
    for handle in handles:
        if handle.array is not None:
            aliases[len(operands)] = len(outs)
            operands.append((handle.array, ANY))
        outs.append((handle.shape, handle.dtype, ANY))

    def body(*refs):
        ins = refs[: len(operands)]
        results = refs[len(operands) : len(operands) + len(outs)]
        rest = refs[len(operands) + len(outs) :]
        for number, handle in enumerate(handles):
            handle.ref = results[first_handle + number]
        views = []
        for task, (a, b, c) in zip(tasks, spans):
            views.append(
                (
                    ins[a : a + len(task.inputs)],
                    results[b : b + len(task.outs)],
                    rest[c : c + len(task.scratch)],
                )
            )
            task.refs = views[-1]

        def bg(point):
            for task, phase in schedule[point]:
                task.run(phase, task.refs)

        kernel(bg, *ins[:n_in], *results[:n_out], *rest[:n_scratch])

    done = pl.pallas_call(
        body,
        out_shape=tuple(jax.ShapeDtypeStruct(shape, dtype) for shape, dtype, _ in outs),
        in_specs=[spec for _, spec in operands],
        out_specs=tuple(spec for _, _, spec in outs),
        scratch_shapes=scratch,
        input_output_aliases=aliases,
        compiler_params=pltpu.CompilerParams(
            collective_id=cid, has_side_effects=True, vmem_limit_bytes=VMEM_LIMIT
        ),
        name=name,
    )(*[array for array, _ in operands])
    for number, handle in enumerate(handles):
        handle.array = done[first_handle + number]
        handle.ref = None
    for task, (_, b, _) in zip(tasks, spans):
        task.results = done[b : b + len(task.outs)]
    return done[:n_out]


def group_size():
    return lax.axis_size("section") * lax.axis_size("ml")


def comm_scratch(tokens, width):
    size = group_size()
    return [pltpu.VMEM((size, tokens, width), BF16)] * 2, [DMA((max(size, 6),))] * 4


def att_fwd(hidden, mod, bias, bproj, w, schedule, cid):
    tokens, width = hidden.shape
    size = group_size()
    part_width = width // size
    bufs, sems = comm_scratch(tokens, width)
    return launch(
        att_fwd_kernel,
        [(hidden, VM), (mod, VM), (bias, VM), (bproj, VM), (w.array, ANY)],
        [
            ((tokens, width), F32, VM),
            ((size, tokens, width), BF16, VM),
            ((3, size, tokens, part_width), BF16, VM),
            ((size, tokens, part_width), BF16, VM),
            ((tokens, width), F32, VM),
        ],
        [pltpu.VMEM(w.shape, BF16), pltpu.VMEM((width, part_width), BF16)]
        + bufs
        + [DMA((1,))]
        + sems,
        schedule,
        cid,
        "att_fwd",
    )


def mlp_fwd(middle, mod, b1, b2, w1, w2, schedule, cid):
    tokens, width = middle.shape
    size = group_size()
    units = w1.shape[1]
    bufs, sems = comm_scratch(tokens, width)
    return launch(
        mlp_fwd_kernel,
        [(middle, VM), (mod, VM), (b1, VM), (b2, VM), (w1.array, ANY), (w2.array, ANY)],
        [
            ((tokens, width), BF16, VM),
            ((size, tokens, width), BF16, VM),
            ((size, tokens, units), F32, VM),
            ((size, tokens, units), BF16, VM),
            ((tokens, width), F32, VM),
        ],
        [pltpu.VMEM(w1.shape, BF16)] * 2 + bufs + [DMA((2,))] + sems,
        schedule,
        cid,
        "mlp_fwd",
    )


def mlp_bwd(grad, middle, mod, branch, normed, pre, gelu, w1, w2, schedule, cid):
    tokens, width = middle.shape
    size = group_size()
    units = w1.shape[1]
    bufs, sems = comm_scratch(tokens, width)
    ins = (grad, middle, mod, branch, normed, pre, gelu)
    return launch(
        mlp_bwd_kernel,
        [(array, VM) for array in ins] + [(w1.array, ANY), (w2.array, ANY)],
        [
            ((tokens, width), F32, VM),
            (w1.shape, BF16, VM),
            (w2.shape, BF16, VM),
            ((1, units), F32, VM),
            ((1, width), F32, VM),
            ((3, width), F32, VM),
        ],
        [pltpu.VMEM(w1.shape, BF16)] * 2
        + [pltpu.VMEM((size, tokens, width), BF16), pltpu.VMEM((size, tokens, units), BF16)]
        + bufs
        + [DMA((2,))]
        + sems,
        schedule,
        cid,
        "mlp_bwd",
    )


def att_bwd(gmid, hidden, mod, branch, normed, proj, att, w, schedule, cid):
    tokens, width = gmid.shape
    size = group_size()
    part_width = width // size
    bufs, sems = comm_scratch(tokens, width)
    seq = size * tokens
    ins = (gmid, hidden, mod, branch, normed, proj, att)
    return launch(
        att_bwd_kernel,
        [(array, VM) for array in ins] + [(w.array, ANY)],
        [
            ((tokens, width), BF16, VM),
            (w.shape, BF16, VM),
            ((1, 3 * part_width), F32, VM),
            ((1, width), F32, VM),
            ((3, width), F32, VM),
        ],
        [
            pltpu.VMEM(w.shape, BF16),
            pltpu.VMEM((width, part_width), BF16),
            pltpu.VMEM((size, tokens, width), BF16),
            pltpu.VMEM((size, tokens, 3 * part_width), BF16),
            pltpu.VMEM((seq, part_width), F32),
            pltpu.VMEM((seq, part_width), F32),
        ]
        + bufs
        + [DMA((1,))]
        + sems,
        schedule,
        cid,
        "att_bwd",
    )


def prologue_kernel(
    bg,
    cond_ref, wada_ref, bada_ref, bias_ref,
    modul_ref, act_ref, bias_out,
    cond_land, share, land, cond_send, cond_recv, mod_send, mod_recv, b_send, b_recv,
):
    place = Place()
    section, dp, high = place.section, place.dp, place.high
    place.greet_all()

    def spread(step):
        other = lax.rem(dp + step, place.n_dp)
        return place.copy(
            cond_ref.at[other], cond_land.at[dp], cond_send.at[step], cond_recv.at[dp],
            (section, other, high, place.low),
        )

    def spread_wait(step):
        other = lax.rem(dp + step, place.n_dp)
        return place.copy(
            cond_land.at[other], cond_land.at[other], cond_send.at[step], cond_recv.at[other],
            (section, other, high, place.low),
        )

    cond_land[dp] = cond_ref[dp]
    for step in range(1, place.n_dp):
        spread(step).start()

    def bias_copy(target):
        return place.copy(
            bias_ref, bias_out.at[section], b_send.at[target], b_recv.at[section],
            place.plane(high, target),
        )

    here = section == high
    for target in range(2):

        @pl.when(jnp.logical_not(here & (high == target)))
        def _():
            bias_copy(target).start()

    @pl.when(here)
    def _():
        bias_out[section] = bias_ref[...]

    bg(0)
    for step in range(1, place.n_dp):
        spread_wait(step).wait_recv()
    parts = [cond_land[index] for index in range(place.n_dp)]
    act = jax.nn.silu(jnp.concatenate(parts, axis=0)).astype(BF16)
    act_ref[...] = act
    bias = jnp.where(dp == 0, bada_ref[...], 0.0)
    product = dot_nn(act, wada_ref[...])
    for row in range(2 * place.n_dp):
        share[row] = product[row : row + 1] + bias
    finish = place.exchange(
        lambda device: share.at[device[1] * 2 + device[2]], land, mod_send, mod_recv
    )
    bg(1)
    bg(2)
    finish()
    for layer in range(2):
        for part in range(2 * place.n_low):
            total = land[layer * place.n_dp * 2 * place.n_low + part]
            for index in range(1, place.n_dp):
                total = total + land[(layer * place.n_dp + index) * 2 * place.n_low + part]
            modul_ref[layer * 2 * place.n_low + part] = total
    bg(3)
    for step in range(1, place.n_dp):
        spread(step).wait_send()
    for target in range(2):

        @pl.when(jnp.logical_not(here & (high == target)))
        def _():
            bias_copy(target).wait_send()

        @pl.when(jnp.logical_not(here & (section == target)))
        def _():
            place.copy(
                bias_out.at[target], bias_out.at[target], b_send.at[0], b_recv.at[target],
                place.plane(section, 1 - high),
            ).wait_recv()

    bg(4)


def prologue(cond, wada, bada, bias, schedule, cid):
    n_dp, _, chunk = cond.shape
    n_mp = 2 * lax.axis_size("ml")
    total = 2 * n_dp * n_mp
    share = wada.shape[1]
    return launch(
        prologue_kernel,
        [(cond, VM), (wada, VM), (bada, VM), (bias, VM)],
        [
            ((2 * n_mp, 1, share), F32, VM),
            ((2 * n_dp, chunk), BF16, VM),
            ((2,) + bias.shape, F32, VM),
        ],
        [
            pltpu.VMEM((n_dp, 2, chunk), F32),
            pltpu.VMEM((2 * n_dp, 1, share), F32),
            pltpu.VMEM((total, 1, share), F32),
            DMA((n_dp,)),
            DMA((n_dp,)),
            DMA((total,)),
            DMA((total,)),
            DMA((2,)),
            DMA((2,)),
        ],
        schedule,
        cid,
        "prologue",
    )


def epilogue_kernel(
    bg,
    dmod_ref, act_ref, wada_ref, dbias_ref,
    gada_ref, gbada_ref, gact_ref, gbias_ref,
    mod_land, act_stage, act_land, bias_land, bias_stage, bias_final,
    mod_send, mod_recv, act_send, act_recv, d_send, d_recv, b_send, b_recv,
):
    place = Place()
    section, dp, high = place.section, place.dp, place.high
    place.greet_all()
    finish_mod = place.exchange(
        lambda device: dmod_ref.at[(device[0] * 2 + device[2]) * place.n_low + device[3]],
        mod_land, mod_send, mod_recv,
    )

    def spread(step):
        other = lax.rem(dp + step, place.n_dp)
        return place.copy(
            dbias_ref, bias_land.at[dp], d_send.at[step], d_recv.at[dp],
            (section, other, high, place.low),
        )

    for step in range(1, place.n_dp):
        spread(step).start()
    bg(0)
    finish_mod()
    parts = 2 * place.n_low
    latents = []
    for index in range(place.n_dp):
        for micro in range(2):
            total = 0.0
            for sec in range(2):
                for low in range(place.n_low):
                    number = ((sec * place.n_dp + index) * 2 + micro) * place.n_low + low
                    total = total + mod_land[number]
            latents.append(total)
    dmod = jnp.concatenate(latents, axis=0).astype(BF16)
    back = dot_nt(dmod, wada_ref[...])
    for index in range(place.n_dp):
        act_stage[index] = back[2 * index : 2 * index + 2]
    finish_act = place.exchange(lambda device: act_stage.at[device[1]], act_land, act_send, act_recv)
    bias_sum = dbias_ref[...]
    for step in range(1, place.n_dp):
        other = lax.rem(dp + step, place.n_dp)
        place.copy(
            bias_land.at[other], bias_land.at[other], d_send.at[step], d_recv.at[other],
            (section, other, high, place.low),
        ).wait_recv()
        bias_sum = bias_sum + bias_land[other]
    bias_stage[...] = bias_sum

    def settle(layer):
        return place.copy(
            bias_stage.at[layer], bias_final.at[high], b_send.at[layer], b_recv.at[high],
            place.plane(layer, section),
        )

    for layer in range(2):
        here = (section == layer) & (high == section)

        @pl.when(here)
        def _():
            bias_final[high] = bias_stage[layer]

        @pl.when(jnp.logical_not(here))
        def _():
            settle(layer).start()

    bg(1)
    gbada_ref[...] = col_sum(dmod.astype(F32))
    gada_ref[...] = dot_tn(act_ref[...], dmod)
    bg(2)
    finish_act()
    for index in range(place.n_dp):
        total = 0.0
        for sec in range(2):
            for part in range(parts):
                total = total + act_land[(sec * place.n_dp + index) * parts + part]
        gact_ref[index] = total
    bg(3)
    for half in range(2):
        here = (section == high) & (high == half)

        @pl.when(jnp.logical_not(here))
        def _():
            place.copy(
                bias_final.at[half], bias_final.at[half], b_send.at[0], b_recv.at[half],
                place.plane(high, half),
            ).wait_recv()

    gbias_ref[...] = bias_final[0] + bias_final[1]
    for layer in range(2):

        @pl.when(jnp.logical_not((section == layer) & (high == section)))
        def _():
            settle(layer).wait_send()

    for step in range(1, place.n_dp):
        spread(step).wait_send()
    bg(4)


def epilogue(dmod, act, wada, dbias, schedule, cid):
    n_dp, n_mp = lax.axis_size("dp"), 2 * lax.axis_size("ml")
    total = 2 * n_dp * n_mp
    chunk, share = wada.shape
    row = dbias.shape[1:]
    return launch(
        epilogue_kernel,
        [(dmod, VM), (act, VM), (wada, VM), (dbias, VM)],
        [
            ((chunk, share), F32, VM),
            ((1, share), F32, VM),
            ((n_dp, 2, chunk), F32, VM),
            (row, F32, VM),
        ],
        [
            pltpu.VMEM((total, 1, share), F32),
            pltpu.VMEM((n_dp, 2, chunk), F32),
            pltpu.VMEM((total, 2, chunk), F32),
            pltpu.VMEM((n_dp,) + dbias.shape, F32),
            pltpu.VMEM(dbias.shape, F32),
            pltpu.VMEM((2,) + row, F32),
            DMA((total,)),
            DMA((total,)),
            DMA((total,)),
            DMA((total,)),
            DMA((n_dp,)),
            DMA((n_dp,)),
            DMA((2,)),
            DMA((2,)),
        ],
        schedule,
        cid,
        "epilogue",
    )


def per_device(
    latents_in, condition, cotangent,
    modulation_weight, modulation_bias, query_key_value_weight, query_value_bias,
    output_proj_weight, output_proj_bias, first_dense_weight, first_dense_bias,
    second_dense_weight, second_dense_bias,
):
    dp = lax.axis_index("dp")
    n_dp, n_low = lax.axis_size("dp"), lax.axis_size("ml")
    n_mp = 2 * n_low
    width = latents_in.shape[-1]
    rows = modulation_weight.shape[1]
    cols = modulation_weight.shape[2]
    part_width = query_key_value_weight.shape[3]
    units = first_dense_weight.shape[2]

    item = jnp.stack(
        [
            jnp.concatenate(
                [query_key_value_weight[0].reshape(rows, -1), output_proj_weight[0].T], axis=1
            ),
            first_dense_weight[0],
            second_dense_weight[0].T,
        ]
    )
    cond = condition[:, 0].astype(F32)
    packed = jnp.concatenate(
        [
            query_value_bias[0, 0], query_value_bias[0, 1], first_dense_bias[0],
            output_proj_bias[0], second_dense_bias[0],
        ]
    ).astype(F32)[None]
    w = [[Handle((width, units), BF16) for _ in range(3)] for _ in range(2)]
    collect = [[Collect(item, t, l, w[l][t]) for t in range(3)] for l in range(2)]
    widen = [[Widen(w[l][t]) for t in range(3)] for l in range(2)]
    tokens_in = Tokens(latents_in[:, 0])
    tokens_cot = Tokens(cotangent[:, 0])

    def plan(*points):
        out = []
        for point in points:
            out.append([(task, phase) for task, phases in point for phase in phases])
        return out

    c, x = collect, widen
    modul, act_rows, biases = prologue(
        cond.reshape(2, n_dp, rows).transpose(1, 0, 2),
        modulation_weight[0],
        modulation_bias.astype(F32),
        packed,
        plan(
            [(tokens_in, "a"), (c[0][0], "a"), (c[1][0], "a")],
            [(c[0][0], "c"), (c[1][0], "c"), (c[0][1], "a"), (c[1][1], "a")]
            + [(c[0][0], "b"), (x[0][0], "a"), (c[1][0], "b")],
            [(c[0][1], "c"), (c[1][1], "c"), (c[0][2], "a"), (c[1][2], "a")]
            + [(x[0][0], "b"), (c[0][1], "b"), (x[0][1], "a"), (c[1][1], "b")],
            [],
            [(c[0][2], "c"), (c[1][2], "c"), (c[0][2], "b"), (c[1][2], "b"), (x[0][1], "b")]
            + [(tokens_in, "c"), (x[0][0], "c"), (x[0][1], "c")],
        ),
        1,
    )
    modul = modul.reshape(2, 6, width)
    bounds = [0, part_width, 2 * part_width, 2 * part_width + units, 2 * part_width + units + width]
    bqkv = jnp.concatenate(
        [
            biases[..., : bounds[1]], jnp.zeros((2, 1, part_width), F32),
            biases[..., bounds[1] : bounds[2]],
        ],
        axis=-1,
    )
    b1 = biases[..., bounds[2] : bounds[3]]
    bproj = biases[..., bounds[3] : bounds[4]]
    b2 = biases[..., bounds[4] :]

    hidden = [tokens_in.results[0]]
    att_plan = [
        plan(
            [(x[0][2], "a")],
            [],
            [],
            [(x[0][2], "b")],
            [(x[0][2], "c")],
        ),
        plan(
            [(x[1][1], "a"), (x[1][2], "a"), (tokens_cot, "a")],
            [],
            [],
            [(x[1][1], "b"), (x[1][2], "b")],
            [(x[1][1], "c"), (x[1][2], "c"), (tokens_cot, "c")],
        ),
    ]
    saved = []
    for layer in range(2):
        middle, normed, proj, att, branch = att_fwd(
            hidden[layer], modul[layer], bqkv[layer], bproj[layer], w[layer][0], att_plan[layer],
            2 + 2 * layer,
        )
        if layer == 0:
            mlp_plan = plan(
                [(x[1][0], "a")],
                [],
                [],
                [(x[1][0], "b")],
                [(x[1][0], "c")],
            )
        else:
            acts_first = Deliver(hidden[1], 0)
            mlp_plan = plan([], [], [], [], [])
        out, normed2, pre, gelu, branch2 = mlp_fwd(
            middle, modul[layer], b1[layer], b2[layer], w[layer][1], w[layer][2], mlp_plan,
            3 + 2 * layer,
        )
        saved.append((middle, normed, proj, att, branch, normed2, pre, gelu, branch2))
        hidden.append(out)

    grad = tokens_cot.results[0]
    narrow = [[None] * 3 for _ in range(2)]
    settle = [[None] * 3 for _ in range(2)]
    d_bias, d_mod, gins = {}, {}, {}
    acts_second = Deliver(hidden[2], 1, acts_first)
    for layer in (1, 0):
        middle, normed, proj, att, branch, normed2, pre, gelu, branch2 = saved[layer]
        if layer == 1:
            mlp_plan = plan(
                [(acts_first, "az"), (acts_second, "az")],
                [],
                [(acts_first, "b"), (acts_second, "b")],
                [],
                [(acts_first, "c"), (acts_second, "c")],
            )
        else:
            third = narrow[1][0]
            mlp_plan = plan([(third, "a")], [(third, "b")], [], [], [(third, "c")])
        gmid, dw1, dw2, db1, db2, dmod2 = mlp_bwd(
            grad, middle, modul[layer], branch2, normed2, pre, gelu, w[layer][1], w[layer][2],
            mlp_plan, 6 + 2 * (1 - layer),
        )
        narrow[layer][1], narrow[layer][2] = Narrow(dw1), Narrow(dw2)
        one, two = narrow[layer][1], narrow[layer][2]
        if layer == 0:
            settle[1][0] = Settle(narrow[1][0].results[0], 1)
            gin_second = Deliver(gins[1], 1)
        att_plan = plan(
            [(two, "a"), (one, "a")], [(two, "b"), (one, "b")], [], [], [(two, "c"), (one, "c")]
        )
        gin, dw, dbqkv, dbproj, dmod1 = att_bwd(
            gmid, hidden[layer], modul[layer], branch, normed, proj, att, w[layer][0],
            att_plan, 7 + 2 * (1 - layer),
        )
        for tensor in (1, 2):
            into = None if layer else settle[1][tensor]
            settle[layer][tensor] = Settle(narrow[layer][tensor].results[0], layer, into=into)
        narrow[layer][0] = Narrow(dw)
        gins[layer] = grad = gin
        d_bias[layer] = jnp.concatenate(
            [dbqkv[:, :part_width], dbqkv[:, 2 * part_width :], db1, dbproj, db2], axis=1
        )
        d_mod[layer] = jnp.concatenate([dmod1.reshape(-1), dmod2.reshape(-1)])

    last = narrow[0][0]
    final = Settle(jax.ShapeDtypeStruct((rows, units), BF16), 0, held=lambda: last.refs[1][0], into=settle[1][0])
    settle[0][0] = final
    gin_first = Deliver(gins[0], 0, gin_second)
    dmod = jnp.stack([d_mod[0], d_mod[1]]).reshape(2 * n_mp, 1, cols)
    g_wada, g_bada, g_act, g_bias = epilogue(
        dmod,
        act_rows,
        modulation_weight[0],
        jnp.stack([d_bias[0], d_bias[1]]),
        plan(
            [(gin_first, "az"), (gin_second, "az"), (last, "a"), (gin_first, "b"), (gin_second, "b")]
            + [(settle[0][2], "az"), (settle[1][2], "az")],
            [(settle[0][2], "b"), (settle[1][2], "b"), (settle[0][1], "a"), (settle[1][1], "a"), (last, "b")]
            + [(settle[0][2], "s"), (settle[1][2], "s"), (settle[0][1], "bz"), (settle[1][1], "bz")],
            [(last, "c"), (settle[1][0], "a"), (final, "a"), (settle[0][1], "s"), (settle[1][1], "s")]
            + [(settle[1][0], "bz"), (final, "bz")],
            [(settle[0][2], "c"), (settle[1][2], "c"), (settle[0][1], "c"), (settle[1][1], "c")],
            [(gin_first, "c"), (gin_second, "c"), (settle[1][0], "s"), (final, "s")]
            + [(settle[1][0], "c"), (final, "c")],
        ),
        10,
    )
    g_act = g_act.transpose(1, 0, 2).reshape(2, width)
    g_att, g_one, g_two = [settle[1][t].results[0] for t in range(3)]
    g_qkv = g_att[:, : 3 * part_width].reshape(rows, 3, part_width)
    g_proj = g_att[:, 3 * part_width :].T

    def dp_part(vec):
        size = vec.shape[-1] // n_dp
        return lax.dynamic_slice_in_dim(vec, dp * size, size, vec.ndim - 1)

    g_bias = g_bias[0]
    g_bqv = dp_part(g_bias[: bounds[2]].reshape(2, part_width))
    g_b1 = dp_part(g_bias[bounds[2] : bounds[3]])
    g_bproj = dp_part(g_bias[bounds[3] : bounds[4]])
    g_b2 = dp_part(g_bias[bounds[4] :])
    g_bada = dp_part(g_bada[0])
    _, silu_back = jax.vjp(jax.nn.silu, cond)
    g_cond = silu_back(g_act)[0][:, None]
    acts_out = acts_first.results[0][None, :, None]
    grad_input = gin_second.results[0].astype(F32)[None, :, None]
    return (
        acts_out,
        grad_input,
        g_cond,
        g_wada[None],
        g_bada[None],
        g_qkv[None],
        g_bqv[None],
        g_proj[None],
        g_bproj[None],
        g_one[None],
        g_b1[None],
        g_two.T[None],
        g_b2[None],
    )


def solution(mesh):
    sizes = mesh.shape
    grid = mesh.devices.reshape(sizes["section"], sizes["dp"], 2, sizes["mp"] // 2)
    fine = Mesh(grid, ("section", "dp", "mh", "ml"))
    mp = ("mh", "ml")
    in_specs = (
        P(None, "dp", mp, None),
        P(None, "dp", None),
        P(None, "dp", mp, None),
        P("section", "dp", mp),
        P("section", mp),
        P("section", "dp", None, mp),
        P("section", None, mp),
        P("section", mp, "dp"),
        P("section", None),
        P("section", "dp", mp),
        P("section", mp),
        P("section", mp, "dp"),
        P("section", None),
    )
    mpdp = ("mh", "ml", "dp")
    out_specs = (
        P("section", None, "dp", mp, None),
        P("section", None, "dp", mp, None),
        P(None, "dp", None),
        P("section", "dp", mp),
        P("section", mpdp),
        P("section", "dp", None, mp),
        P("section", None, mpdp),
        P("section", mp, "dp"),
        P("section", "dp"),
        P("section", "dp", mp),
        P("section", mpdp),
        P("section", mp, "dp"),
        P("section", "dp"),
    )
    return jax.shard_map(
        per_device, mesh=fine, in_specs=in_specs, out_specs=out_specs, check_vma=False
    )
```

```python
import jax
import jax.numpy as jnp
from jax import lax
from jax.experimental import pallas as pl
from jax.experimental.pallas import tpu as pltpu
from jax.sharding import Mesh
from jax.sharding import PartitionSpec as P

HEAD_SIZE = 72
EPS = 1e-06
MESH = pl.DeviceIdType.MESH
BF16 = jnp.bfloat16
F32 = jnp.float32
GELU_C = 0.7978845608028654
GELU_A = 0.044715
NT = (((1,), (1,)), ((), ()))
TN = (((0,), (0,)), ((), ()))
VMEM_LIMIT = 50 * 1024 * 1024


def dot_nn(a, b):
    return jnp.dot(a, b, preferred_element_type=F32)


def dot_nt(a, b):
    return lax.dot_general(a, b, NT, preferred_element_type=F32)


def dot_tn(a, b):
    return lax.dot_general(a, b, TN, preferred_element_type=F32)


def norm_parts(values):
    center = values - jnp.mean(values, axis=-1, keepdims=True)
    spread = jnp.mean(center * center, axis=-1, keepdims=True)
    rstd = lax.rsqrt(spread + EPS)
    return center * rstd, rstd


def norm_back(grad, normed, rstd, scale):
    dn = grad * (1.0 + scale)
    first = jnp.mean(dn, axis=-1, keepdims=True)
    second = jnp.mean(dn * normed, axis=-1, keepdims=True)
    return (dn - first - normed * second) * rstd


def col_sum(values):
    return jnp.sum(values, axis=0, keepdims=True)


class Group:
    def __init__(self, tokens):
        self.low = lax.axis_size("ml")
        self.size = lax.axis_size("section") * self.low
        self.me = lax.axis_index("section") * self.low + lax.axis_index("ml")
        self.square = self.size == 4
        self.half = (slice(0, tokens // 2), slice(tokens // 2, tokens))

    def device(self, member):
        return (
            lax.div(member, self.low),
            lax.axis_index("dp"),
            lax.axis_index("mh"),
            lax.rem(member, self.low),
        )

    def member(self, step):
        if not self.square:
            return lax.rem(self.me + step, self.size)
        section = lax.rem(lax.axis_index("section") + lax.rem(step, 2), 2)
        low = lax.rem(lax.axis_index("ml") + lax.div(step, 2), 2)
        return section * 2 + low

    def copy(self, src, dst, send_sem, recv_sem, member):
        return pltpu.make_async_remote_copy(
            src_ref=src,
            dst_ref=dst,
            send_sem=send_sem,
            recv_sem=recv_sem,
            device_id=self.device(member),
            device_id_type=MESH,
        )

    def first_copies(self, buf, send_sem, recv_sem):
        steps = (1, 2) if self.square else range(1, self.size)
        mine = buf.at[self.me]
        return [
            self.copy(mine, mine, send_sem.at[step], recv_sem.at[self.me], self.member(step))
            for step in steps
        ]

    def relay_copy(self, buf, send_sem, recv_sem, step):
        rows = buf.at[self.member(step), self.half[step - 1]]
        return self.copy(
            rows, rows, send_sem.at[2 + step], recv_sem.at[3 + step], self.member(3 - step)
        )

    def spread(self, buf, send_sem, recv_sem):
        for copy in self.first_copies(buf, send_sem, recv_sem):
            copy.start()

    def arrive(self, buf, send_sem, recv_sem, step):
        def landed(rows, sem):
            self.copy(rows, rows, send_sem.at[1], sem, self.member(1)).wait_recv()

        if not self.square:

            @pl.when(step > 0)
            def _():
                landed(buf.at[self.member(step)], recv_sem.at[self.member(step)])

            return

        @pl.when(step == 1)
        def _():
            for near in (1, 2):
                landed(buf.at[self.member(near)], recv_sem.at[self.member(near)])
                self.relay_copy(buf, send_sem, recv_sem, near).start()

        @pl.when(step == 3)
        def _():
            for near in (1, 2):
                landed(buf.at[self.member(3), self.half[near - 1]], recv_sem.at[3 + near])

    def spread_sent(self, buf, send_sem, recv_sem):
        for copy in self.first_copies(buf, send_sem, recv_sem):
            copy.wait_send()
        if self.square:
            for step in (1, 2):
                self.relay_copy(buf, send_sem, recv_sem, step).wait_send()

    def straight(self, stage, landing, send_sem, recv_sem, step):
        rows = self.half[step - 1]
        return self.copy(
            stage.at[self.member(step), rows], landing.at[step - 1, rows],
            send_sem.at[step - 1], recv_sem.at[step - 1], self.member(step),
        )

    def corner(self, stage, landing, send_sem, recv_sem, step):
        rows = self.half[step - 1]
        return self.copy(
            stage.at[self.member(3), rows], landing.at[2, rows],
            send_sem.at[1 + step], recv_sem.at[1 + step], self.member(step),
        )

    def summed(self, landing, send_sem, recv_sem, step):
        rows = self.half[2 - step]
        return self.copy(
            landing.at[3, rows], landing.at[step - 1, rows],
            send_sem.at[3 + step], recv_sem.at[3 + step], self.member(step),
        )

    def reduce_copy(self, stage, landing, send_sem, recv_sem, member):
        return self.copy(
            stage.at[member], landing.at[self.me], send_sem.at[member], recv_sem.at[self.me], member
        )

    def give(self, stage, landing, send_sem, recv_sem, step):
        args = (stage, landing, send_sem, recv_sem)
        if not self.square:

            @pl.when(step > 0)
            def _():
                self.reduce_copy(*args, self.member(step)).start()

            return
        for near in (1, 2):

            @pl.when(step == near)
            def _():
                self.straight(*args, near).start()

        @pl.when(step == 3)
        def _():
            for near in (1, 2):
                self.corner(*args, near).start()

    def combine(self, stage, landing, send_sem, recv_sem):
        if not self.square:
            return
        for step in (1, 2):
            rows = self.half[2 - step]
            self.copy(
                landing.at[2, rows], landing.at[2, rows], send_sem.at[0], recv_sem.at[4 - step],
                self.member(1),
            ).wait_recv()
            total = stage[self.member(step), rows].astype(F32) + landing[2, rows].astype(F32)
            landing[3, rows] = total.astype(BF16)
            self.summed(landing, send_sem, recv_sem, step).start()

    def landed_sum(self, own, stage, landing, send_sem, recv_sem):
        args = (stage, landing, send_sem, recv_sem)
        total = own

        def landed(rows, sem):
            self.copy(rows, rows, send_sem.at[0], sem, self.member(1)).wait_recv()

        if self.square:
            for step in (1, 2):
                first, second = self.half[step - 1], self.half[2 - step]
                landed(landing.at[step - 1, first], recv_sem.at[step - 1])
                landed(landing.at[step - 1, second], recv_sem.at[3 + step])
                total = total + landing[step - 1].astype(F32)
            for step in (1, 2):
                self.straight(*args, step).wait_send()
                self.corner(*args, step).wait_send()
                self.summed(landing, send_sem, recv_sem, step).wait_send()
            return total
        for step in range(1, self.size):
            member = self.member(step)
            landed(landing.at[member], recv_sem.at[member])
            total = total + landing[member].astype(F32)
        for step in range(1, self.size):
            self.reduce_copy(*args, self.member(step)).wait_send()
        return total


def load(src, dst, sem):
    copy = pltpu.make_async_copy(src, dst, sem)
    copy.start()
    return [copy]


def lane_mask(shape, head):
    lanes = lax.broadcasted_iota(jnp.int32, shape, len(shape) - 1)
    return (lanes >= head * HEAD_SIZE) & (lanes < (head + 1) * HEAD_SIZE)


def row_mask(shape, head):
    rows = lax.broadcasted_iota(jnp.int32, shape, 0)
    return (rows >= head * HEAD_SIZE) & (rows < (head + 1) * HEAD_SIZE)


def stack_heads(block):
    heads = block.shape[-1] // HEAD_SIZE
    zero = jnp.zeros_like(block)
    return jnp.concatenate(
        [jnp.where(lane_mask(block.shape, head), block, zero) for head in range(heads)], axis=0
    )


def identity(size):
    rows = lax.broadcasted_iota(jnp.int32, (size, size), 0)
    cols = lax.broadcasted_iota(jnp.int32, (size, size), 1)
    return jnp.where(rows == cols, 1.0, 0.0).astype(BF16)


def att_fwd_kernel(
    bg,
    hidden_ref, mod_ref, bias_ref, bproj_ref, w_ref,
    middle_ref, normed_ref, proj_ref, att_ref, branch_ref,
    w_buf, wo_buf, stage, landing, w_sem, ag_send, ag_recv, rs_send, rs_recv,
):
    tokens, width = hidden_ref.shape
    group = Group(tokens)
    me, size = group.me, group.size
    part_width = att_ref.shape[-1]
    heads = part_width // HEAD_SIZE
    loads = load(w_ref, w_buf, w_sem.at[0])
    hidden = hidden_ref[...].astype(F32)
    normed, _ = norm_parts(hidden)
    normed_ref[me] = (normed * (1.0 + mod_ref[1:2]) + mod_ref[0:1]).astype(BF16)
    Place().greet()
    group.spread(normed_ref, ag_send, ag_recv)
    bg(0)
    for copy in loads:
        copy.wait()

    def project(step, carry):
        member = group.member(step)
        group.arrive(normed_ref, ag_send, ag_recv, step)
        out = dot_nn(normed_ref[member], w_buf[:, : 3 * part_width]) + bias_ref[...]
        for part in range(3):
            cols = slice(part * part_width, (part + 1) * part_width)
            proj_ref[part, member] = out[:, cols].astype(BF16)
        return carry

    wo_buf[...] = w_buf[:, 3 * part_width :]
    lax.fori_loop(0, size, project, 0)
    bg(1)
    seq = size * tokens
    keys = proj_ref[1].reshape(seq, -1)
    values = proj_ref[2].reshape(seq, -1)

    def attend(member):
        stacked = stack_heads(proj_ref[0, member])
        powered = jnp.exp(dot_nt(stacked, keys) * HEAD_SIZE**-0.5)
        probs = powered * (1.0 / jnp.sum(powered, axis=-1, keepdims=True))
        mixed = dot_nn(probs.astype(BF16), values)
        out = mixed[:tokens]
        for head in range(1, heads):
            part = mixed[head * tokens : (head + 1) * tokens]
            out = jnp.where(lane_mask(part.shape, head), part, out)
        low = out.astype(BF16)
        att_ref[member] = low
        return dot_nt(low, wo_buf[...])

    def send(step, carry):
        @pl.when(step == size)
        def _():
            group.combine(stage, landing, rs_send, rs_recv)
            bg(2)

        member = group.member(size - step)
        stage[member] = attend(member).astype(BF16)
        group.give(stage, landing, rs_send, rs_recv, size - step)
        return carry

    lax.fori_loop(1, size + 1, send, 0)
    group.spread_sent(normed_ref, ag_send, ag_recv)
    bg(3)
    own = stage[me].astype(F32)
    branch = group.landed_sum(own, stage, landing, rs_send, rs_recv) + bproj_ref[...]
    branch_ref[...] = branch
    middle_ref[...] = hidden_ref[...].astype(F32) + mod_ref[2:3] * branch
    bg(4)


def mlp_fwd_kernel(
    bg,
    middle_ref, mod_ref, b1_ref, b2_ref, w1_ref, w2_ref,
    out_ref, normed_ref, pre_ref, gelu_ref, branch_ref,
    w1_buf, w2_buf, stage, landing, w_sem, ag_send, ag_recv, rs_send, rs_recv,
):
    group = Group(middle_ref.shape[0])
    me, size = group.me, group.size
    loads = load(w1_ref, w1_buf, w_sem.at[0]) + load(w2_ref, w2_buf, w_sem.at[1])
    normed, _ = norm_parts(middle_ref[...])
    normed_ref[me] = (normed * (1.0 + mod_ref[4:5]) + mod_ref[3:4]).astype(BF16)
    Place().greet()
    group.spread(normed_ref, ag_send, ag_recv)
    bg(0)
    for copy in loads:
        copy.wait()

    def dense(member):
        pre = dot_nn(normed_ref[member], w1_buf[...]) + b1_ref[...]
        pre_ref[member] = pre
        bent = jnp.tanh(GELU_C * (pre + GELU_A * pre * pre * pre))
        low = (0.5 * pre * (1.0 + bent)).astype(BF16)
        gelu_ref[member] = low
        return dot_nt(low, w2_buf[...])

    def send(step, carry):
        @pl.when(step == 1)
        def _():
            bg(1)

        member = group.member(step)
        group.arrive(normed_ref, ag_send, ag_recv, step)
        stage[member] = dense(member).astype(BF16)
        group.give(stage, landing, rs_send, rs_recv, step)
        return carry

    lax.fori_loop(0, size, send, 0)
    group.combine(stage, landing, rs_send, rs_recv)
    bg(2)
    group.spread_sent(normed_ref, ag_send, ag_recv)
    bg(3)
    own = stage[me].astype(F32)
    branch = group.landed_sum(own, stage, landing, rs_send, rs_recv) + b2_ref[...]
    branch_ref[...] = branch
    out_ref[...] = (middle_ref[...] + mod_ref[5:6] * branch).astype(BF16)
    bg(4)


def weight_grad(lhs_ref, rhs, out_ref, tile):
    def body(index, carry):
        cols = pl.ds(pl.multiple_of(index * tile, tile), tile)
        out_ref[cols, :] = dot_tn(lhs_ref[:, cols], rhs).astype(BF16)
        return carry

    lax.fori_loop(0, lhs_ref.shape[-1] // tile, body, 0)


def mlp_bwd_kernel(
    bg,
    grad_ref, middle_ref, mod_ref, branch_ref, normed_ref, pre_ref, gelu_ref, w1_ref, w2_ref,
    gmid_ref, dw1_ref, dw2_ref, db1_ref, db2_ref, dmod_ref,
    w1_buf, w2_buf, dbr, dpre, stage, landing, w_sem, ag_send, ag_recv, rs_send, rs_recv,
):
    tokens, width = grad_ref.shape
    group = Group(tokens)
    me, size = group.me, group.size
    loads = load(w1_ref, w1_buf, w_sem.at[0]) + load(w2_ref, w2_buf, w_sem.at[1])
    grad = grad_ref[...].astype(F32)
    dbr[me] = (grad * mod_ref[5:6]).astype(BF16)
    Place().greet()
    group.spread(dbr, ag_send, ag_recv)
    bg(0)
    dmod_ref[2:3] = col_sum(grad * branch_ref[...])
    for copy in loads:
        copy.wait()

    def back(member):
        dgelu = dot_nn(dbr[member], w2_buf[...])
        pre = pre_ref[member]
        bent = jnp.tanh(GELU_C * (pre + GELU_A * pre * pre * pre))
        slope = 0.5 * (1.0 + bent) + 0.5 * pre * (1.0 - bent * bent) * (
            GELU_C * (1.0 + 3.0 * GELU_A * pre * pre)
        )
        low = (dgelu * slope).astype(BF16)
        dpre[member] = low
        return dot_nt(low, w1_buf[...])

    stage[me] = back(me).astype(BF16)
    bg(1)

    def send(step, carry):
        member = group.member(step)
        group.arrive(dbr, ag_send, ag_recv, step)
        stage[member] = back(member).astype(BF16)
        group.give(stage, landing, rs_send, rs_recv, step)
        return carry

    lax.fori_loop(1, size, send, 0)
    group.combine(stage, landing, rs_send, rs_recv)
    bg(2)
    seq = size * tokens
    dpre_all = dpre[...].reshape(seq, -1)
    gelu_all = gelu_ref[...].reshape(seq, -1)
    db1_ref[...] = col_sum(dpre_all.astype(F32))
    db2_ref[...] = col_sum(dbr[...].reshape(seq, -1).astype(F32))
    weight_grad(normed_ref.reshape(seq, width), dpre_all, dw1_ref, 384)
    weight_grad(dbr.reshape(seq, width), gelu_all, dw2_ref, 384)
    group.spread_sent(dbr, ag_send, ag_recv)
    bg(3)
    total = group.landed_sum(stage[me].astype(F32), stage, landing, rs_send, rs_recv)
    normed, rstd = norm_parts(middle_ref[...])
    dmod_ref[0:1] = col_sum(total)
    dmod_ref[1:2] = col_sum(total * normed)
    gmid_ref[...] = norm_back(total, normed, rstd, mod_ref[4:5]) + grad_ref[...].astype(F32)
    bg(4)


def att_bwd_kernel(
    bg,
    gmid_ref, hidden_ref, mod_ref, branch_ref, normed_ref, proj_ref, att_ref, w_ref,
    gin_ref, dw_ref, dbqkv_ref, dbproj_ref, dmod_ref,
    w_buf, wo_buf, dba, dproj, dkey, dval, stage, landing, w_sem, ag_send, ag_recv, rs_send, rs_recv,
):
    tokens, width = gmid_ref.shape
    group = Group(tokens)
    me, size = group.me, group.size
    seq = size * tokens
    part_width = att_ref.shape[-1]
    heads = part_width // HEAD_SIZE
    loads = load(w_ref, w_buf, w_sem.at[0])
    gmid = gmid_ref[...]
    dba[me] = (gmid * mod_ref[2:3]).astype(BF16)
    Place().greet()
    group.spread(dba, ag_send, ag_recv)
    bg(0)
    dmod_ref[2:3] = col_sum(gmid * branch_ref[...])
    keys = proj_ref[1].reshape(seq, part_width)
    values = proj_ref[2].reshape(seq, part_width)
    keys_t = dot_nt(identity(part_width), keys).astype(BF16)
    dkey[...] = jnp.zeros_like(dkey)
    dval[...] = jnp.zeros_like(dval)
    for copy in loads:
        copy.wait()
    wo_buf[...] = w_buf[:, 3 * part_width :]

    def back(step, carry):
        @pl.when(step == 1)
        def _():
            bg(1)

        member = group.member(step)
        group.arrive(dba, ag_send, ag_recv, step)
        datt = dot_nn(dba[member], wo_buf[...]).astype(BF16)
        datt_st = stack_heads(datt)
        query_st = stack_heads(proj_ref[0, member])
        powered = jnp.exp(dot_nt(keys, query_st) * HEAD_SIZE**-0.5)
        probs = powered * (1.0 / jnp.sum(powered, axis=0, keepdims=True))
        dval[...] += dot_nn(probs.astype(BF16), datt_st)
        dprobs = dot_nt(values, datt_st)
        dscore = (probs * (dprobs - jnp.sum(probs * dprobs, axis=0, keepdims=True))).astype(BF16)
        dkey[...] += dot_nn(dscore, query_st)
        dq_t = dot_nn(keys_t, dscore)
        picked = dq_t[:, :tokens]
        for head in range(1, heads):
            part = dq_t[:, head * tokens : (head + 1) * tokens]
            picked = jnp.where(row_mask(part.shape, head), part, picked)
        low = (picked * HEAD_SIZE**-0.5).astype(BF16)
        dproj[member, :, :part_width] = dot_nt(identity(tokens), low).astype(BF16)
        return carry

    lax.fori_loop(0, size, back, 0)
    for member in range(size):
        rows = slice(member * tokens, (member + 1) * tokens)
        dproj[member, :, part_width : 2 * part_width] = (dkey[rows] * HEAD_SIZE**-0.5).astype(BF16)
        dproj[member, :, 2 * part_width :] = dval[rows].astype(BF16)

    def partial_rows(member):
        return dot_nt(dproj[member], w_buf[:, : 3 * part_width])

    def send(step, carry):
        member = group.member(size - step)
        stage[member] = partial_rows(member).astype(BF16)
        group.give(stage, landing, rs_send, rs_recv, size - step)
        return carry

    lax.fori_loop(1, size + 1, send, 0)
    group.combine(stage, landing, rs_send, rs_recv)
    bg(2)
    grads = dproj[...].reshape(seq, -1)
    dbqkv_ref[...] = col_sum(grads.astype(F32))
    dbproj_ref[...] = col_sum(dba[...].reshape(seq, width).astype(F32))
    mixed = att_ref[...].reshape(seq, part_width)
    normed_rows, dba_rows = normed_ref.reshape(seq, width), dba.reshape(seq, width)

    def weights(index, carry):
        cols = pl.ds(pl.multiple_of(index * 384, 128), 384)
        dw_ref[cols, : 3 * part_width] = dot_tn(normed_rows[:, cols], grads).astype(BF16)
        dw_ref[cols, 3 * part_width :] = dot_tn(dba_rows[:, cols], mixed).astype(BF16)
        return carry

    lax.fori_loop(0, width // 384, weights, 0)
    group.spread_sent(dba, ag_send, ag_recv)
    bg(3)
    total = group.landed_sum(stage[me].astype(F32), stage, landing, rs_send, rs_recv)
    hidden = hidden_ref[...].astype(F32)
    normed, rstd = norm_parts(hidden)
    dmod_ref[0:1] = col_sum(total)
    dmod_ref[1:2] = col_sum(total * normed)
    gin = norm_back(total, normed, rstd, mod_ref[1:2]) + gmid_ref[...]
    gin_ref[...] = gin.astype(BF16)
    bg(4)


class Place:
    def __init__(self):
        self.section, self.dp = lax.axis_index("section"), lax.axis_index("dp")
        self.high, self.low = lax.axis_index("mh"), lax.axis_index("ml")
        self.n_dp, self.n_low = lax.axis_size("dp"), lax.axis_size("ml")
        self.total = 4 * self.n_dp * self.n_low
        self.me = ((self.section * self.n_dp + self.dp) * 2 + self.high) * self.n_low + self.low

    def unflatten(self, number):
        low = lax.rem(number, self.n_low)
        rest = lax.div(number, self.n_low)
        high, rest = lax.rem(rest, 2), lax.div(rest, 2)
        return lax.div(rest, self.n_dp), lax.rem(rest, self.n_dp), high, low

    def greet(self):
        barrier = pltpu.get_barrier_semaphore()
        others = []
        for sec in range(2):
            for step in range(self.n_low):
                if sec or step:
                    section = lax.rem(self.section + sec, 2)
                    others.append((section, self.dp, self.high, lax.rem(self.low + step, self.n_low)))
        for sec in range(2):
            others.append(self.plane(sec, 1 - self.high))
        for step in range(1, self.n_dp // 2):
            others.append((self.section, self.same_core(step), self.high, self.low))
        others.append(self.core_mate())
        for device in others:
            pl.semaphore_signal(barrier, inc=1, device_id=device, device_id_type=MESH)
        pl.semaphore_wait(barrier, len(others))

    def role(self, layer, number):
        same = (self.section == layer) if number < 2 else (self.section != layer)
        return same & ((self.high == layer) if number % 2 == 0 else (self.high != layer))

    def role_device(self, layer, number):
        section = layer if number < 2 else 1 - layer
        return self.plane(section, layer if number % 2 == 0 else 1 - layer)

    def greet_all(self):
        barrier = pltpu.get_barrier_semaphore()

        def body(step, carry):
            pl.semaphore_signal(
                barrier,
                inc=1,
                device_id=self.unflatten(lax.rem(self.me + step, self.total)),
                device_id_type=MESH,
            )
            return carry

        lax.fori_loop(1, self.total, body, 0)
        pl.semaphore_wait(barrier, self.total - 1)

    def copy(self, src, dst, send_sem, recv_sem, device):
        return pltpu.make_async_remote_copy(
            src_ref=src,
            dst_ref=dst,
            send_sem=send_sem,
            recv_sem=recv_sem,
            device_id=device,
            device_id_type=MESH,
        )

    def core_mate(self):
        return (self.section, self.dp + 1 - 2 * lax.rem(self.dp, 2), self.high, self.low)

    def same_core(self, step):
        return lax.rem(self.dp + 2 * step, self.n_dp)

    def plane(self, section, high):
        return (section, self.dp, high, self.low)

    def exchange(self, pick, landing, send_sem, recv_sem):
        landing[self.me] = pick((self.section, self.dp, self.high, self.low))[...]

        def copy(number):
            device = self.unflatten(number)
            return self.copy(
                pick(device), landing.at[self.me], send_sem.at[number], recv_sem.at[self.me], device
            )

        def start(step, carry):
            copy(lax.rem(self.me + step, self.total)).start()
            return carry

        def finish(step, carry):
            number = lax.rem(self.me + step, self.total)
            device = self.unflatten(number)
            self.copy(
                landing.at[number], landing.at[number], send_sem.at[number], recv_sem.at[number], device
            ).wait_recv()
            copy(number).wait_send()
            return carry

        lax.fori_loop(1, self.total, start, 0)
        return lambda: lax.fori_loop(1, self.total, finish, 0)


VM = pl.BlockSpec(memory_space=pltpu.VMEM)
ANY = pl.BlockSpec(memory_space=pltpu.HBM)
DMA = pltpu.SemaphoreType.DMA


class Handle:
    def __init__(self, shape, dtype):
        self.shape, self.dtype = shape, dtype
        self.array = None
        self.ref = None


class Task:
    inputs = ()
    outs = ()
    scratch = ()
    handles = ()


class Collect(Task):
    def __init__(self, item, layer, handle):
        self.layer, self.handle = layer, handle
        self.inputs = ((item, VM),)
        self.handles = (handle,)
        self.chunk = item.shape[0]
        self.scratch = (DMA((2,)), DMA, DMA)

    def run(self, phase, refs):
        (item,), _, (send, recv, own) = refs
        place = Place()
        source = item
        rows = self.handle.ref.at[pl.ds(pl.multiple_of(place.dp * self.chunk, 16), self.chunk)]

        def to(number, role):
            return place.copy(
                source, rows, send.at[number], recv, place.role_device(self.layer, role)
            )

        targets = {0: (1,), 1: (2, 3), 2: (), 3: ()}
        for role in range(4):

            @pl.when(place.role(self.layer, role))
            def _():
                if phase == "a":
                    for number, target in enumerate(targets[role]):
                        to(number, target).start()
                    if role == 0:
                        pltpu.make_async_copy(source, rows, own).start()
                if phase == "b":
                    if role == 0:
                        pltpu.make_async_copy(source, rows, own).wait()
                    else:
                        place.copy(
                            rows, rows, send.at[0], recv, place.role_device(self.layer, 0)
                        ).wait_recv()
                if phase == "c":
                    for number, target in enumerate(targets[role]):
                        to(number, target).wait_send()


class Widen(Task):
    def __init__(self, handle):
        self.handle = handle
        self.handles = (handle,)
        chips = lax.axis_size("dp") // 2
        self.scratch = (DMA((chips,)),) * 4

    def rows(self, index):
        chunk = self.handle.shape[0] // lax.axis_size("dp")
        return self.handle.ref.at[pl.ds(pl.multiple_of(index * chunk, 16), chunk)]

    def run(self, phase, refs):
        _, _, (x_send, x_recv, c_send, c_recv) = refs
        place = Place()
        chips = place.n_dp // 2

        def across(step):
            return place.copy(
                self.rows(place.dp), self.rows(place.dp), x_send.at[step], x_recv.at[step],
                (place.section, place.same_core(step), place.high, place.low),
            )

        def landed(step):
            held = self.rows(place.same_core(chips - step))
            return place.copy(
                held, held, x_send.at[step], x_recv.at[step],
                (place.section, place.same_core(step), place.high, place.low),
            )

        def to_mate(step):
            held = self.rows(place.same_core(step))
            return place.copy(held, held, c_send.at[step], c_recv.at[step], place.core_mate())

        def from_mate(step):
            held = self.rows(lax.rem(place.core_mate()[1] + 2 * step, place.n_dp))
            return place.copy(held, held, c_send.at[step], c_recv.at[step], place.core_mate())

        if phase == "a":
            for step in range(1, chips):
                across(step).start()
            to_mate(0).start()
        if phase == "b":
            for step in range(1, chips):
                landed(step).wait_recv()
                to_mate(chips - step).start()
        if phase == "c":
            for step in range(chips):
                from_mate(step).wait_recv()
                to_mate(step).wait_send()
                if step:
                    across(step).wait_send()


class Narrow(Task):
    def __init__(self, grad):
        n_dp = lax.axis_size("dp")
        chips = n_dp // 2
        self.chunk = grad.shape[0] // n_dp
        block = (chips, self.chunk, grad.shape[1])
        self.inputs = ((grad, ANY),)
        self.outs = (((self.chunk, grad.shape[1]), BF16, VM),)
        self.scratch = (pltpu.VMEM(block, BF16),) * 3 + (DMA((chips,)),) * 5

    def run(self, phase, refs):
        (grad,), (out,), scratch = refs
        own, near, far, own_sem, c_send, c_recv, x_send, x_recv = scratch
        place = Place()
        chips = place.n_dp // 2

        def rows(index):
            return grad.at[pl.ds(pl.multiple_of(index * self.chunk, 16), self.chunk)]

        def to_mate(step):
            other = lax.rem(place.core_mate()[1] + 2 * step, place.n_dp)
            return place.copy(
                rows(other), near.at[step], c_send.at[step], c_recv.at[step], place.core_mate()
            )

        def load_own(step):
            return pltpu.make_async_copy(
                rows(place.same_core(step)), own.at[step], own_sem.at[step]
            )

        def across(step):
            return place.copy(
                own.at[step], far.at[step], x_send.at[step], x_recv.at[step],
                (place.section, place.same_core(step), place.high, place.low),
            )

        order = list(range(1, chips)) + [0]
        if phase == "a":
            for step in order:
                to_mate(step).start()
                load_own(step).start()
        if phase == "b":
            for step in order:
                load_own(step).wait()
                to_mate(step).wait_recv()
                own[step] = (own[step].astype(F32) + near[step].astype(F32)).astype(BF16)
                if step:
                    across(step).start()
        if phase == "c":
            total = own[0].astype(F32)
            for step in range(1, chips):
                across(step).wait_recv()
                total = total + far[step].astype(F32)
            out[...] = total.astype(BF16)
            for step in range(chips):
                to_mate(step).wait_send()
                if step:
                    across(step).wait_send()


class Settle(Task):
    def __init__(self, part, layer, held=None, into=None):
        self.layer = layer
        self.held = held
        self.into = into
        self.inputs = () if held else ((part, ANY),)
        self.outs = () if into else ((part.shape, F32, VM),)
        self.scratch = (
            pltpu.VMEM((2,) + part.shape, BF16), pltpu.VMEM(part.shape, BF16),
            DMA((2,)), DMA((3,)), DMA,
        )

    def run(self, phase, refs):
        ins, outs, (land, temp, send, recv, own_sem) = refs
        (out,) = self.into.refs[1] if self.into else outs
        part = self.held() if self.held else ins[0]
        place = Place()
        layer = self.layer

        def to(src, dst, s, r, role):
            return place.copy(src, dst, send.at[s], recv.at[r], place.role_device(layer, role))

        def direct(role):
            if role == 2:
                return to(part, temp, 0, 2, 0)
            return to(part, land.at[0], 0, 0, 0 if role == 1 else 1)

        def relay():
            return to(temp, land.at[1], 1, 1, 1)

        for role in range(4):

            @pl.when(place.role(layer, role))
            def _():
                if phase == "z" and role == 1:
                    direct(role).start()
                if phase == "a":
                    if role > 1:
                        direct(role).start()
                    if role == 0:
                        pltpu.make_async_copy(part, land.at[1], own_sem).start()
                if phase == "b":
                    if role == 0:
                        to(temp, temp, 0, 2, 0).wait_recv()
                        relay().start()
                    if role > 1:
                        direct(role).wait_send()
                if phase == "s":
                    if role == 0:
                        relay().wait_send()
                    if role == 1:
                        direct(role).wait_send()
                if phase == "c":
                    if role == 0:
                        pltpu.make_async_copy(part, land.at[1], own_sem).wait()
                    if role < 2:
                        to(land.at[0], land.at[0], 0, 0, role).wait_recv()
                    if role == 1:
                        to(land.at[1], land.at[1], 0, 1, 1).wait_recv()
                    if role < 2:
                        out[...] = land[0].astype(F32) + land[1].astype(F32)


class Deliver(Task):
    def __init__(self, rows, layer, into=None):
        self.layer = layer
        self.into = into
        self.inputs = ((rows, VM),)
        self.outs = () if into else (((2,) + rows.shape, rows.dtype, VM),)
        self.scratch = (pltpu.VMEM(rows.shape, rows.dtype), DMA((2,)), DMA((3,)))

    def run(self, phase, refs):
        (rows,), outs, (temp, send, recv) = refs
        (out,) = self.into.refs[1] if self.into else outs
        place = Place()
        layer = self.layer

        def to(src, dst, s, r, role):
            return place.copy(src, dst, send.at[s], recv.at[r], place.role_device(layer, role))

        def direct(role):
            if role == 2:
                return to(rows, temp, 0, 2, 0)
            return to(rows, out.at[1 - layer], 0, 0, 0 if role == 1 else 1)

        def relay():
            return to(temp, out.at[layer], 1, 1, 1)

        for role in range(4):

            @pl.when(place.role(layer, role))
            def _():
                if phase == "z" and role == 1:
                    direct(role).start()
                if phase == "a":
                    if role > 1:
                        direct(role).start()
                    if role == 0:
                        out[layer] = rows[...]
                if phase == "b" and role == 0:
                    to(temp, temp, 0, 2, 0).wait_recv()
                    relay().start()
                if phase == "c":
                    if role == 0:
                        relay().wait_send()
                    else:
                        direct(role).wait_send()
                    if role < 2:
                        to(out.at[1 - layer], out.at[1 - layer], 0, 0, role).wait_recv()
                    if role == 1:
                        to(out.at[layer], out.at[layer], 0, 1, 1).wait_recv()


class Tokens(Task):
    def __init__(self, rows):
        self.inputs = ((rows, VM),)
        self.outs = ((rows.shape[1:], rows.dtype, VM),)
        self.scratch = (DMA, DMA((2,)))

    def run(self, phase, refs):
        (rows,), (out,), (send, recv) = refs
        place = Place()
        half = rows.shape[1] // 2
        parts = (slice(0, half), slice(half, 2 * half))

        def copy(part, section):
            return place.copy(
                rows.at[1 - place.high, parts[part]], out.at[parts[part]], send, recv.at[part],
                place.plane(section, 1 - place.high),
            )

        @pl.when(place.section == place.high)
        def _():
            if phase == "a":
                copy(0, place.section).start()
                out[...] = rows[place.high]
            if phase == "c":
                copy(0, place.section).wait_send()

        @pl.when(place.section != place.high)
        def _():
            if phase == "a":
                copy(1, 1 - place.section).start()
            if phase == "c":
                copy(1, 1 - place.section).wait_send()
                copy(0, place.section).wait_recv()
                copy(1, place.section).wait_recv()


def launch(kernel, operands, outs, scratch, schedule, cid, name):
    tasks = []
    for point in schedule:
        for task, _ in point:
            if task not in tasks:
                tasks.append(task)
    operands, outs, scratch = list(operands), list(outs), list(scratch)
    n_in, n_out, n_scratch = len(operands), len(outs), len(scratch)
    spans = []
    for task in tasks:
        spans.append((len(operands), len(outs), len(scratch)))
        operands += task.inputs
        outs += task.outs
        scratch += task.scratch
    handles = []
    for task in tasks:
        for handle in task.handles:
            if handle not in handles:
                handles.append(handle)
    aliases = {}
    first_handle = len(outs)
    for handle in handles:
        if handle.array is not None:
            aliases[len(operands)] = len(outs)
            operands.append((handle.array, ANY))
        outs.append((handle.shape, handle.dtype, ANY))

    def body(*refs):
        ins = refs[: len(operands)]
        results = refs[len(operands) : len(operands) + len(outs)]
        rest = refs[len(operands) + len(outs) :]
        for number, handle in enumerate(handles):
            handle.ref = results[first_handle + number]
        views = []
        for task, (a, b, c) in zip(tasks, spans):
            views.append(
                (
                    ins[a : a + len(task.inputs)],
                    results[b : b + len(task.outs)],
                    rest[c : c + len(task.scratch)],
                )
            )
            task.refs = views[-1]

        def bg(point):
            for task, phase in schedule[point]:
                task.run(phase, task.refs)

        kernel(bg, *ins[:n_in], *results[:n_out], *rest[:n_scratch])

    done = pl.pallas_call(
        body,
        out_shape=tuple(jax.ShapeDtypeStruct(shape, dtype) for shape, dtype, _ in outs),
        in_specs=[spec for _, spec in operands],
        out_specs=tuple(spec for _, _, spec in outs),
        scratch_shapes=scratch,
        input_output_aliases=aliases,
        compiler_params=pltpu.CompilerParams(
            collective_id=cid, has_side_effects=True, vmem_limit_bytes=VMEM_LIMIT
        ),
        name=name,
    )(*[array for array, _ in operands])
    for number, handle in enumerate(handles):
        handle.array = done[first_handle + number]
        handle.ref = None
    for task, (_, b, _) in zip(tasks, spans):
        task.results = done[b : b + len(task.outs)]
    return done[:n_out]


def group_size():
    return lax.axis_size("section") * lax.axis_size("ml")


def comm_scratch(tokens, width):
    size = group_size()
    return [pltpu.VMEM((size, tokens, width), BF16)] * 2, [DMA((max(size, 6),))] * 4


def att_fwd(hidden, mod, bias, bproj, w, schedule, cid):
    tokens, width = hidden.shape
    size = group_size()
    part_width = width // size
    bufs, sems = comm_scratch(tokens, width)
    return launch(
        att_fwd_kernel,
        [(hidden, VM), (mod, VM), (bias, VM), (bproj, VM), (w.array, ANY)],
        [
            ((tokens, width), F32, VM),
            ((size, tokens, width), BF16, VM),
            ((3, size, tokens, part_width), BF16, VM),
            ((size, tokens, part_width), BF16, VM),
            ((tokens, width), F32, VM),
        ],
        [pltpu.VMEM(w.shape, BF16), pltpu.VMEM((width, part_width), BF16)]
        + bufs
        + [DMA((1,))]
        + sems,
        schedule,
        cid,
        "att_fwd",
    )


def mlp_fwd(middle, mod, b1, b2, w1, w2, schedule, cid):
    tokens, width = middle.shape
    size = group_size()
    units = w1.shape[1]
    bufs, sems = comm_scratch(tokens, width)
    return launch(
        mlp_fwd_kernel,
        [(middle, VM), (mod, VM), (b1, VM), (b2, VM), (w1.array, ANY), (w2.array, ANY)],
        [
            ((tokens, width), BF16, VM),
            ((size, tokens, width), BF16, VM),
            ((size, tokens, units), F32, VM),
            ((size, tokens, units), BF16, VM),
            ((tokens, width), F32, VM),
        ],
        [pltpu.VMEM(w1.shape, BF16)] * 2 + bufs + [DMA((2,))] + sems,
        schedule,
        cid,
        "mlp_fwd",
    )


def mlp_bwd(grad, middle, mod, branch, normed, pre, gelu, w1, w2, schedule, cid):
    tokens, width = middle.shape
    size = group_size()
    units = w1.shape[1]
    bufs, sems = comm_scratch(tokens, width)
    ins = (grad, middle, mod, branch, normed, pre, gelu)
    return launch(
        mlp_bwd_kernel,
        [(array, VM) for array in ins] + [(w1.array, ANY), (w2.array, ANY)],
        [
            ((tokens, width), F32, VM),
            (w1.shape, BF16, VM),
            (w2.shape, BF16, VM),
            ((1, units), F32, VM),
            ((1, width), F32, VM),
            ((3, width), F32, VM),
        ],
        [pltpu.VMEM(w1.shape, BF16)] * 2
        + [pltpu.VMEM((size, tokens, width), BF16), pltpu.VMEM((size, tokens, units), BF16)]
        + bufs
        + [DMA((2,))]
        + sems,
        schedule,
        cid,
        "mlp_bwd",
    )


def att_bwd(gmid, hidden, mod, branch, normed, proj, att, w, schedule, cid):
    tokens, width = gmid.shape
    size = group_size()
    part_width = width // size
    bufs, sems = comm_scratch(tokens, width)
    seq = size * tokens
    ins = (gmid, hidden, mod, branch, normed, proj, att)
    return launch(
        att_bwd_kernel,
        [(array, VM) for array in ins] + [(w.array, ANY)],
        [
            ((tokens, width), BF16, VM),
            (w.shape, BF16, VM),
            ((1, 3 * part_width), F32, VM),
            ((1, width), F32, VM),
            ((3, width), F32, VM),
        ],
        [
            pltpu.VMEM(w.shape, BF16),
            pltpu.VMEM((width, part_width), BF16),
            pltpu.VMEM((size, tokens, width), BF16),
            pltpu.VMEM((size, tokens, 3 * part_width), BF16),
            pltpu.VMEM((seq, part_width), F32),
            pltpu.VMEM((seq, part_width), F32),
        ]
        + bufs
        + [DMA((1,))]
        + sems,
        schedule,
        cid,
        "att_bwd",
    )


def prologue_kernel(
    bg,
    cond_ref, wada_ref, bada_ref, bias_ref,
    modul_ref, act_ref, bias_out,
    cond_land, share, land, cond_send, cond_recv, mod_send, mod_recv, b_send, b_recv,
):
    place = Place()
    section, dp, high = place.section, place.dp, place.high
    place.greet_all()

    def spread(step):
        other = lax.rem(dp + step, place.n_dp)
        return place.copy(
            cond_ref.at[other], cond_land.at[dp], cond_send.at[step], cond_recv.at[dp],
            (section, other, high, place.low),
        )

    def spread_wait(step):
        other = lax.rem(dp + step, place.n_dp)
        return place.copy(
            cond_land.at[other], cond_land.at[other], cond_send.at[step], cond_recv.at[other],
            (section, other, high, place.low),
        )

    cond_land[dp] = cond_ref[dp]
    for step in range(1, place.n_dp):
        spread(step).start()

    def bias_copy(target):
        return place.copy(
            bias_ref, bias_out.at[section], b_send.at[target], b_recv.at[section],
            place.plane(high, target),
        )

    here = section == high
    for target in range(2):

        @pl.when(jnp.logical_not(here & (high == target)))
        def _():
            bias_copy(target).start()

    @pl.when(here)
    def _():
        bias_out[section] = bias_ref[...]

    bg(0)
    for step in range(1, place.n_dp):
        spread_wait(step).wait_recv()
    parts = [cond_land[index] for index in range(place.n_dp)]
    act = jax.nn.silu(jnp.concatenate(parts, axis=0)).astype(BF16)
    act_ref[...] = act
    bias = jnp.where(dp == 0, bada_ref[...], 0.0)
    product = dot_nn(act, wada_ref[...])
    for row in range(2 * place.n_dp):
        share[row] = product[row : row + 1] + bias
    finish = place.exchange(
        lambda device: share.at[device[1] * 2 + device[2]], land, mod_send, mod_recv
    )
    bg(1)
    bg(2)
    finish()
    for layer in range(2):
        for part in range(2 * place.n_low):
            total = land[layer * place.n_dp * 2 * place.n_low + part]
            for index in range(1, place.n_dp):
                total = total + land[(layer * place.n_dp + index) * 2 * place.n_low + part]
            modul_ref[layer * 2 * place.n_low + part] = total
    bg(3)
    for step in range(1, place.n_dp):
        spread(step).wait_send()
    for target in range(2):

        @pl.when(jnp.logical_not(here & (high == target)))
        def _():
            bias_copy(target).wait_send()

        @pl.when(jnp.logical_not(here & (section == target)))
        def _():
            place.copy(
                bias_out.at[target], bias_out.at[target], b_send.at[0], b_recv.at[target],
                place.plane(section, 1 - high),
            ).wait_recv()

    bg(4)


def prologue(cond, wada, bada, bias, schedule, cid):
    n_dp, _, chunk = cond.shape
    n_mp = 2 * lax.axis_size("ml")
    total = 2 * n_dp * n_mp
    share = wada.shape[1]
    return launch(
        prologue_kernel,
        [(cond, VM), (wada, VM), (bada, VM), (bias, VM)],
        [
            ((2 * n_mp, 1, share), F32, VM),
            ((2 * n_dp, chunk), BF16, VM),
            ((2,) + bias.shape, F32, VM),
        ],
        [
            pltpu.VMEM((n_dp, 2, chunk), F32),
            pltpu.VMEM((2 * n_dp, 1, share), F32),
            pltpu.VMEM((total, 1, share), F32),
            DMA((n_dp,)),
            DMA((n_dp,)),
            DMA((total,)),
            DMA((total,)),
            DMA((2,)),
            DMA((2,)),
        ],
        schedule,
        cid,
        "prologue",
    )


def epilogue_kernel(
    bg,
    dmod_ref, wada_ref, dbias_ref,
    dmod_out, gbada_ref, gact_ref, gbias_ref,
    mod_land, act_stage, act_land, bias_land, bias_stage, bias_final,
    mod_send, mod_recv, act_send, act_recv, d_send, d_recv, b_send, b_recv,
):
    place = Place()
    section, dp, high = place.section, place.dp, place.high
    place.greet_all()
    finish_mod = place.exchange(
        lambda device: dmod_ref.at[(device[0] * 2 + device[2]) * place.n_low + device[3]],
        mod_land, mod_send, mod_recv,
    )

    def spread(step):
        other = lax.rem(dp + step, place.n_dp)
        return place.copy(
            dbias_ref, bias_land.at[dp], d_send.at[step], d_recv.at[dp],
            (section, other, high, place.low),
        )

    for step in range(1, place.n_dp):
        spread(step).start()
    bg(0)
    finish_mod()
    parts = 2 * place.n_low
    latents = []
    for index in range(place.n_dp):
        for micro in range(2):
            total = 0.0
            for sec in range(2):
                for low in range(place.n_low):
                    number = ((sec * place.n_dp + index) * 2 + micro) * place.n_low + low
                    total = total + mod_land[number]
            latents.append(total)
    dmod = jnp.concatenate(latents, axis=0).astype(BF16)
    back = dot_nt(dmod, wada_ref[...])
    for index in range(place.n_dp):
        act_stage[index] = back[2 * index : 2 * index + 2]
    finish_act = place.exchange(lambda device: act_stage.at[device[1]], act_land, act_send, act_recv)
    bias_sum = dbias_ref[...]
    for step in range(1, place.n_dp):
        other = lax.rem(dp + step, place.n_dp)
        place.copy(
            bias_land.at[other], bias_land.at[other], d_send.at[step], d_recv.at[other],
            (section, other, high, place.low),
        ).wait_recv()
        bias_sum = bias_sum + bias_land[other]
    bias_stage[...] = bias_sum

    def settle(layer):
        return place.copy(
            bias_stage.at[layer], bias_final.at[high], b_send.at[layer], b_recv.at[high],
            place.plane(layer, section),
        )

    for layer in range(2):
        here = (section == layer) & (high == section)

        @pl.when(here)
        def _():
            bias_final[high] = bias_stage[layer]

        @pl.when(jnp.logical_not(here))
        def _():
            settle(layer).start()

    bg(1)
    gbada_ref[...] = col_sum(dmod.astype(F32))
    dmod_out[...] = dmod
    bg(2)
    finish_act()
    for index in range(place.n_dp):
        total = 0.0
        for sec in range(2):
            for part in range(parts):
                total = total + act_land[(sec * place.n_dp + index) * parts + part]
        gact_ref[index] = total
    bg(3)
    for half in range(2):
        here = (section == high) & (high == half)

        @pl.when(jnp.logical_not(here))
        def _():
            place.copy(
                bias_final.at[half], bias_final.at[half], b_send.at[0], b_recv.at[half],
                place.plane(high, half),
            ).wait_recv()

    gbias_ref[...] = bias_final[0] + bias_final[1]
    for layer in range(2):

        @pl.when(jnp.logical_not((section == layer) & (high == section)))
        def _():
            settle(layer).wait_send()

    for step in range(1, place.n_dp):
        spread(step).wait_send()
    bg(4)


def epilogue(dmod, wada, dbias, schedule, cid):
    n_dp, n_mp = lax.axis_size("dp"), 2 * lax.axis_size("ml")
    total = 2 * n_dp * n_mp
    chunk, share = wada.shape
    row = dbias.shape[1:]
    return launch(
        epilogue_kernel,
        [(dmod, VM), (wada, VM), (dbias, VM)],
        [
            ((2 * n_dp, share), BF16, VM),
            ((1, share), F32, VM),
            ((n_dp, 2, chunk), F32, VM),
            (row, F32, VM),
        ],
        [
            pltpu.VMEM((total, 1, share), F32),
            pltpu.VMEM((n_dp, 2, chunk), F32),
            pltpu.VMEM((total, 2, chunk), F32),
            pltpu.VMEM((n_dp,) + dbias.shape, F32),
            pltpu.VMEM(dbias.shape, F32),
            pltpu.VMEM((2,) + row, F32),
            DMA((total,)),
            DMA((total,)),
            DMA((total,)),
            DMA((total,)),
            DMA((n_dp,)),
            DMA((n_dp,)),
            DMA((2,)),
            DMA((2,)),
        ],
        schedule,
        cid,
        "epilogue",
    )


def per_device(
    latents_in, condition, cotangent,
    modulation_weight, modulation_bias, query_key_value_weight, query_value_bias,
    output_proj_weight, output_proj_bias, first_dense_weight, first_dense_bias,
    second_dense_weight, second_dense_bias,
):
    dp = lax.axis_index("dp")
    n_dp, n_low = lax.axis_size("dp"), lax.axis_size("ml")
    n_mp = 2 * n_low
    width = latents_in.shape[-1]
    rows = modulation_weight.shape[1]
    cols = modulation_weight.shape[2]
    part_width = query_key_value_weight.shape[3]
    units = first_dense_weight.shape[2]

    item = (
        jnp.concatenate(
            [query_key_value_weight[0].reshape(rows, -1), output_proj_weight[0].T], axis=1
        ),
        first_dense_weight[0],
        second_dense_weight[0].T,
    )
    cond = condition[:, 0].astype(F32)
    packed = jnp.concatenate(
        [
            query_value_bias[0, 0], query_value_bias[0, 1], first_dense_bias[0],
            output_proj_bias[0], second_dense_bias[0],
        ]
    ).astype(F32)[None]
    w = [[Handle((width, units), BF16) for _ in range(3)] for _ in range(2)]
    collect = [[Collect(item[t], l, w[l][t]) for t in range(3)] for l in range(2)]
    widen = [[Widen(w[l][t]) for t in range(3)] for l in range(2)]
    tokens_in = Tokens(latents_in[:, 0])
    tokens_cot = Tokens(cotangent[:, 0])

    def plan(*points):
        out = []
        for point in points:
            out.append([(task, phase) for task, phases in point for phase in phases])
        return out

    c, x = collect, widen
    modul, act_rows, biases = prologue(
        cond.reshape(2, n_dp, rows).transpose(1, 0, 2),
        modulation_weight[0],
        modulation_bias.astype(F32),
        packed,
        plan(
            [(tokens_in, "a"), (c[0][0], "a"), (c[1][0], "a")],
            [(c[0][0], "c"), (c[1][0], "c"), (c[0][1], "a"), (c[1][1], "a")]
            + [(c[0][0], "b"), (x[0][0], "a"), (c[1][0], "b")],
            [(c[0][1], "c"), (c[1][1], "c"), (c[0][2], "a"), (c[1][2], "a")]
            + [(x[0][0], "b"), (c[0][1], "b"), (x[0][1], "a"), (c[1][1], "b")],
            [],
            [(c[0][2], "c"), (c[1][2], "c"), (c[0][2], "b"), (c[1][2], "b"), (x[0][1], "b")]
            + [(tokens_in, "c"), (x[0][0], "c"), (x[0][1], "c")],
        ),
        1,
    )
    modul = modul.reshape(2, 6, width)
    bounds = [0, part_width, 2 * part_width, 2 * part_width + units, 2 * part_width + units + width]
    bqkv = jnp.concatenate(
        [
            biases[..., : bounds[1]], jnp.zeros((2, 1, part_width), F32),
            biases[..., bounds[1] : bounds[2]],
        ],
        axis=-1,
    )
    b1 = biases[..., bounds[2] : bounds[3]]
    bproj = biases[..., bounds[3] : bounds[4]]
    b2 = biases[..., bounds[4] :]

    hidden = [tokens_in.results[0]]
    att_plan = [
        plan(
            [(x[0][2], "a")],
            [],
            [],
            [(x[0][2], "b")],
            [(x[0][2], "c")],
        ),
        plan(
            [(x[1][1], "a"), (x[1][2], "a"), (tokens_cot, "a")],
            [],
            [],
            [(x[1][1], "b"), (x[1][2], "b")],
            [(x[1][1], "c"), (x[1][2], "c"), (tokens_cot, "c")],
        ),
    ]
    saved = []
    for layer in range(2):
        middle, normed, proj, att, branch = att_fwd(
            hidden[layer], modul[layer], bqkv[layer], bproj[layer], w[layer][0], att_plan[layer],
            2 + 2 * layer,
        )
        if layer == 0:
            mlp_plan = plan(
                [(x[1][0], "a")],
                [],
                [],
                [(x[1][0], "b")],
                [(x[1][0], "c")],
            )
        else:
            acts_first = Deliver(hidden[1], 0)
            mlp_plan = plan([], [], [], [], [])
        out, normed2, pre, gelu, branch2 = mlp_fwd(
            middle, modul[layer], b1[layer], b2[layer], w[layer][1], w[layer][2], mlp_plan,
            3 + 2 * layer,
        )
        saved.append((middle, normed, proj, att, branch, normed2, pre, gelu, branch2))
        hidden.append(out)

    grad = tokens_cot.results[0]
    narrow = [[None] * 3 for _ in range(2)]
    settle = [[None] * 3 for _ in range(2)]
    d_bias, d_mod, gins = {}, {}, {}
    acts_second = Deliver(hidden[2], 1, acts_first)
    for layer in (1, 0):
        middle, normed, proj, att, branch, normed2, pre, gelu, branch2 = saved[layer]
        if layer == 1:
            mlp_plan = plan(
                [(acts_first, "a"), (acts_second, "a")],
                [],
                [(acts_first, "zb"), (acts_second, "zb")],
                [],
                [(acts_first, "c"), (acts_second, "c")],
            )
        else:
            third = narrow[1][0]
            mlp_plan = plan([(third, "a")], [(third, "b")], [], [], [(third, "c")])
        gmid, dw1, dw2, db1, db2, dmod2 = mlp_bwd(
            grad, middle, modul[layer], branch2, normed2, pre, gelu, w[layer][1], w[layer][2],
            mlp_plan, 6 + 2 * (1 - layer),
        )
        narrow[layer][1], narrow[layer][2] = Narrow(dw1), Narrow(dw2)
        one, two = narrow[layer][1], narrow[layer][2]
        if layer == 0:
            settle[1][0] = Settle(narrow[1][0].results[0], 1)
            gin_second = Deliver(gins[1], 1)
        att_plan = plan(
            [(two, "a"), (one, "a")], [(two, "b"), (one, "b")], [], [], [(two, "c"), (one, "c")]
        )
        gin, dw, dbqkv, dbproj, dmod1 = att_bwd(
            gmid, hidden[layer], modul[layer], branch, normed, proj, att, w[layer][0],
            att_plan, 7 + 2 * (1 - layer),
        )
        for tensor in (1, 2):
            into = None if layer else settle[1][tensor]
            settle[layer][tensor] = Settle(narrow[layer][tensor].results[0], layer, into=into)
        narrow[layer][0] = Narrow(dw)
        gins[layer] = grad = gin
        d_bias[layer] = jnp.concatenate(
            [dbqkv[:, :part_width], dbqkv[:, 2 * part_width :], db1, dbproj, db2], axis=1
        )
        d_mod[layer] = jnp.concatenate([dmod1.reshape(-1), dmod2.reshape(-1)])

    last = narrow[0][0]
    final = Settle(jax.ShapeDtypeStruct((rows, units), BF16), 0, held=lambda: last.refs[1][0], into=settle[1][0])
    settle[0][0] = final
    gin_first = Deliver(gins[0], 0, gin_second)
    dmod = jnp.stack([d_mod[0], d_mod[1]]).reshape(2 * n_mp, 1, cols)
    dmod_all, g_bada, g_act, g_bias = epilogue(
        dmod,
        modulation_weight[0],
        jnp.stack([d_bias[0], d_bias[1]]),
        plan(
            [(gin_first, "az"), (gin_second, "az"), (last, "a"), (gin_first, "b"), (gin_second, "b")]
            + [(settle[0][2], "az"), (settle[1][2], "az")],
            [(settle[0][2], "b"), (settle[1][2], "b"), (settle[0][1], "a"), (settle[1][1], "a"), (last, "b")]
            + [(settle[0][2], "s"), (settle[1][2], "s"), (settle[0][1], "bz"), (settle[1][1], "bz")],
            [(last, "c"), (settle[1][0], "a"), (final, "a"), (settle[0][1], "s"), (settle[1][1], "s")]
            + [(settle[1][0], "bz"), (final, "bz")],
            [(settle[0][2], "c"), (settle[1][2], "c"), (settle[0][1], "c"), (settle[1][1], "c")],
            [(gin_first, "c"), (gin_second, "c"), (settle[1][0], "s"), (final, "s")]
            + [(settle[1][0], "c"), (final, "c")],
        ),
        10,
    )
    g_wada = dot_tn(act_rows, dmod_all)
    g_act = g_act.transpose(1, 0, 2).reshape(2, width)
    g_att, g_one, g_two = [settle[1][t].results[0] for t in range(3)]
    g_qkv = g_att[:, : 3 * part_width].reshape(rows, 3, part_width)
    g_proj = g_att[:, 3 * part_width :].T

    def dp_part(vec):
        size = vec.shape[-1] // n_dp
        return lax.dynamic_slice_in_dim(vec, dp * size, size, vec.ndim - 1)

    g_bias = g_bias[0]
    g_bqv = dp_part(g_bias[: bounds[2]].reshape(2, part_width))
    g_b1 = dp_part(g_bias[bounds[2] : bounds[3]])
    g_bproj = dp_part(g_bias[bounds[3] : bounds[4]])
    g_b2 = dp_part(g_bias[bounds[4] :])
    g_bada = dp_part(g_bada[0])
    _, silu_back = jax.vjp(jax.nn.silu, cond)
    g_cond = silu_back(g_act)[0][:, None]
    acts_out = acts_first.results[0][None, :, None]
    grad_input = gin_second.results[0].astype(F32)[None, :, None]
    return (
        acts_out,
        grad_input,
        g_cond,
        g_wada[None],
        g_bada[None],
        g_qkv[None],
        g_bqv[None],
        g_proj[None],
        g_bproj[None],
        g_one[None],
        g_b1[None],
        g_two.T[None],
        g_b2[None],
    )


def solution(mesh):
    sizes = mesh.shape
    grid = mesh.devices.reshape(sizes["section"], sizes["dp"], 2, sizes["mp"] // 2)
    fine = Mesh(grid, ("section", "dp", "mh", "ml"))
    mp = ("mh", "ml")
    in_specs = (
        P(None, "dp", mp, None),
        P(None, "dp", None),
        P(None, "dp", mp, None),
        P("section", "dp", mp),
        P("section", mp),
        P("section", "dp", None, mp),
        P("section", None, mp),
        P("section", mp, "dp"),
        P("section", None),
        P("section", "dp", mp),
        P("section", mp),
        P("section", mp, "dp"),
        P("section", None),
    )
    mpdp = ("mh", "ml", "dp")
    out_specs = (
        P("section", None, "dp", mp, None),
        P("section", None, "dp", mp, None),
        P(None, "dp", None),
        P("section", "dp", mp),
        P("section", mpdp),
        P("section", "dp", None, mp),
        P("section", None, mpdp),
        P("section", mp, "dp"),
        P("section", "dp"),
        P("section", "dp", mp),
        P("section", mpdp),
        P("section", mp, "dp"),
        P("section", "dp"),
    )
    return jax.shard_map(
        per_device, mesh=fine, in_specs=in_specs, out_specs=out_specs, check_vma=False
    )
```

```python
import jax
import jax.numpy as jnp
from jax import lax
from jax.experimental import pallas as pl
from jax.experimental.pallas import tpu as pltpu
from jax.sharding import Mesh
from jax.sharding import PartitionSpec as P

HEAD_SIZE = 72
EPS = 1e-06
MESH = pl.DeviceIdType.MESH
BF16 = jnp.bfloat16
F32 = jnp.float32
GELU_C = 0.7978845608028654
GELU_A = 0.044715
NT = (((1,), (1,)), ((), ()))
TN = (((0,), (0,)), ((), ()))
VMEM_LIMIT = 50 * 1024 * 1024


def dot_nn(a, b):
    return jnp.dot(a, b, preferred_element_type=F32)


def dot_nt(a, b):
    return lax.dot_general(a, b, NT, preferred_element_type=F32)


def dot_tn(a, b):
    return lax.dot_general(a, b, TN, preferred_element_type=F32)


def norm_parts(values):
    center = values - jnp.mean(values, axis=-1, keepdims=True)
    spread = jnp.mean(center * center, axis=-1, keepdims=True)
    rstd = lax.rsqrt(spread + EPS)
    return center * rstd, rstd


def norm_back(grad, normed, rstd, scale):
    dn = grad * (1.0 + scale)
    first = jnp.mean(dn, axis=-1, keepdims=True)
    second = jnp.mean(dn * normed, axis=-1, keepdims=True)
    return (dn - first - normed * second) * rstd


def col_sum(values):
    return jnp.sum(values, axis=0, keepdims=True)


def row_total(low):
    return dot_nn(jnp.ones((16, low.shape[0]), BF16), low)[0:1]


class Group:
    def __init__(self, tokens):
        self.low = lax.axis_size("ml")
        self.size = lax.axis_size("section") * self.low
        self.me = lax.axis_index("section") * self.low + lax.axis_index("ml")
        self.square = self.size == 4
        self.half = (slice(0, tokens // 2), slice(tokens // 2, tokens))

    def device(self, member):
        return (
            lax.div(member, self.low),
            lax.axis_index("dp"),
            lax.axis_index("mh"),
            lax.rem(member, self.low),
        )

    def member(self, step):
        if not self.square:
            return lax.rem(self.me + step, self.size)
        section = lax.rem(lax.axis_index("section") + lax.rem(step, 2), 2)
        low = lax.rem(lax.axis_index("ml") + lax.div(step, 2), 2)
        return section * 2 + low

    def copy(self, src, dst, send_sem, recv_sem, member):
        return pltpu.make_async_remote_copy(
            src_ref=src,
            dst_ref=dst,
            send_sem=send_sem,
            recv_sem=recv_sem,
            device_id=self.device(member),
            device_id_type=MESH,
        )

    def first_copies(self, buf, send_sem, recv_sem):
        steps = (1, 2) if self.square else range(1, self.size)
        mine = buf.at[self.me]
        return [
            self.copy(mine, mine, send_sem.at[step], recv_sem.at[self.me], self.member(step))
            for step in steps
        ]

    def relay_copy(self, buf, send_sem, recv_sem, step):
        rows = buf.at[self.member(step), self.half[step - 1]]
        return self.copy(
            rows, rows, send_sem.at[2 + step], recv_sem.at[3 + step], self.member(3 - step)
        )

    def spread(self, buf, send_sem, recv_sem):
        for copy in self.first_copies(buf, send_sem, recv_sem):
            copy.start()

    def arrive(self, buf, send_sem, recv_sem, step):
        def landed(rows, sem):
            self.copy(rows, rows, send_sem.at[1], sem, self.member(1)).wait_recv()

        if not self.square:

            @pl.when(step > 0)
            def _():
                landed(buf.at[self.member(step)], recv_sem.at[self.member(step)])

            return

        @pl.when(step == 1)
        def _():
            for near in (1, 2):
                landed(buf.at[self.member(near)], recv_sem.at[self.member(near)])
                self.relay_copy(buf, send_sem, recv_sem, near).start()

        @pl.when(step == 3)
        def _():
            for near in (1, 2):
                landed(buf.at[self.member(3), self.half[near - 1]], recv_sem.at[3 + near])

    def spread_sent(self, buf, send_sem, recv_sem):
        for copy in self.first_copies(buf, send_sem, recv_sem):
            copy.wait_send()
        if self.square:
            for step in (1, 2):
                self.relay_copy(buf, send_sem, recv_sem, step).wait_send()

    def straight(self, stage, landing, send_sem, recv_sem, step):
        rows = self.half[step - 1]
        return self.copy(
            stage.at[self.member(step), rows], landing.at[step - 1, rows],
            send_sem.at[step - 1], recv_sem.at[step - 1], self.member(step),
        )

    def corner(self, stage, landing, send_sem, recv_sem, step):
        rows = self.half[step - 1]
        return self.copy(
            stage.at[self.member(3), rows], landing.at[2, rows],
            send_sem.at[1 + step], recv_sem.at[1 + step], self.member(step),
        )

    def summed(self, landing, send_sem, recv_sem, step):
        rows = self.half[2 - step]
        return self.copy(
            landing.at[3, rows], landing.at[step - 1, rows],
            send_sem.at[3 + step], recv_sem.at[3 + step], self.member(step),
        )

    def reduce_copy(self, stage, landing, send_sem, recv_sem, member):
        return self.copy(
            stage.at[member], landing.at[self.me], send_sem.at[member], recv_sem.at[self.me], member
        )

    def give(self, stage, landing, send_sem, recv_sem, step):
        args = (stage, landing, send_sem, recv_sem)
        if not self.square:

            @pl.when(step > 0)
            def _():
                self.reduce_copy(*args, self.member(step)).start()

            return
        for near in (1, 2):

            @pl.when(step == near)
            def _():
                self.straight(*args, near).start()

        @pl.when(step == 3)
        def _():
            for near in (1, 2):
                self.corner(*args, near).start()

    def combine(self, stage, landing, send_sem, recv_sem):
        if not self.square:
            return
        for step in (1, 2):
            rows = self.half[2 - step]
            self.copy(
                landing.at[2, rows], landing.at[2, rows], send_sem.at[0], recv_sem.at[4 - step],
                self.member(1),
            ).wait_recv()
            total = stage[self.member(step), rows].astype(F32) + landing[2, rows].astype(F32)
            landing[3, rows] = total.astype(BF16)
            self.summed(landing, send_sem, recv_sem, step).start()

    def landed_sum(self, own, stage, landing, send_sem, recv_sem):
        args = (stage, landing, send_sem, recv_sem)
        total = own

        def landed(rows, sem):
            self.copy(rows, rows, send_sem.at[0], sem, self.member(1)).wait_recv()

        if self.square:
            for step in (1, 2):
                first, second = self.half[step - 1], self.half[2 - step]
                landed(landing.at[step - 1, first], recv_sem.at[step - 1])
                landed(landing.at[step - 1, second], recv_sem.at[3 + step])
                total = total + landing[step - 1].astype(F32)
            for step in (1, 2):
                self.straight(*args, step).wait_send()
                self.corner(*args, step).wait_send()
                self.summed(landing, send_sem, recv_sem, step).wait_send()
            return total
        for step in range(1, self.size):
            member = self.member(step)
            landed(landing.at[member], recv_sem.at[member])
            total = total + landing[member].astype(F32)
        for step in range(1, self.size):
            self.reduce_copy(*args, self.member(step)).wait_send()
        return total


def load(src, dst, sem):
    copy = pltpu.make_async_copy(src, dst, sem)
    copy.start()
    return [copy]


def flush(pairs, sems):
    copies = [
        pltpu.make_async_copy(src, dst, sems.at[number]) for number, (src, dst) in enumerate(pairs)
    ]
    for copy in copies:
        copy.start()
    return copies


def lane_mask(shape, head):
    lanes = lax.broadcasted_iota(jnp.int32, shape, len(shape) - 1)
    return (lanes >= head * HEAD_SIZE) & (lanes < (head + 1) * HEAD_SIZE)


def row_mask(shape, head):
    rows = lax.broadcasted_iota(jnp.int32, shape, 0)
    return (rows >= head * HEAD_SIZE) & (rows < (head + 1) * HEAD_SIZE)


def stack_heads(block):
    heads = block.shape[-1] // HEAD_SIZE
    zero = jnp.zeros_like(block)
    return jnp.concatenate(
        [jnp.where(lane_mask(block.shape, head), block, zero) for head in range(heads)], axis=0
    )


def identity(size):
    rows = lax.broadcasted_iota(jnp.int32, (size, size), 0)
    cols = lax.broadcasted_iota(jnp.int32, (size, size), 1)
    return jnp.where(rows == cols, 1.0, 0.0).astype(BF16)


def att_fwd_kernel(
    bg,
    hidden_ref, mod_ref, bias_ref, bproj_ref, w_ref,
    middle_ref, normed_out, proj_out, att_out, branch_ref,
    normed_ref, proj_ref, att_ref, out_sem,
    w_buf, wo_buf, stage, landing, w_sem, ag_send, ag_recv, rs_send, rs_recv,
):
    tokens, width = hidden_ref.shape
    group = Group(tokens)
    me, size = group.me, group.size
    part_width = att_ref.shape[-1]
    heads = part_width // HEAD_SIZE
    loads = load(w_ref, w_buf, w_sem.at[0])
    hidden = hidden_ref[...].astype(F32)
    normed, _ = norm_parts(hidden)
    normed_ref[me] = (normed * (1.0 + mod_ref[1:2]) + mod_ref[0:1]).astype(BF16)
    Place().greet()
    group.spread(normed_ref, ag_send, ag_recv)
    bg(0)
    for copy in loads:
        copy.wait()

    def project(step, carry):
        member = group.member(step)
        group.arrive(normed_ref, ag_send, ag_recv, step)
        out = dot_nn(normed_ref[member], w_buf[:, : 3 * part_width]) + bias_ref[...]
        for part in range(3):
            cols = slice(part * part_width, (part + 1) * part_width)
            proj_ref[part, member] = out[:, cols].astype(BF16)
        return carry

    wo_buf[...] = w_buf[:, 3 * part_width :]
    lax.fori_loop(0, size, project, 0)
    bg(1)
    seq = size * tokens
    keys = proj_ref[1].reshape(seq, -1)
    values = proj_ref[2].reshape(seq, -1)

    def attend(member):
        stacked = stack_heads(proj_ref[0, member])
        powered = jnp.exp(dot_nt(stacked, keys) * HEAD_SIZE**-0.5)
        probs = powered * (1.0 / jnp.sum(powered, axis=-1, keepdims=True))
        mixed = dot_nn(probs.astype(BF16), values)
        out = mixed[:tokens]
        for head in range(1, heads):
            part = mixed[head * tokens : (head + 1) * tokens]
            out = jnp.where(lane_mask(part.shape, head), part, out)
        low = out.astype(BF16)
        att_ref[member] = low
        return dot_nt(low, wo_buf[...])

    def send(step, carry):
        @pl.when(step == size)
        def _():
            group.combine(stage, landing, rs_send, rs_recv)
            bg(2)

        member = group.member(size - step)
        stage[member] = attend(member).astype(BF16)
        group.give(stage, landing, rs_send, rs_recv, size - step)
        return carry

    lax.fori_loop(1, size + 1, send, 0)
    group.spread_sent(normed_ref, ag_send, ag_recv)
    flushed = flush(
        [(normed_ref, normed_out), (proj_ref, proj_out), (att_ref, att_out)], out_sem
    )
    bg(3)
    own = stage[me].astype(F32)
    branch = group.landed_sum(own, stage, landing, rs_send, rs_recv) + bproj_ref[...]
    branch_ref[...] = branch
    middle_ref[...] = hidden_ref[...].astype(F32) + mod_ref[2:3] * branch
    bg(4)
    for copy in flushed:
        copy.wait()


def mlp_fwd_kernel(
    bg,
    middle_ref, mod_ref, b1_ref, b2_ref, w1_ref, w2_ref,
    out_ref, normed_out, pre_out, gelu_out, branch_ref,
    normed_ref, pre_ref, gelu_ref, out_sem,
    w1_buf, w2_buf, stage, landing, w_sem, ag_send, ag_recv, rs_send, rs_recv,
):
    group = Group(middle_ref.shape[0])
    me, size = group.me, group.size
    loads = load(w1_ref, w1_buf, w_sem.at[0]) + load(w2_ref, w2_buf, w_sem.at[1])
    normed, _ = norm_parts(middle_ref[...])
    normed_ref[me] = (normed * (1.0 + mod_ref[4:5]) + mod_ref[3:4]).astype(BF16)
    Place().greet()
    group.spread(normed_ref, ag_send, ag_recv)
    bg(0)
    for copy in loads:
        copy.wait()

    def dense(member):
        pre = dot_nn(normed_ref[member], w1_buf[...]) + b1_ref[...]
        pre_ref[member] = pre
        bent = jnp.tanh(GELU_C * (pre + GELU_A * pre * pre * pre))
        low = (0.5 * pre * (1.0 + bent)).astype(BF16)
        gelu_ref[member] = low
        return dot_nt(low, w2_buf[...])

    def send(step, carry):
        @pl.when(step == 1)
        def _():
            bg(1)

        member = group.member(step)
        group.arrive(normed_ref, ag_send, ag_recv, step)
        stage[member] = dense(member).astype(BF16)
        group.give(stage, landing, rs_send, rs_recv, step)
        return carry

    lax.fori_loop(0, size, send, 0)
    group.combine(stage, landing, rs_send, rs_recv)
    bg(2)
    group.spread_sent(normed_ref, ag_send, ag_recv)
    flushed = flush(
        [(normed_ref, normed_out), (pre_ref, pre_out), (gelu_ref, gelu_out)], out_sem
    )
    bg(3)
    own = stage[me].astype(F32)
    branch = group.landed_sum(own, stage, landing, rs_send, rs_recv) + b2_ref[...]
    branch_ref[...] = branch
    out_ref[...] = (middle_ref[...] + mod_ref[5:6] * branch).astype(BF16)
    bg(4)
    for copy in flushed:
        copy.wait()


def weight_grad(lhs_ref, rhs, out_ref, tile):
    def body(index, carry):
        cols = pl.ds(pl.multiple_of(index * tile, tile), tile)
        out_ref[cols, :] = dot_tn(lhs_ref[:, cols], rhs).astype(BF16)
        return carry

    lax.fori_loop(0, lhs_ref.shape[-1] // tile, body, 0)


def mlp_bwd_kernel(
    bg,
    grad_ref, middle_ref, mod_ref, branch_ref, normed_in, pre_in, gelu_in, w1_ref, w2_ref,
    gmid_ref, dw1_out, dw2_out, db1_ref, db2_ref, dmod_ref,
    dw1_ref, dw2_ref, out_sem, normed_ref, pre_ref, gelu_ref, in_sem,
    w1_buf, w2_buf, dbr, dpre, stage, landing, w_sem, ag_send, ag_recv, rs_send, rs_recv,
):
    tokens, width = grad_ref.shape
    group = Group(tokens)
    me, size = group.me, group.size
    loads = load(w2_ref, w2_buf, w_sem.at[1]) + load(pre_in, pre_ref, in_sem.at[0])
    loads += load(w1_ref, w1_buf, w_sem.at[0]) + load(gelu_in, gelu_ref, in_sem.at[1])
    loads += load(normed_in, normed_ref, in_sem.at[2])
    grad = grad_ref[...].astype(F32)
    dbr[me] = (grad * mod_ref[5:6]).astype(BF16)
    Place().greet()
    group.spread(dbr, ag_send, ag_recv)
    bg(0)
    dmod_ref[2:3] = col_sum(grad * branch_ref[...])
    for copy in loads:
        copy.wait()

    def back(member):
        dgelu = dot_nn(dbr[member], w2_buf[...])
        pre = pre_ref[member]
        bent = jnp.tanh(GELU_C * (pre + GELU_A * pre * pre * pre))
        slope = 0.5 * (1.0 + bent) + 0.5 * pre * (1.0 - bent * bent) * (
            GELU_C * (1.0 + 3.0 * GELU_A * pre * pre)
        )
        low = (dgelu * slope).astype(BF16)
        dpre[member] = low
        return dot_nt(low, w1_buf[...])

    stage[me] = back(me).astype(BF16)
    bg(1)

    def send(step, carry):
        member = group.member(step)
        group.arrive(dbr, ag_send, ag_recv, step)
        stage[member] = back(member).astype(BF16)
        group.give(stage, landing, rs_send, rs_recv, step)
        return carry

    lax.fori_loop(1, size, send, 0)
    group.combine(stage, landing, rs_send, rs_recv)
    bg(2)
    seq = size * tokens
    dpre_all = dpre[...].reshape(seq, -1)
    gelu_all = gelu_ref[...].reshape(seq, -1)
    db1_ref[...] = row_total(dpre_all)
    db2_ref[...] = row_total(dbr[...].reshape(seq, -1))
    weight_grad(normed_ref.reshape(seq, width), dpre_all, dw1_ref, 384)
    weight_grad(dbr.reshape(seq, width), gelu_all, dw2_ref, 384)
    flushed = flush([(dw1_ref, dw1_out), (dw2_ref, dw2_out)], out_sem)
    group.spread_sent(dbr, ag_send, ag_recv)
    bg(3)
    total = group.landed_sum(stage[me].astype(F32), stage, landing, rs_send, rs_recv)
    normed, rstd = norm_parts(middle_ref[...])
    dmod_ref[0:1] = col_sum(total)
    dmod_ref[1:2] = col_sum(total * normed)
    gmid_ref[...] = norm_back(total, normed, rstd, mod_ref[4:5]) + grad_ref[...].astype(F32)
    bg(4)
    for copy in flushed:
        copy.wait()


def att_bwd_kernel(
    bg,
    gmid_ref, hidden_ref, mod_ref, branch_ref, normed_in, proj_in, att_in, w_ref,
    gin_ref, dw_out, dbqkv_ref, dbproj_ref, dmod_ref,
    dw_ref, out_sem, normed_ref, proj_ref, att_ref, in_sem,
    w_buf, wo_buf, dba, dproj, dkey, dval, stage, landing, w_sem, ag_send, ag_recv, rs_send, rs_recv,
):
    tokens, width = gmid_ref.shape
    group = Group(tokens)
    me, size = group.me, group.size
    seq = size * tokens
    part_width = att_in.shape[-1]
    heads = part_width // HEAD_SIZE
    loads = load(proj_in, proj_ref, in_sem.at[0]) + load(w_ref, w_buf, w_sem.at[0])
    loads += load(att_in, att_ref, in_sem.at[1]) + load(normed_in, normed_ref, in_sem.at[2])
    gmid = gmid_ref[...]
    dba[me] = (gmid * mod_ref[2:3]).astype(BF16)
    Place().greet()
    group.spread(dba, ag_send, ag_recv)
    bg(0)
    dmod_ref[2:3] = col_sum(gmid * branch_ref[...])
    for copy in loads:
        copy.wait()
    keys = proj_ref[1].reshape(seq, part_width)
    values = proj_ref[2].reshape(seq, part_width)
    keys_t = dot_nt(identity(part_width), keys).astype(BF16)
    dkey[...] = jnp.zeros_like(dkey)
    dval[...] = jnp.zeros_like(dval)
    wo_buf[...] = w_buf[:, 3 * part_width :]

    def back(step, carry):
        @pl.when(step == 1)
        def _():
            bg(1)

        member = group.member(step)
        group.arrive(dba, ag_send, ag_recv, step)
        datt = dot_nn(dba[member], wo_buf[...]).astype(BF16)
        datt_st = stack_heads(datt)
        query_st = stack_heads(proj_ref[0, member])
        powered = jnp.exp(dot_nt(keys, query_st) * HEAD_SIZE**-0.5)
        probs = powered * (1.0 / jnp.sum(powered, axis=0, keepdims=True))
        dval[...] += dot_nn(probs.astype(BF16), datt_st)
        dprobs = dot_nt(values, datt_st)
        dscore = (probs * (dprobs - jnp.sum(probs * dprobs, axis=0, keepdims=True))).astype(BF16)
        dkey[...] += dot_nn(dscore, query_st)
        dq_t = dot_nn(keys_t, dscore)
        picked = dq_t[:, :tokens]
        for head in range(1, heads):
            part = dq_t[:, head * tokens : (head + 1) * tokens]
            picked = jnp.where(row_mask(part.shape, head), part, picked)
        low = (picked * HEAD_SIZE**-0.5).astype(BF16)
        dproj[member, :, :part_width] = dot_nt(identity(tokens), low).astype(BF16)
        return carry

    lax.fori_loop(0, size, back, 0)
    for member in range(size):
        rows = slice(member * tokens, (member + 1) * tokens)
        dproj[member, :, part_width : 2 * part_width] = (dkey[rows] * HEAD_SIZE**-0.5).astype(BF16)
        dproj[member, :, 2 * part_width :] = dval[rows].astype(BF16)

    def partial_rows(member):
        return dot_nt(dproj[member], w_buf[:, : 3 * part_width])

    def send(step, carry):
        member = group.member(size - step)
        stage[member] = partial_rows(member).astype(BF16)
        group.give(stage, landing, rs_send, rs_recv, size - step)
        return carry

    lax.fori_loop(1, size + 1, send, 0)
    group.combine(stage, landing, rs_send, rs_recv)
    bg(2)
    grads = dproj[...].reshape(seq, -1)
    dbqkv_ref[...] = row_total(grads)
    dbproj_ref[...] = row_total(dba[...].reshape(seq, width))
    mixed = att_ref[...].reshape(seq, part_width)
    normed_rows, dba_rows = normed_ref.reshape(seq, width), dba.reshape(seq, width)

    def weights(index, carry):
        cols = pl.ds(pl.multiple_of(index * 128, 128), 128)
        dw_ref[cols, : 3 * part_width] = dot_tn(normed_rows[:, cols], grads).astype(BF16)
        dw_ref[cols, 3 * part_width :] = dot_tn(dba_rows[:, cols], mixed).astype(BF16)
        return carry

    lax.fori_loop(0, width // 128, weights, 0)
    flushed = flush([(dw_ref, dw_out)], out_sem)
    group.spread_sent(dba, ag_send, ag_recv)
    bg(3)
    total = group.landed_sum(stage[me].astype(F32), stage, landing, rs_send, rs_recv)
    hidden = hidden_ref[...].astype(F32)
    normed, rstd = norm_parts(hidden)
    dmod_ref[0:1] = col_sum(total)
    dmod_ref[1:2] = col_sum(total * normed)
    gin = norm_back(total, normed, rstd, mod_ref[1:2]) + gmid_ref[...]
    gin_ref[...] = gin.astype(BF16)
    bg(4)
    for copy in flushed:
        copy.wait()


class Place:
    def __init__(self):
        self.section, self.dp = lax.axis_index("section"), lax.axis_index("dp")
        self.high, self.low = lax.axis_index("mh"), lax.axis_index("ml")
        self.n_dp, self.n_low = lax.axis_size("dp"), lax.axis_size("ml")
        self.total = 4 * self.n_dp * self.n_low
        self.me = ((self.section * self.n_dp + self.dp) * 2 + self.high) * self.n_low + self.low

    def unflatten(self, number):
        low = lax.rem(number, self.n_low)
        rest = lax.div(number, self.n_low)
        high, rest = lax.rem(rest, 2), lax.div(rest, 2)
        return lax.div(rest, self.n_dp), lax.rem(rest, self.n_dp), high, low

    def greet(self):
        barrier = pltpu.get_barrier_semaphore()
        others = []
        for sec in range(2):
            for step in range(self.n_low):
                if sec or step:
                    section = lax.rem(self.section + sec, 2)
                    others.append((section, self.dp, self.high, lax.rem(self.low + step, self.n_low)))
        for sec in range(2):
            others.append(self.plane(sec, 1 - self.high))
        for step in range(1, self.n_dp // 2):
            others.append((self.section, self.same_core(step), self.high, self.low))
        others.append(self.core_mate())
        for device in others:
            pl.semaphore_signal(barrier, inc=1, device_id=device, device_id_type=MESH)
        pl.semaphore_wait(barrier, len(others))

    def role(self, layer, number):
        same = (self.section == layer) if number < 2 else (self.section != layer)
        return same & ((self.high == layer) if number % 2 == 0 else (self.high != layer))

    def role_device(self, layer, number):
        section = layer if number < 2 else 1 - layer
        return self.plane(section, layer if number % 2 == 0 else 1 - layer)

    def greet_all(self):
        barrier = pltpu.get_barrier_semaphore()

        def body(step, carry):
            pl.semaphore_signal(
                barrier,
                inc=1,
                device_id=self.unflatten(lax.rem(self.me + step, self.total)),
                device_id_type=MESH,
            )
            return carry

        lax.fori_loop(1, self.total, body, 0)
        pl.semaphore_wait(barrier, self.total - 1)

    def copy(self, src, dst, send_sem, recv_sem, device):
        return pltpu.make_async_remote_copy(
            src_ref=src,
            dst_ref=dst,
            send_sem=send_sem,
            recv_sem=recv_sem,
            device_id=device,
            device_id_type=MESH,
        )

    def core_mate(self):
        return (self.section, self.dp + 1 - 2 * lax.rem(self.dp, 2), self.high, self.low)

    def same_core(self, step):
        return lax.rem(self.dp + 2 * step, self.n_dp)

    def plane(self, section, high):
        return (section, self.dp, high, self.low)

    def exchange(self, pick, landing, send_sem, recv_sem):
        landing[self.me] = pick((self.section, self.dp, self.high, self.low))[...]

        def copy(number):
            device = self.unflatten(number)
            return self.copy(
                pick(device), landing.at[self.me], send_sem.at[number], recv_sem.at[self.me], device
            )

        def start(step, carry):
            copy(lax.rem(self.me + step, self.total)).start()
            return carry

        def finish(step, carry):
            number = lax.rem(self.me + step, self.total)
            device = self.unflatten(number)
            self.copy(
                landing.at[number], landing.at[number], send_sem.at[number], recv_sem.at[number], device
            ).wait_recv()
            copy(number).wait_send()
            return carry

        lax.fori_loop(1, self.total, start, 0)
        return lambda: lax.fori_loop(1, self.total, finish, 0)


VM = pl.BlockSpec(memory_space=pltpu.VMEM)
ANY = pl.BlockSpec(memory_space=pltpu.HBM)
DMA = pltpu.SemaphoreType.DMA


def by_rows(count, body):
    block = count // 9 if count % 144 == 0 else count

    def step(index, carry):
        body(pl.ds(pl.multiple_of(index * block, 16), block))
        return carry

    lax.fori_loop(0, count // block, step, 0)


class Handle:
    def __init__(self, shape, dtype):
        self.shape, self.dtype = shape, dtype
        self.array = None
        self.ref = None


class Task:
    inputs = ()
    outs = ()
    scratch = ()
    handles = ()


class Collect(Task):
    def __init__(self, item, layer, handle):
        self.layer, self.handle = layer, handle
        self.inputs = ((item, VM),)
        self.handles = (handle,)
        self.chunk = item.shape[0]
        self.scratch = (DMA((2,)), DMA, DMA)

    def run(self, phase, refs):
        (item,), _, (send, recv, own) = refs
        place = Place()
        source = item
        rows = self.handle.ref.at[pl.ds(pl.multiple_of(place.dp * self.chunk, 16), self.chunk)]

        def to(number, role):
            return place.copy(
                source, rows, send.at[number], recv, place.role_device(self.layer, role)
            )

        targets = {0: (1,), 1: (2, 3), 2: (), 3: ()}
        for role in range(4):

            @pl.when(place.role(self.layer, role))
            def _():
                if phase == "a":
                    for number, target in enumerate(targets[role]):
                        to(number, target).start()
                    if role == 0:
                        pltpu.make_async_copy(source, rows, own).start()
                if phase == "b":
                    if role == 0:
                        pltpu.make_async_copy(source, rows, own).wait()
                    else:
                        place.copy(
                            rows, rows, send.at[0], recv, place.role_device(self.layer, 0)
                        ).wait_recv()
                if phase == "c":
                    for number, target in enumerate(targets[role]):
                        to(number, target).wait_send()


class Widen(Task):
    def __init__(self, handle):
        self.handle = handle
        self.handles = (handle,)
        chips = lax.axis_size("dp") // 2
        self.scratch = (DMA((chips,)),) * 4

    def rows(self, index):
        chunk = self.handle.shape[0] // lax.axis_size("dp")
        return self.handle.ref.at[pl.ds(pl.multiple_of(index * chunk, 16), chunk)]

    def run(self, phase, refs):
        _, _, (x_send, x_recv, c_send, c_recv) = refs
        place = Place()
        chips = place.n_dp // 2

        def across(step):
            return place.copy(
                self.rows(place.dp), self.rows(place.dp), x_send.at[step], x_recv.at[step],
                (place.section, place.same_core(step), place.high, place.low),
            )

        def landed(step):
            held = self.rows(place.same_core(chips - step))
            return place.copy(
                held, held, x_send.at[step], x_recv.at[step],
                (place.section, place.same_core(step), place.high, place.low),
            )

        def to_mate(step):
            held = self.rows(place.same_core(step))
            return place.copy(held, held, c_send.at[step], c_recv.at[step], place.core_mate())

        def from_mate(step):
            held = self.rows(lax.rem(place.core_mate()[1] + 2 * step, place.n_dp))
            return place.copy(held, held, c_send.at[step], c_recv.at[step], place.core_mate())

        if phase == "a":
            for step in range(1, chips):
                across(step).start()
            to_mate(0).start()
        if phase == "b":
            for step in range(1, chips):
                landed(step).wait_recv()
                to_mate(chips - step).start()
        if phase == "c":
            for step in range(chips):
                from_mate(step).wait_recv()
                to_mate(step).wait_send()
                if step:
                    across(step).wait_send()


class Narrow(Task):
    def __init__(self, grad):
        n_dp = lax.axis_size("dp")
        chips = n_dp // 2
        self.chunk = grad.shape[0] // n_dp
        block = (chips, self.chunk, grad.shape[1])
        self.inputs = ((grad, ANY),)
        self.outs = (((self.chunk, grad.shape[1]), BF16, VM),)
        self.scratch = (pltpu.VMEM(block, BF16),) * 3 + (DMA((chips,)),) * 5

    def run(self, phase, refs):
        (grad,), (out,), scratch = refs
        own, near, far, own_sem, c_send, c_recv, x_send, x_recv = scratch
        place = Place()
        chips = place.n_dp // 2

        def rows(index):
            return grad.at[pl.ds(pl.multiple_of(index * self.chunk, 16), self.chunk)]

        def to_mate(step):
            other = lax.rem(place.core_mate()[1] + 2 * step, place.n_dp)
            return place.copy(
                rows(other), near.at[step], c_send.at[step], c_recv.at[step], place.core_mate()
            )

        def load_own(step):
            return pltpu.make_async_copy(
                rows(place.same_core(step)), own.at[step], own_sem.at[step]
            )

        def across(step):
            return place.copy(
                own.at[step], far.at[step], x_send.at[step], x_recv.at[step],
                (place.section, place.same_core(step), place.high, place.low),
            )

        order = list(range(1, chips)) + [0]
        if phase == "a":
            for step in order:
                to_mate(step).start()
                load_own(step).start()
        if phase == "b":
            for step in order:
                load_own(step).wait()
                to_mate(step).wait_recv()

                def add(rows):
                    total = own[step, rows].astype(F32) + near[step, rows].astype(F32)
                    own[step, rows] = total.astype(BF16)

                by_rows(self.chunk, add)
                if step:
                    across(step).start()
        if phase == "c":
            for step in range(1, chips):
                across(step).wait_recv()

            def add(rows):
                total = own[0, rows].astype(F32)
                for step in range(1, chips):
                    total = total + far[step, rows].astype(F32)
                out[rows] = total.astype(BF16)

            by_rows(self.chunk, add)
            for step in range(chips):
                to_mate(step).wait_send()
                if step:
                    across(step).wait_send()


class Settle(Task):
    def __init__(self, part, layer, held=None, into=None):
        self.layer = layer
        self.held = held
        self.into = into
        self.inputs = () if held else ((part, ANY),)
        self.outs = () if into else ((part.shape, F32, VM),)
        self.scratch = (
            pltpu.VMEM((2,) + part.shape, BF16), pltpu.VMEM(part.shape, BF16),
            DMA((2,)), DMA((3,)), DMA,
        )

    def run(self, phase, refs):
        ins, outs, (land, temp, send, recv, own_sem) = refs
        (out,) = self.into.refs[1] if self.into else outs
        part = self.held() if self.held else ins[0]
        place = Place()
        layer = self.layer

        def to(src, dst, s, r, role):
            return place.copy(src, dst, send.at[s], recv.at[r], place.role_device(layer, role))

        def direct(role):
            if role == 2:
                return to(part, temp, 0, 2, 0)
            return to(part, land.at[0], 0, 0, 0 if role == 1 else 1)

        def relay():
            return to(temp, land.at[1], 1, 1, 1)

        for role in range(4):

            @pl.when(place.role(layer, role))
            def _():
                if phase == "z" and role == 1:
                    direct(role).start()
                if phase == "a":
                    if role > 1:
                        direct(role).start()
                    if role == 0:
                        pltpu.make_async_copy(part, land.at[1], own_sem).start()
                if phase == "b":
                    if role == 0:
                        to(temp, temp, 0, 2, 0).wait_recv()
                        relay().start()
                    if role > 1:
                        direct(role).wait_send()
                if phase == "s":
                    if role == 0:
                        relay().wait_send()
                    if role == 1:
                        direct(role).wait_send()
                if phase == "c":
                    if role == 0:
                        pltpu.make_async_copy(part, land.at[1], own_sem).wait()
                    if role < 2:
                        to(land.at[0], land.at[0], 0, 0, role).wait_recv()
                    if role == 1:
                        to(land.at[1], land.at[1], 0, 1, 1).wait_recv()
                    if role < 2:

                        def add(rows):
                            out[rows] = land[0, rows].astype(F32) + land[1, rows].astype(F32)

                        by_rows(part.shape[0], add)


class Deliver(Task):
    def __init__(self, rows, layer, into=None):
        self.layer = layer
        self.into = into
        self.inputs = ((rows, VM),)
        self.outs = () if into else (((2,) + rows.shape, rows.dtype, VM),)
        self.scratch = (pltpu.VMEM(rows.shape, rows.dtype), DMA((2,)), DMA((3,)))

    def run(self, phase, refs):
        (rows,), outs, (temp, send, recv) = refs
        (out,) = self.into.refs[1] if self.into else outs
        place = Place()
        layer = self.layer

        def to(src, dst, s, r, role):
            return place.copy(src, dst, send.at[s], recv.at[r], place.role_device(layer, role))

        def direct(role):
            if role == 2:
                return to(rows, temp, 0, 2, 0)
            return to(rows, out.at[1 - layer], 0, 0, 0 if role == 1 else 1)

        def relay():
            return to(temp, out.at[layer], 1, 1, 1)

        for role in range(4):

            @pl.when(place.role(layer, role))
            def _():
                if phase == "z" and role == 1:
                    direct(role).start()
                if phase == "a":
                    if role > 1:
                        direct(role).start()
                    if role == 0:
                        out[layer] = rows[...]
                if phase == "b" and role == 0:
                    to(temp, temp, 0, 2, 0).wait_recv()
                    relay().start()
                if phase == "c":
                    if role == 0:
                        relay().wait_send()
                    else:
                        direct(role).wait_send()
                    if role < 2:
                        to(out.at[1 - layer], out.at[1 - layer], 0, 0, role).wait_recv()
                    if role == 1:
                        to(out.at[layer], out.at[layer], 0, 1, 1).wait_recv()


class Tokens(Task):
    def __init__(self, rows):
        self.inputs = ((rows, VM),)
        self.outs = ((rows.shape[1:], rows.dtype, VM),)
        self.scratch = (DMA, DMA((2,)))

    def run(self, phase, refs):
        (rows,), (out,), (send, recv) = refs
        place = Place()
        half = rows.shape[1] // 2
        parts = (slice(0, half), slice(half, 2 * half))

        def copy(part, section):
            return place.copy(
                rows.at[1 - place.high, parts[part]], out.at[parts[part]], send, recv.at[part],
                place.plane(section, 1 - place.high),
            )

        @pl.when(place.section == place.high)
        def _():
            if phase == "a":
                copy(0, place.section).start()
                out[...] = rows[place.high]
            if phase == "c":
                copy(0, place.section).wait_send()

        @pl.when(place.section != place.high)
        def _():
            if phase == "a":
                copy(1, 1 - place.section).start()
            if phase == "c":
                copy(1, 1 - place.section).wait_send()
                copy(0, place.section).wait_recv()
                copy(1, place.section).wait_recv()


def launch(kernel, operands, outs, scratch, schedule, cid, name):
    tasks = []
    for point in schedule:
        for task, _ in point:
            if task not in tasks:
                tasks.append(task)
    operands, outs, scratch = list(operands), list(outs), list(scratch)
    n_in, n_out, n_scratch = len(operands), len(outs), len(scratch)
    spans = []
    for task in tasks:
        spans.append((len(operands), len(outs), len(scratch)))
        operands += task.inputs
        outs += task.outs
        scratch += task.scratch
    handles = []
    for task in tasks:
        for handle in task.handles:
            if handle not in handles:
                handles.append(handle)
    aliases = {}
    first_handle = len(outs)
    for handle in handles:
        if handle.array is not None:
            aliases[len(operands)] = len(outs)
            operands.append((handle.array, ANY))
        outs.append((handle.shape, handle.dtype, ANY))

    def body(*refs):
        ins = refs[: len(operands)]
        results = refs[len(operands) : len(operands) + len(outs)]
        rest = refs[len(operands) + len(outs) :]
        for number, handle in enumerate(handles):
            handle.ref = results[first_handle + number]
        views = []
        for task, (a, b, c) in zip(tasks, spans):
            views.append(
                (
                    ins[a : a + len(task.inputs)],
                    results[b : b + len(task.outs)],
                    rest[c : c + len(task.scratch)],
                )
            )
            task.refs = views[-1]

        def bg(point):
            for task, phase in schedule[point]:
                task.run(phase, task.refs)

        kernel(bg, *ins[:n_in], *results[:n_out], *rest[:n_scratch])

    done = pl.pallas_call(
        body,
        out_shape=tuple(jax.ShapeDtypeStruct(shape, dtype) for shape, dtype, _ in outs),
        in_specs=[spec for _, spec in operands],
        out_specs=tuple(spec for _, _, spec in outs),
        scratch_shapes=scratch,
        input_output_aliases=aliases,
        compiler_params=pltpu.CompilerParams(
            collective_id=cid, has_side_effects=True, vmem_limit_bytes=VMEM_LIMIT
        ),
        name=name,
    )(*[array for array, _ in operands])
    for number, handle in enumerate(handles):
        handle.array = done[first_handle + number]
        handle.ref = None
    for task, (_, b, _) in zip(tasks, spans):
        task.results = done[b : b + len(task.outs)]
    return done[:n_out]


def group_size():
    return lax.axis_size("section") * lax.axis_size("ml")


def comm_scratch(tokens, width):
    size = group_size()
    return [pltpu.VMEM((size, tokens, width), BF16)] * 2, [DMA((max(size, 6),))] * 4


def att_fwd(hidden, mod, bias, bproj, w, schedule, cid):
    tokens, width = hidden.shape
    size = group_size()
    part_width = width // size
    bufs, sems = comm_scratch(tokens, width)
    return launch(
        att_fwd_kernel,
        [(hidden, VM), (mod, VM), (bias, VM), (bproj, VM), (w.array, ANY)],
        [
            ((tokens, width), F32, VM),
            ((size, tokens, width), BF16, ANY),
            ((3, size, tokens, part_width), BF16, ANY),
            ((size, tokens, part_width), BF16, ANY),
            ((tokens, width), F32, VM),
        ],
        [
            pltpu.VMEM((size, tokens, width), BF16),
            pltpu.VMEM((3, size, tokens, part_width), BF16),
            pltpu.VMEM((size, tokens, part_width), BF16),
            DMA((3,)),
        ]
        + [pltpu.VMEM(w.shape, BF16), pltpu.VMEM((width, part_width), BF16)]
        + bufs
        + [DMA((1,))]
        + sems,
        schedule,
        cid,
        "att_fwd",
    )


def mlp_fwd(middle, mod, b1, b2, w1, w2, schedule, cid):
    tokens, width = middle.shape
    size = group_size()
    units = w1.shape[1]
    bufs, sems = comm_scratch(tokens, width)
    return launch(
        mlp_fwd_kernel,
        [(middle, VM), (mod, VM), (b1, VM), (b2, VM), (w1.array, ANY), (w2.array, ANY)],
        [
            ((tokens, width), BF16, VM),
            ((size, tokens, width), BF16, ANY),
            ((size, tokens, units), F32, ANY),
            ((size, tokens, units), BF16, ANY),
            ((tokens, width), F32, VM),
        ],
        [
            pltpu.VMEM((size, tokens, width), BF16),
            pltpu.VMEM((size, tokens, units), F32),
            pltpu.VMEM((size, tokens, units), BF16),
            DMA((3,)),
        ]
        + [pltpu.VMEM(w1.shape, BF16)] * 2 + bufs + [DMA((2,))] + sems,
        schedule,
        cid,
        "mlp_fwd",
    )


def mlp_bwd(grad, middle, mod, branch, normed, pre, gelu, w1, w2, schedule, cid):
    tokens, width = middle.shape
    size = group_size()
    units = w1.shape[1]
    bufs, sems = comm_scratch(tokens, width)
    ins = (grad, middle, mod, branch, normed, pre, gelu)
    return launch(
        mlp_bwd_kernel,
        [(array, spec) for array, spec in zip(ins, [VM] * 4 + [ANY] * 3)]
        + [(w1.array, ANY), (w2.array, ANY)],
        [
            ((tokens, width), F32, VM),
            (w1.shape, BF16, ANY),
            (w2.shape, BF16, ANY),
            ((1, units), F32, VM),
            ((1, width), F32, VM),
            ((3, width), F32, VM),
        ],
        [pltpu.VMEM(w1.shape, BF16)] * 2
        + [
            DMA((2,)),
            pltpu.VMEM(normed.shape, BF16),
            pltpu.VMEM(pre.shape, F32),
            pltpu.VMEM(gelu.shape, BF16),
            DMA((3,)),
        ]
        + [pltpu.VMEM(w1.shape, BF16)] * 2
        + [pltpu.VMEM((size, tokens, width), BF16), pltpu.VMEM((size, tokens, units), BF16)]
        + bufs
        + [DMA((2,))]
        + sems,
        schedule,
        cid,
        "mlp_bwd",
    )


def att_bwd(gmid, hidden, mod, branch, normed, proj, att, w, schedule, cid):
    tokens, width = gmid.shape
    size = group_size()
    part_width = width // size
    bufs, sems = comm_scratch(tokens, width)
    seq = size * tokens
    ins = (gmid, hidden, mod, branch, normed, proj, att)
    return launch(
        att_bwd_kernel,
        [(array, spec) for array, spec in zip(ins, [VM] * 4 + [ANY] * 3)] + [(w.array, ANY)],
        [
            ((tokens, width), BF16, VM),
            (w.shape, BF16, ANY),
            ((1, 3 * part_width), F32, VM),
            ((1, width), F32, VM),
            ((3, width), F32, VM),
        ],
        [
            pltpu.VMEM(w.shape, BF16),
            DMA((1,)),
            pltpu.VMEM(normed.shape, BF16),
            pltpu.VMEM(proj.shape, BF16),
            pltpu.VMEM(att.shape, BF16),
            DMA((3,)),
            pltpu.VMEM(w.shape, BF16),
            pltpu.VMEM((width, part_width), BF16),
            pltpu.VMEM((size, tokens, width), BF16),
            pltpu.VMEM((size, tokens, 3 * part_width), BF16),
            pltpu.VMEM((seq, part_width), F32),
            pltpu.VMEM((seq, part_width), F32),
        ]
        + bufs
        + [DMA((1,))]
        + sems,
        schedule,
        cid,
        "att_bwd",
    )


def prologue_kernel(
    bg,
    cond_ref, wada_ref, bada_ref, bias_ref,
    modul_ref, act_ref, bias_out,
    cond_land, share, land, cond_send, cond_recv, mod_send, mod_recv, b_send, b_recv,
):
    place = Place()
    section, dp, high = place.section, place.dp, place.high
    place.greet_all()

    def spread(step):
        other = lax.rem(dp + step, place.n_dp)
        return place.copy(
            cond_ref.at[other], cond_land.at[dp], cond_send.at[step], cond_recv.at[dp],
            (section, other, high, place.low),
        )

    def spread_wait(step):
        other = lax.rem(dp + step, place.n_dp)
        return place.copy(
            cond_land.at[other], cond_land.at[other], cond_send.at[step], cond_recv.at[other],
            (section, other, high, place.low),
        )

    cond_land[dp] = cond_ref[dp]
    for step in range(1, place.n_dp):
        spread(step).start()

    def bias_copy(target):
        return place.copy(
            bias_ref, bias_out.at[section], b_send.at[target], b_recv.at[section],
            place.plane(high, target),
        )

    here = section == high
    for target in range(2):

        @pl.when(jnp.logical_not(here & (high == target)))
        def _():
            bias_copy(target).start()

    @pl.when(here)
    def _():
        bias_out[section] = bias_ref[...]

    bg(0)
    for step in range(1, place.n_dp):
        spread_wait(step).wait_recv()
    parts = [cond_land[index] for index in range(place.n_dp)]
    act = jax.nn.silu(jnp.concatenate(parts, axis=0)).astype(BF16)
    act_ref[...] = act
    bias = jnp.where(dp == 0, bada_ref[...], 0.0)
    product = dot_nn(act, wada_ref[...])
    for row in range(2 * place.n_dp):
        share[row] = product[row : row + 1] + bias
    finish = place.exchange(
        lambda device: share.at[device[1] * 2 + device[2]], land, mod_send, mod_recv
    )
    bg(1)
    bg(2)
    finish()
    for layer in range(2):
        for part in range(2 * place.n_low):
            total = land[layer * place.n_dp * 2 * place.n_low + part]
            for index in range(1, place.n_dp):
                total = total + land[(layer * place.n_dp + index) * 2 * place.n_low + part]
            modul_ref[layer * 2 * place.n_low + part] = total
    bg(3)
    for step in range(1, place.n_dp):
        spread(step).wait_send()
    for target in range(2):

        @pl.when(jnp.logical_not(here & (high == target)))
        def _():
            bias_copy(target).wait_send()

        @pl.when(jnp.logical_not(here & (section == target)))
        def _():
            place.copy(
                bias_out.at[target], bias_out.at[target], b_send.at[0], b_recv.at[target],
                place.plane(section, 1 - high),
            ).wait_recv()

    bg(4)


def prologue(cond, wada, bada, bias, schedule, cid):
    n_dp, _, chunk = cond.shape
    n_mp = 2 * lax.axis_size("ml")
    total = 2 * n_dp * n_mp
    share = wada.shape[1]
    return launch(
        prologue_kernel,
        [(cond, VM), (wada, VM), (bada, VM), (bias, VM)],
        [
            ((2 * n_mp, 1, share), F32, VM),
            ((2 * n_dp, chunk), BF16, VM),
            ((2,) + bias.shape, F32, VM),
        ],
        [
            pltpu.VMEM((n_dp, 2, chunk), F32),
            pltpu.VMEM((2 * n_dp, 1, share), F32),
            pltpu.VMEM((total, 1, share), F32),
            DMA((n_dp,)),
            DMA((n_dp,)),
            DMA((total,)),
            DMA((total,)),
            DMA((2,)),
            DMA((2,)),
        ],
        schedule,
        cid,
        "prologue",
    )


def epilogue_kernel(
    bg,
    dmod_ref, wada_ref, dbias_ref,
    dmod_out, gbada_ref, gact_ref, gbias_ref,
    mod_land, act_stage, act_land, bias_land, bias_stage, bias_final,
    mod_send, mod_recv, act_send, act_recv, d_send, d_recv, b_send, b_recv,
):
    place = Place()
    section, dp, high = place.section, place.dp, place.high
    place.greet_all()
    finish_mod = place.exchange(
        lambda device: dmod_ref.at[(device[0] * 2 + device[2]) * place.n_low + device[3]],
        mod_land, mod_send, mod_recv,
    )

    def spread(step):
        other = lax.rem(dp + step, place.n_dp)
        return place.copy(
            dbias_ref, bias_land.at[dp], d_send.at[step], d_recv.at[dp],
            (section, other, high, place.low),
        )

    for step in range(1, place.n_dp):
        spread(step).start()
    bg(0)
    finish_mod()
    parts = 2 * place.n_low
    latents = []
    for index in range(place.n_dp):
        for micro in range(2):
            total = 0.0
            for sec in range(2):
                for low in range(place.n_low):
                    number = ((sec * place.n_dp + index) * 2 + micro) * place.n_low + low
                    total = total + mod_land[number]
            latents.append(total)
    dmod = jnp.concatenate(latents, axis=0).astype(BF16)
    back = dot_nt(dmod, wada_ref[...])
    for index in range(place.n_dp):
        act_stage[index] = back[2 * index : 2 * index + 2]
    finish_act = place.exchange(lambda device: act_stage.at[device[1]], act_land, act_send, act_recv)
    bias_sum = dbias_ref[...]
    for step in range(1, place.n_dp):
        other = lax.rem(dp + step, place.n_dp)
        place.copy(
            bias_land.at[other], bias_land.at[other], d_send.at[step], d_recv.at[other],
            (section, other, high, place.low),
        ).wait_recv()
        bias_sum = bias_sum + bias_land[other]
    bias_stage[...] = bias_sum

    def settle(layer):
        return place.copy(
            bias_stage.at[layer], bias_final.at[high], b_send.at[layer], b_recv.at[high],
            place.plane(layer, section),
        )

    for layer in range(2):
        here = (section == layer) & (high == section)

        @pl.when(here)
        def _():
            bias_final[high] = bias_stage[layer]

        @pl.when(jnp.logical_not(here))
        def _():
            settle(layer).start()

    bg(1)
    gbada_ref[...] = col_sum(dmod.astype(F32))
    dmod_out[...] = dmod
    bg(2)
    finish_act()
    for index in range(place.n_dp):
        total = 0.0
        for sec in range(2):
            for part in range(parts):
                total = total + act_land[(sec * place.n_dp + index) * parts + part]
        gact_ref[index] = total
    bg(3)
    for half in range(2):
        here = (section == high) & (high == half)

        @pl.when(jnp.logical_not(here))
        def _():
            place.copy(
                bias_final.at[half], bias_final.at[half], b_send.at[0], b_recv.at[half],
                place.plane(high, half),
            ).wait_recv()

    gbias_ref[...] = bias_final[0] + bias_final[1]
    for layer in range(2):

        @pl.when(jnp.logical_not((section == layer) & (high == section)))
        def _():
            settle(layer).wait_send()

    for step in range(1, place.n_dp):
        spread(step).wait_send()
    bg(4)


def epilogue(dmod, wada, dbias, schedule, cid):
    n_dp, n_mp = lax.axis_size("dp"), 2 * lax.axis_size("ml")
    total = 2 * n_dp * n_mp
    chunk, share = wada.shape
    row = dbias.shape[1:]
    return launch(
        epilogue_kernel,
        [(dmod, VM), (wada, VM), (dbias, VM)],
        [
            ((2 * n_dp, share), BF16, VM),
            ((1, share), F32, VM),
            ((n_dp, 2, chunk), F32, VM),
            (row, F32, VM),
        ],
        [
            pltpu.VMEM((total, 1, share), F32),
            pltpu.VMEM((n_dp, 2, chunk), F32),
            pltpu.VMEM((total, 2, chunk), F32),
            pltpu.VMEM((n_dp,) + dbias.shape, F32),
            pltpu.VMEM(dbias.shape, F32),
            pltpu.VMEM((2,) + row, F32),
            DMA((total,)),
            DMA((total,)),
            DMA((total,)),
            DMA((total,)),
            DMA((n_dp,)),
            DMA((n_dp,)),
            DMA((2,)),
            DMA((2,)),
        ],
        schedule,
        cid,
        "epilogue",
    )


def per_device(
    latents_in, condition, cotangent,
    modulation_weight, modulation_bias, query_key_value_weight, query_value_bias,
    output_proj_weight, output_proj_bias, first_dense_weight, first_dense_bias,
    second_dense_weight, second_dense_bias,
):
    dp = lax.axis_index("dp")
    n_dp, n_low = lax.axis_size("dp"), lax.axis_size("ml")
    n_mp = 2 * n_low
    width = latents_in.shape[-1]
    rows = modulation_weight.shape[1]
    cols = modulation_weight.shape[2]
    part_width = query_key_value_weight.shape[3]
    units = first_dense_weight.shape[2]

    item = (
        jnp.concatenate(
            [query_key_value_weight[0].reshape(rows, -1), output_proj_weight[0].T], axis=1
        ),
        first_dense_weight[0],
        second_dense_weight[0].T,
    )
    cond = condition[:, 0].astype(F32)
    packed = jnp.concatenate(
        [
            query_value_bias[0, 0], query_value_bias[0, 1], first_dense_bias[0],
            output_proj_bias[0], second_dense_bias[0],
        ]
    ).astype(F32)[None]
    w = [[Handle((width, units), BF16) for _ in range(3)] for _ in range(2)]
    collect = [[Collect(item[t], l, w[l][t]) for t in range(3)] for l in range(2)]
    widen = [[Widen(w[l][t]) for t in range(3)] for l in range(2)]
    tokens_in = Tokens(latents_in[:, 0])
    tokens_cot = Tokens(cotangent[:, 0])

    def plan(*points):
        out = []
        for point in points:
            out.append([(task, phase) for task, phases in point for phase in phases])
        return out

    c, x = collect, widen
    modul, act_rows, biases = prologue(
        cond.reshape(2, n_dp, rows).transpose(1, 0, 2),
        modulation_weight[0],
        modulation_bias.astype(F32),
        packed,
        plan(
            [(tokens_in, "a"), (c[0][0], "a"), (c[1][0], "a")],
            [(c[0][0], "c"), (c[1][0], "c"), (c[0][1], "a"), (c[1][1], "a")]
            + [(c[0][0], "b"), (x[0][0], "a"), (c[1][0], "b")],
            [(c[0][1], "c"), (c[1][1], "c"), (c[0][2], "a"), (c[1][2], "a")]
            + [(x[0][0], "b"), (c[0][1], "b"), (x[0][1], "a"), (c[1][1], "b")],
            [],
            [(c[0][2], "c"), (c[1][2], "c"), (c[0][2], "b"), (c[1][2], "b"), (x[0][1], "b")]
            + [(tokens_in, "c"), (x[0][0], "c"), (x[0][1], "c")],
        ),
        1,
    )
    modul = modul.reshape(2, 6, width)
    bounds = [0, part_width, 2 * part_width, 2 * part_width + units, 2 * part_width + units + width]
    bqkv = jnp.concatenate(
        [
            biases[..., : bounds[1]], jnp.zeros((2, 1, part_width), F32),
            biases[..., bounds[1] : bounds[2]],
        ],
        axis=-1,
    )
    b1 = biases[..., bounds[2] : bounds[3]]
    bproj = biases[..., bounds[3] : bounds[4]]
    b2 = biases[..., bounds[4] :]

    hidden = [tokens_in.results[0]]
    att_plan = [
        plan(
            [(x[0][2], "a")],
            [],
            [],
            [(x[0][2], "b")],
            [(x[0][2], "c")],
        ),
        plan(
            [(x[1][1], "a"), (x[1][2], "a"), (tokens_cot, "a")],
            [],
            [],
            [(x[1][1], "b"), (x[1][2], "b")],
            [(x[1][1], "c"), (x[1][2], "c"), (tokens_cot, "c")],
        ),
    ]
    saved = []
    for layer in range(2):
        middle, normed, proj, att, branch = att_fwd(
            hidden[layer], modul[layer], bqkv[layer], bproj[layer], w[layer][0], att_plan[layer],
            2 + 2 * layer,
        )
        if layer == 0:
            mlp_plan = plan(
                [(x[1][0], "a")],
                [],
                [],
                [(x[1][0], "b")],
                [(x[1][0], "c")],
            )
        else:
            acts_first = Deliver(hidden[1], 0)
            mlp_plan = plan([], [], [], [], [])
        out, normed2, pre, gelu, branch2 = mlp_fwd(
            middle, modul[layer], b1[layer], b2[layer], w[layer][1], w[layer][2], mlp_plan,
            3 + 2 * layer,
        )
        saved.append((middle, normed, proj, att, branch, normed2, pre, gelu, branch2))
        hidden.append(out)

    grad = tokens_cot.results[0]
    narrow = [[None] * 3 for _ in range(2)]
    settle = [[None] * 3 for _ in range(2)]
    d_bias, d_mod, gins = {}, {}, {}
    acts_second = Deliver(hidden[2], 1, acts_first)
    for layer in (1, 0):
        middle, normed, proj, att, branch, normed2, pre, gelu, branch2 = saved[layer]
        if layer == 1:
            mlp_plan = plan(
                [(acts_first, "a"), (acts_second, "a")],
                [],
                [(acts_first, "zb"), (acts_second, "zb")],
                [],
                [(acts_first, "c"), (acts_second, "c")],
            )
        else:
            third = narrow[1][0]
            mlp_plan = plan([(third, "a")], [(third, "b")], [], [], [(third, "c")])
        gmid, dw1, dw2, db1, db2, dmod2 = mlp_bwd(
            grad, middle, modul[layer], branch2, normed2, pre, gelu, w[layer][1], w[layer][2],
            mlp_plan, 6 + 2 * (1 - layer),
        )
        narrow[layer][1], narrow[layer][2] = Narrow(dw1), Narrow(dw2)
        one, two = narrow[layer][1], narrow[layer][2]
        if layer == 0:
            settle[1][0] = Settle(narrow[1][0].results[0], 1)
            gin_second = Deliver(gins[1], 1)
        att_plan = plan(
            [(two, "a"), (one, "a")], [(two, "b"), (one, "b")], [], [], [(two, "c"), (one, "c")]
        )
        gin, dw, dbqkv, dbproj, dmod1 = att_bwd(
            gmid, hidden[layer], modul[layer], branch, normed, proj, att, w[layer][0],
            att_plan, 7 + 2 * (1 - layer),
        )
        for tensor in (1, 2):
            into = None if layer else settle[1][tensor]
            settle[layer][tensor] = Settle(narrow[layer][tensor].results[0], layer, into=into)
        narrow[layer][0] = Narrow(dw)
        gins[layer] = grad = gin
        d_bias[layer] = jnp.concatenate(
            [dbqkv[:, :part_width], dbqkv[:, 2 * part_width :], db1, dbproj, db2], axis=1
        )
        d_mod[layer] = jnp.concatenate([dmod1.reshape(-1), dmod2.reshape(-1)])

    last = narrow[0][0]
    final = Settle(jax.ShapeDtypeStruct((rows, units), BF16), 0, held=lambda: last.refs[1][0], into=settle[1][0])
    settle[0][0] = final
    gin_first = Deliver(gins[0], 0, gin_second)
    dmod = jnp.stack([d_mod[0], d_mod[1]]).reshape(2 * n_mp, 1, cols)
    dmod_all, g_bada, g_act, g_bias = epilogue(
        dmod,
        modulation_weight[0],
        jnp.stack([d_bias[0], d_bias[1]]),
        plan(
            [(gin_first, "az"), (gin_second, "az"), (last, "a"), (gin_first, "b"), (gin_second, "b")]
            + [(settle[0][2], "az"), (settle[1][2], "az")],
            [(settle[0][2], "b"), (settle[1][2], "b"), (settle[0][1], "a"), (settle[1][1], "a"), (last, "b")]
            + [(settle[0][2], "s"), (settle[1][2], "s"), (settle[0][1], "bz"), (settle[1][1], "bz")],
            [(last, "c"), (settle[1][0], "a"), (final, "a"), (settle[0][1], "s"), (settle[1][1], "s")]
            + [(settle[1][0], "bz"), (final, "bz")],
            [(settle[0][2], "c"), (settle[1][2], "c"), (settle[0][1], "c"), (settle[1][1], "c")],
            [(gin_first, "c"), (gin_second, "c"), (settle[1][0], "s"), (final, "s")]
            + [(settle[1][0], "c"), (final, "c")],
        ),
        10,
    )
    g_wada = dot_tn(act_rows, dmod_all)
    g_act = g_act.transpose(1, 0, 2).reshape(2, width)
    g_att, g_one, g_two = [settle[1][t].results[0] for t in range(3)]
    g_qkv = g_att[:, : 3 * part_width].reshape(rows, 3, part_width)
    g_proj = g_att[:, 3 * part_width :].T

    def dp_part(vec):
        size = vec.shape[-1] // n_dp
        return lax.dynamic_slice_in_dim(vec, dp * size, size, vec.ndim - 1)

    g_bias = g_bias[0]
    g_bqv = dp_part(g_bias[: bounds[2]].reshape(2, part_width))
    g_b1 = dp_part(g_bias[bounds[2] : bounds[3]])
    g_bproj = dp_part(g_bias[bounds[3] : bounds[4]])
    g_b2 = dp_part(g_bias[bounds[4] :])
    g_bada = dp_part(g_bada[0])
    _, silu_back = jax.vjp(jax.nn.silu, cond)
    g_cond = silu_back(g_act)[0][:, None]
    acts_out = acts_first.results[0][None, :, None]
    grad_input = gin_second.results[0].astype(F32)[None, :, None]
    return (
        acts_out,
        grad_input,
        g_cond,
        g_wada[None],
        g_bada[None],
        g_qkv[None],
        g_bqv[None],
        g_proj[None],
        g_bproj[None],
        g_one[None],
        g_b1[None],
        g_two.T[None],
        g_b2[None],
    )


def solution(mesh):
    sizes = mesh.shape
    grid = mesh.devices.reshape(sizes["section"], sizes["dp"], 2, sizes["mp"] // 2)
    fine = Mesh(grid, ("section", "dp", "mh", "ml"))
    mp = ("mh", "ml")
    in_specs = (
        P(None, "dp", mp, None),
        P(None, "dp", None),
        P(None, "dp", mp, None),
        P("section", "dp", mp),
        P("section", mp),
        P("section", "dp", None, mp),
        P("section", None, mp),
        P("section", mp, "dp"),
        P("section", None),
        P("section", "dp", mp),
        P("section", mp),
        P("section", mp, "dp"),
        P("section", None),
    )
    mpdp = ("mh", "ml", "dp")
    out_specs = (
        P("section", None, "dp", mp, None),
        P("section", None, "dp", mp, None),
        P(None, "dp", None),
        P("section", "dp", mp),
        P("section", mpdp),
        P("section", "dp", None, mp),
        P("section", None, mpdp),
        P("section", mp, "dp"),
        P("section", "dp"),
        P("section", "dp", mp),
        P("section", mpdp),
        P("section", mp, "dp"),
        P("section", "dp"),
    )
    return jax.shard_map(
        per_device, mesh=fine, in_specs=in_specs, out_specs=out_specs, check_vma=False
    )
```

```python
import jax
import jax.numpy as jnp
from jax import lax
from jax.experimental import pallas as pl
from jax.experimental.pallas import tpu as pltpu
from jax.sharding import Mesh
from jax.sharding import PartitionSpec as P

HEAD_SIZE = 72
EPS = 1e-06
MESH = pl.DeviceIdType.MESH
BF16 = jnp.bfloat16
F32 = jnp.float32
GELU_C = 0.7978845608028654
GELU_A = 0.044715
NT = (((1,), (1,)), ((), ()))
TN = (((0,), (0,)), ((), ()))
VMEM_LIMIT = 50 * 1024 * 1024


def dot_nn(a, b):
    return jnp.dot(a, b, preferred_element_type=F32)


def dot_nt(a, b):
    return lax.dot_general(a, b, NT, preferred_element_type=F32)


def dot_tn(a, b):
    return lax.dot_general(a, b, TN, preferred_element_type=F32)


def norm_parts(values):
    center = values - jnp.mean(values, axis=-1, keepdims=True)
    spread = jnp.mean(center * center, axis=-1, keepdims=True)
    rstd = lax.rsqrt(spread + EPS)
    return center * rstd, rstd


def norm_back(grad, normed, rstd, scale):
    dn = grad * (1.0 + scale)
    first = jnp.mean(dn, axis=-1, keepdims=True)
    second = jnp.mean(dn * normed, axis=-1, keepdims=True)
    return (dn - first - normed * second) * rstd


def col_sum(values):
    return jnp.sum(values, axis=0, keepdims=True)


def row_total(low):
    return dot_nn(jnp.ones((16, low.shape[0]), BF16), low)[0:1]


class Group:
    def __init__(self, tokens):
        self.low = lax.axis_size("ml")
        self.size = lax.axis_size("section") * self.low
        self.me = lax.axis_index("section") * self.low + lax.axis_index("ml")
        self.square = self.size == 4
        self.half = (slice(0, tokens // 2), slice(tokens // 2, tokens))

    def device(self, member):
        return (
            lax.div(member, self.low),
            lax.axis_index("dp"),
            lax.axis_index("mh"),
            lax.rem(member, self.low),
        )

    def member(self, step):
        if not self.square:
            return lax.rem(self.me + step, self.size)
        section = lax.rem(lax.axis_index("section") + lax.rem(step, 2), 2)
        low = lax.rem(lax.axis_index("ml") + lax.div(step, 2), 2)
        return section * 2 + low

    def copy(self, src, dst, send_sem, recv_sem, member):
        return pltpu.make_async_remote_copy(
            src_ref=src,
            dst_ref=dst,
            send_sem=send_sem,
            recv_sem=recv_sem,
            device_id=self.device(member),
            device_id_type=MESH,
        )

    def first_copies(self, buf, send_sem, recv_sem):
        steps = (1, 2) if self.square else range(1, self.size)
        mine = buf.at[self.me]
        return [
            self.copy(mine, mine, send_sem.at[step], recv_sem.at[self.me], self.member(step))
            for step in steps
        ]

    def relay_copy(self, buf, send_sem, recv_sem, step):
        rows = buf.at[self.member(step), self.half[step - 1]]
        return self.copy(
            rows, rows, send_sem.at[2 + step], recv_sem.at[3 + step], self.member(3 - step)
        )

    def spread(self, buf, send_sem, recv_sem):
        for copy in self.first_copies(buf, send_sem, recv_sem):
            copy.start()

    def arrive(self, buf, send_sem, recv_sem, step):
        def landed(rows, sem):
            self.copy(rows, rows, send_sem.at[1], sem, self.member(1)).wait_recv()

        if not self.square:

            @pl.when(step > 0)
            def _():
                landed(buf.at[self.member(step)], recv_sem.at[self.member(step)])

            return

        @pl.when(step == 1)
        def _():
            for near in (1, 2):
                landed(buf.at[self.member(near)], recv_sem.at[self.member(near)])
                self.relay_copy(buf, send_sem, recv_sem, near).start()

        @pl.when(step == 3)
        def _():
            for near in (1, 2):
                landed(buf.at[self.member(3), self.half[near - 1]], recv_sem.at[3 + near])

    def spread_sent(self, buf, send_sem, recv_sem):
        for copy in self.first_copies(buf, send_sem, recv_sem):
            copy.wait_send()
        if self.square:
            for step in (1, 2):
                self.relay_copy(buf, send_sem, recv_sem, step).wait_send()

    def straight(self, stage, landing, send_sem, recv_sem, step):
        rows = self.half[step - 1]
        return self.copy(
            stage.at[self.member(step), rows], landing.at[step - 1, rows],
            send_sem.at[step - 1], recv_sem.at[step - 1], self.member(step),
        )

    def corner(self, stage, landing, send_sem, recv_sem, step):
        rows = self.half[step - 1]
        return self.copy(
            stage.at[self.member(3), rows], landing.at[2, rows],
            send_sem.at[1 + step], recv_sem.at[1 + step], self.member(step),
        )

    def summed(self, landing, send_sem, recv_sem, step):
        rows = self.half[2 - step]
        return self.copy(
            landing.at[3, rows], landing.at[step - 1, rows],
            send_sem.at[3 + step], recv_sem.at[3 + step], self.member(step),
        )

    def reduce_copy(self, stage, landing, send_sem, recv_sem, member):
        return self.copy(
            stage.at[member], landing.at[self.me], send_sem.at[member], recv_sem.at[self.me], member
        )

    def give(self, stage, landing, send_sem, recv_sem, step):
        args = (stage, landing, send_sem, recv_sem)
        if not self.square:

            @pl.when(step > 0)
            def _():
                self.reduce_copy(*args, self.member(step)).start()

            return
        for near in (1, 2):

            @pl.when(step == near)
            def _():
                self.straight(*args, near).start()

        @pl.when(step == 3)
        def _():
            for near in (1, 2):
                self.corner(*args, near).start()

    def combine(self, stage, landing, send_sem, recv_sem):
        if not self.square:
            return
        for step in (1, 2):
            rows = self.half[2 - step]
            self.copy(
                landing.at[2, rows], landing.at[2, rows], send_sem.at[0], recv_sem.at[4 - step],
                self.member(1),
            ).wait_recv()
            total = stage[self.member(step), rows].astype(F32) + landing[2, rows].astype(F32)
            landing[3, rows] = total.astype(BF16)
            self.summed(landing, send_sem, recv_sem, step).start()

    def landed_sum(self, own, stage, landing, send_sem, recv_sem):
        args = (stage, landing, send_sem, recv_sem)
        total = own

        def landed(rows, sem):
            self.copy(rows, rows, send_sem.at[0], sem, self.member(1)).wait_recv()

        if self.square:
            for step in (1, 2):
                first, second = self.half[step - 1], self.half[2 - step]
                landed(landing.at[step - 1, first], recv_sem.at[step - 1])
                landed(landing.at[step - 1, second], recv_sem.at[3 + step])
                total = total + landing[step - 1].astype(F32)
            for step in (1, 2):
                self.straight(*args, step).wait_send()
                self.corner(*args, step).wait_send()
                self.summed(landing, send_sem, recv_sem, step).wait_send()
            return total
        for step in range(1, self.size):
            member = self.member(step)
            landed(landing.at[member], recv_sem.at[member])
            total = total + landing[member].astype(F32)
        for step in range(1, self.size):
            self.reduce_copy(*args, self.member(step)).wait_send()
        return total


def load(src, dst, sem):
    copy = pltpu.make_async_copy(src, dst, sem)
    copy.start()
    return [copy]


def flush(pairs, sems):
    copies = [
        pltpu.make_async_copy(src, dst, sems.at[number]) for number, (src, dst) in enumerate(pairs)
    ]
    for copy in copies:
        copy.start()
    return copies


def lane_mask(shape, head):
    lanes = lax.broadcasted_iota(jnp.int32, shape, len(shape) - 1)
    return (lanes >= head * HEAD_SIZE) & (lanes < (head + 1) * HEAD_SIZE)


def row_mask(shape, head):
    rows = lax.broadcasted_iota(jnp.int32, shape, 0)
    return (rows >= head * HEAD_SIZE) & (rows < (head + 1) * HEAD_SIZE)


def stack_heads(block):
    heads = block.shape[-1] // HEAD_SIZE
    zero = jnp.zeros_like(block)
    return jnp.concatenate(
        [jnp.where(lane_mask(block.shape, head), block, zero) for head in range(heads)], axis=0
    )


def identity(size):
    rows = lax.broadcasted_iota(jnp.int32, (size, size), 0)
    cols = lax.broadcasted_iota(jnp.int32, (size, size), 1)
    return jnp.where(rows == cols, 1.0, 0.0).astype(BF16)


def att_fwd_kernel(
    bg,
    hidden_ref, mod_ref, bias_ref, bproj_ref, w_ref,
    middle_ref, normed_out, proj_out, att_out, branch_ref,
    normed_ref, proj_ref, att_ref, out_sem,
    w_buf, wo_buf, stage, landing, w_sem, ag_send, ag_recv, rs_send, rs_recv,
):
    tokens, width = hidden_ref.shape
    group = Group(tokens)
    me, size = group.me, group.size
    part_width = att_ref.shape[-1]
    heads = part_width // HEAD_SIZE
    loads = load(w_ref, w_buf, w_sem.at[0])
    hidden = hidden_ref[...].astype(F32)
    normed, _ = norm_parts(hidden)
    normed_ref[me] = (normed * (1.0 + mod_ref[1:2]) + mod_ref[0:1]).astype(BF16)
    Place().greet()
    group.spread(normed_ref, ag_send, ag_recv)
    bg(0)
    for copy in loads:
        copy.wait()

    def project(step, carry):
        member = group.member(step)
        group.arrive(normed_ref, ag_send, ag_recv, step)
        out = dot_nn(normed_ref[member], w_buf[:, : 3 * part_width]) + bias_ref[...]
        for part in range(3):
            cols = slice(part * part_width, (part + 1) * part_width)
            proj_ref[part, member] = out[:, cols].astype(BF16)
        return carry

    wo_buf[...] = w_buf[:, 3 * part_width :]
    lax.fori_loop(0, size, project, 0)
    bg(1)
    seq = size * tokens
    keys = proj_ref[1].reshape(seq, -1)
    values = proj_ref[2].reshape(seq, -1)

    def attend(member):
        stacked = stack_heads(proj_ref[0, member])
        powered = jnp.exp(dot_nt(stacked, keys) * HEAD_SIZE**-0.5)
        probs = powered * (1.0 / jnp.sum(powered, axis=-1, keepdims=True))
        mixed = dot_nn(probs.astype(BF16), values)
        out = mixed[:tokens]
        for head in range(1, heads):
            part = mixed[head * tokens : (head + 1) * tokens]
            out = jnp.where(lane_mask(part.shape, head), part, out)
        low = out.astype(BF16)
        att_ref[member] = low
        return dot_nt(low, wo_buf[...])

    def send(step, carry):
        @pl.when(step == size)
        def _():
            group.combine(stage, landing, rs_send, rs_recv)
            bg(2)

        member = group.member(size - step)
        stage[member] = attend(member).astype(BF16)
        group.give(stage, landing, rs_send, rs_recv, size - step)
        return carry

    lax.fori_loop(1, size + 1, send, 0)
    group.spread_sent(normed_ref, ag_send, ag_recv)
    flushed = flush(
        [(normed_ref, normed_out), (proj_ref, proj_out), (att_ref, att_out)], out_sem
    )
    bg(3)
    own = stage[me].astype(F32)
    branch = group.landed_sum(own, stage, landing, rs_send, rs_recv) + bproj_ref[...]
    branch_ref[...] = branch
    middle_ref[...] = hidden_ref[...].astype(F32) + mod_ref[2:3] * branch
    bg(4)
    for copy in flushed:
        copy.wait()


def mlp_fwd_kernel(
    bg,
    middle_ref, mod_ref, b1_ref, b2_ref, w1_ref, w2_ref,
    out_ref, normed_out, pre_out, gelu_out, branch_ref,
    normed_ref, pre_ref, gelu_ref, out_sem,
    w1_buf, w2_buf, stage, landing, w_sem, ag_send, ag_recv, rs_send, rs_recv,
):
    group = Group(middle_ref.shape[0])
    me, size = group.me, group.size
    loads = load(w1_ref, w1_buf, w_sem.at[0]) + load(w2_ref, w2_buf, w_sem.at[1])
    normed, _ = norm_parts(middle_ref[...])
    normed_ref[me] = (normed * (1.0 + mod_ref[4:5]) + mod_ref[3:4]).astype(BF16)
    Place().greet()
    group.spread(normed_ref, ag_send, ag_recv)
    bg(0)
    for copy in loads:
        copy.wait()

    def dense(member):
        pre = dot_nn(normed_ref[member], w1_buf[...]) + b1_ref[...]
        pre_ref[member] = pre
        bent = jnp.tanh(GELU_C * (pre + GELU_A * pre * pre * pre))
        low = (0.5 * pre * (1.0 + bent)).astype(BF16)
        gelu_ref[member] = low
        return dot_nt(low, w2_buf[...])

    def send(step, carry):
        @pl.when(step == 1)
        def _():
            bg(1)

        member = group.member(step)
        group.arrive(normed_ref, ag_send, ag_recv, step)
        stage[member] = dense(member).astype(BF16)
        group.give(stage, landing, rs_send, rs_recv, step)
        return carry

    lax.fori_loop(0, size, send, 0)
    group.combine(stage, landing, rs_send, rs_recv)
    bg(2)
    group.spread_sent(normed_ref, ag_send, ag_recv)
    flushed = flush(
        [(normed_ref, normed_out), (pre_ref, pre_out), (gelu_ref, gelu_out)], out_sem
    )
    bg(3)
    own = stage[me].astype(F32)
    branch = group.landed_sum(own, stage, landing, rs_send, rs_recv) + b2_ref[...]
    branch_ref[...] = branch
    out_ref[...] = (middle_ref[...] + mod_ref[5:6] * branch).astype(BF16)
    bg(4)
    for copy in flushed:
        copy.wait()


def weight_grad(lhs_ref, rhs, out_ref, tile):
    def body(index, carry):
        cols = pl.ds(pl.multiple_of(index * tile, tile), tile)
        out_ref[cols, :] = dot_tn(lhs_ref[:, cols], rhs).astype(BF16)
        return carry

    lax.fori_loop(0, lhs_ref.shape[-1] // tile, body, 0)


def mlp_bwd_kernel(
    bg,
    grad_ref, middle_ref, mod_ref, branch_ref, normed_in, pre_in, gelu_in, w1_ref, w2_ref,
    gmid_ref, dw1_out, dw2_out, db1_ref, db2_ref, dmod_ref,
    dw1_ref, dw2_ref, out_sem, normed_ref, pre_ref, gelu_ref, in_sem,
    w1_buf, w2_buf, dbr, dpre, stage, landing, w_sem, ag_send, ag_recv, rs_send, rs_recv,
):
    tokens, width = grad_ref.shape
    group = Group(tokens)
    me, size = group.me, group.size
    loads = load(w2_ref, w2_buf, w_sem.at[1]) + load(pre_in, pre_ref, in_sem.at[0])
    loads += load(w1_ref, w1_buf, w_sem.at[0]) + load(gelu_in, gelu_ref, in_sem.at[1])
    loads += load(normed_in, normed_ref, in_sem.at[2])
    grad = grad_ref[...].astype(F32)
    dbr[me] = (grad * mod_ref[5:6]).astype(BF16)
    Place().greet()
    group.spread(dbr, ag_send, ag_recv)
    bg(0)
    dmod_ref[2:3] = col_sum(grad * branch_ref[...])
    for copy in loads:
        copy.wait()

    def back(member):
        dgelu = dot_nn(dbr[member], w2_buf[...])
        pre = pre_ref[member]
        bent = jnp.tanh(GELU_C * (pre + GELU_A * pre * pre * pre))
        slope = 0.5 * (1.0 + bent) + 0.5 * pre * (1.0 - bent * bent) * (
            GELU_C * (1.0 + 3.0 * GELU_A * pre * pre)
        )
        low = (dgelu * slope).astype(BF16)
        dpre[member] = low
        return dot_nt(low, w1_buf[...])

    stage[me] = back(me).astype(BF16)
    bg(1)

    def send(step, carry):
        member = group.member(step)
        group.arrive(dbr, ag_send, ag_recv, step)
        stage[member] = back(member).astype(BF16)
        group.give(stage, landing, rs_send, rs_recv, step)
        return carry

    lax.fori_loop(1, size, send, 0)
    group.combine(stage, landing, rs_send, rs_recv)
    bg(2)
    seq = size * tokens
    dpre_all = dpre[...].reshape(seq, -1)
    gelu_all = gelu_ref[...].reshape(seq, -1)
    db1_ref[...] = row_total(dpre_all)
    db2_ref[...] = row_total(dbr[...].reshape(seq, -1))
    weight_grad(normed_ref.reshape(seq, width), dpre_all, dw1_ref, 384)
    weight_grad(dbr.reshape(seq, width), gelu_all, dw2_ref, 384)
    flushed = flush([(dw1_ref, dw1_out), (dw2_ref, dw2_out)], out_sem)
    group.spread_sent(dbr, ag_send, ag_recv)
    bg(3)
    total = group.landed_sum(stage[me].astype(F32), stage, landing, rs_send, rs_recv)
    normed, rstd = norm_parts(middle_ref[...])
    dmod_ref[0:1] = col_sum(total)
    dmod_ref[1:2] = col_sum(total * normed)
    gmid_ref[...] = norm_back(total, normed, rstd, mod_ref[4:5]) + grad_ref[...].astype(F32)
    bg(4)
    for copy in flushed:
        copy.wait()


def att_bwd_kernel(
    bg,
    gmid_ref, hidden_ref, mod_ref, branch_ref, normed_in, proj_in, att_in, w_ref,
    gin_ref, dw_out, dbqkv_ref, dbproj_ref, dmod_ref,
    dw_ref, out_sem, normed_ref, proj_ref, att_ref, in_sem,
    w_buf, wo_buf, dba, dproj, dkey, dval, stage, landing, w_sem, ag_send, ag_recv, rs_send, rs_recv,
):
    tokens, width = gmid_ref.shape
    group = Group(tokens)
    me, size = group.me, group.size
    seq = size * tokens
    part_width = att_in.shape[-1]
    heads = part_width // HEAD_SIZE
    loads = load(proj_in, proj_ref, in_sem.at[0]) + load(w_ref, w_buf, w_sem.at[0])
    loads += load(att_in, att_ref, in_sem.at[1]) + load(normed_in, normed_ref, in_sem.at[2])
    gmid = gmid_ref[...]
    dba[me] = (gmid * mod_ref[2:3]).astype(BF16)
    Place().greet()
    group.spread(dba, ag_send, ag_recv)
    bg(0)
    dmod_ref[2:3] = col_sum(gmid * branch_ref[...])
    for copy in loads:
        copy.wait()
    keys = proj_ref[1].reshape(seq, part_width)
    values = proj_ref[2].reshape(seq, part_width)
    keys_t = dot_nt(identity(part_width), keys).astype(BF16)
    dkey[...] = jnp.zeros_like(dkey)
    dval[...] = jnp.zeros_like(dval)
    wo_buf[...] = w_buf[:, 3 * part_width :]

    def back(step, carry):
        @pl.when(step == 1)
        def _():
            bg(1)

        member = group.member(step)
        group.arrive(dba, ag_send, ag_recv, step)
        datt = dot_nn(dba[member], wo_buf[...]).astype(BF16)
        datt_st = stack_heads(datt)
        query_st = stack_heads(proj_ref[0, member])
        powered = jnp.exp(dot_nt(keys, query_st) * HEAD_SIZE**-0.5)
        probs = powered * (1.0 / jnp.sum(powered, axis=0, keepdims=True))
        dval[...] += dot_nn(probs.astype(BF16), datt_st)
        dprobs = dot_nt(values, datt_st)
        dscore = (probs * (dprobs - jnp.sum(probs * dprobs, axis=0, keepdims=True))).astype(BF16)
        dkey[...] += dot_nn(dscore, query_st)
        dq_t = dot_nn(keys_t, dscore)
        picked = dq_t[:, :tokens]
        for head in range(1, heads):
            part = dq_t[:, head * tokens : (head + 1) * tokens]
            picked = jnp.where(row_mask(part.shape, head), part, picked)
        low = (picked * HEAD_SIZE**-0.5).astype(BF16)
        dproj[member, :, :part_width] = dot_nt(identity(tokens), low).astype(BF16)
        return carry

    lax.fori_loop(0, size, back, 0)
    for member in range(size):
        rows = slice(member * tokens, (member + 1) * tokens)
        dproj[member, :, part_width : 2 * part_width] = (dkey[rows] * HEAD_SIZE**-0.5).astype(BF16)
        dproj[member, :, 2 * part_width :] = dval[rows].astype(BF16)

    def partial_rows(member):
        return dot_nt(dproj[member], w_buf[:, : 3 * part_width])

    def send(step, carry):
        member = group.member(size - step)
        stage[member] = partial_rows(member).astype(BF16)
        group.give(stage, landing, rs_send, rs_recv, size - step)
        return carry

    lax.fori_loop(1, size + 1, send, 0)
    group.combine(stage, landing, rs_send, rs_recv)
    bg(2)
    grads = dproj[...].reshape(seq, -1)
    dbqkv_ref[...] = row_total(grads)
    dbproj_ref[...] = row_total(dba[...].reshape(seq, width))
    mixed = att_ref[...].reshape(seq, part_width)
    normed_rows, dba_rows = normed_ref.reshape(seq, width), dba.reshape(seq, width)

    def weights(index, carry):
        cols = pl.ds(pl.multiple_of(index * 128, 128), 128)
        dw_ref[cols, : 3 * part_width] = dot_tn(normed_rows[:, cols], grads).astype(BF16)
        dw_ref[cols, 3 * part_width :] = dot_tn(dba_rows[:, cols], mixed).astype(BF16)
        return carry

    lax.fori_loop(0, width // 128, weights, 0)
    flushed = flush([(dw_ref, dw_out)], out_sem)
    group.spread_sent(dba, ag_send, ag_recv)
    bg(3)
    total = group.landed_sum(stage[me].astype(F32), stage, landing, rs_send, rs_recv)
    hidden = hidden_ref[...].astype(F32)
    normed, rstd = norm_parts(hidden)
    dmod_ref[0:1] = col_sum(total)
    dmod_ref[1:2] = col_sum(total * normed)
    gin = norm_back(total, normed, rstd, mod_ref[1:2]) + gmid_ref[...]
    gin_ref[...] = gin.astype(BF16)
    bg(4)
    for copy in flushed:
        copy.wait()


class Place:
    def __init__(self):
        self.section, self.dp = lax.axis_index("section"), lax.axis_index("dp")
        self.high, self.low = lax.axis_index("mh"), lax.axis_index("ml")
        self.n_dp, self.n_low = lax.axis_size("dp"), lax.axis_size("ml")
        self.total = 4 * self.n_dp * self.n_low
        self.me = ((self.section * self.n_dp + self.dp) * 2 + self.high) * self.n_low + self.low

    def unflatten(self, number):
        low = lax.rem(number, self.n_low)
        rest = lax.div(number, self.n_low)
        high, rest = lax.rem(rest, 2), lax.div(rest, 2)
        return lax.div(rest, self.n_dp), lax.rem(rest, self.n_dp), high, low

    def greet(self):
        barrier = pltpu.get_barrier_semaphore()
        others = []
        for sec in range(2):
            for step in range(self.n_low):
                if sec or step:
                    section = lax.rem(self.section + sec, 2)
                    others.append((section, self.dp, self.high, lax.rem(self.low + step, self.n_low)))
        for sec in range(2):
            others.append(self.plane(sec, 1 - self.high))
        for step in range(1, self.n_dp // 2):
            others.append((self.section, self.same_core(step), self.high, self.low))
        others.append(self.core_mate())
        for device in others:
            pl.semaphore_signal(barrier, inc=1, device_id=device, device_id_type=MESH)
        pl.semaphore_wait(barrier, len(others))

    def role(self, layer, number):
        same = (self.section == layer) if number < 2 else (self.section != layer)
        return same & ((self.high == layer) if number % 2 == 0 else (self.high != layer))

    def role_device(self, layer, number):
        section = layer if number < 2 else 1 - layer
        return self.plane(section, layer if number % 2 == 0 else 1 - layer)

    def greet_all(self):
        barrier = pltpu.get_barrier_semaphore()

        def body(step, carry):
            pl.semaphore_signal(
                barrier,
                inc=1,
                device_id=self.unflatten(lax.rem(self.me + step, self.total)),
                device_id_type=MESH,
            )
            return carry

        lax.fori_loop(1, self.total, body, 0)
        pl.semaphore_wait(barrier, self.total - 1)

    def copy(self, src, dst, send_sem, recv_sem, device):
        return pltpu.make_async_remote_copy(
            src_ref=src,
            dst_ref=dst,
            send_sem=send_sem,
            recv_sem=recv_sem,
            device_id=device,
            device_id_type=MESH,
        )

    def core_mate(self):
        return (self.section, self.dp + 1 - 2 * lax.rem(self.dp, 2), self.high, self.low)

    def same_core(self, step):
        return lax.rem(self.dp + 2 * step, self.n_dp)

    def plane(self, section, high):
        return (section, self.dp, high, self.low)

    def exchange(self, pick, landing, send_sem, recv_sem):
        landing[self.me] = pick((self.section, self.dp, self.high, self.low))[...]

        def copy(number):
            device = self.unflatten(number)
            return self.copy(
                pick(device), landing.at[self.me], send_sem.at[number], recv_sem.at[self.me], device
            )

        def start(step, carry):
            copy(lax.rem(self.me + step, self.total)).start()
            return carry

        def finish(step, carry):
            number = lax.rem(self.me + step, self.total)
            device = self.unflatten(number)
            self.copy(
                landing.at[number], landing.at[number], send_sem.at[number], recv_sem.at[number], device
            ).wait_recv()
            copy(number).wait_send()
            return carry

        lax.fori_loop(1, self.total, start, 0)
        return lambda: lax.fori_loop(1, self.total, finish, 0)


VM = pl.BlockSpec(memory_space=pltpu.VMEM)
ANY = pl.BlockSpec(memory_space=pltpu.HBM)
DMA = pltpu.SemaphoreType.DMA


def by_rows(count, body):
    block = count // 9 if count % 144 == 0 else count

    def step(index, carry):
        body(pl.ds(pl.multiple_of(index * block, 16), block))
        return carry

    lax.fori_loop(0, count // block, step, 0)


class Handle:
    def __init__(self, shape, dtype):
        self.shape, self.dtype = shape, dtype
        self.array = None
        self.ref = None


class Task:
    inputs = ()
    outs = ()
    scratch = ()
    handles = ()


class Collect(Task):
    def __init__(self, item, layer, handle):
        self.layer, self.handle = layer, handle
        self.inputs = ((item, VM),)
        self.handles = (handle,)
        self.chunk = item.shape[0]
        self.scratch = (DMA((2,)), DMA, DMA)

    def run(self, phase, refs):
        (item,), _, (send, recv, own) = refs
        place = Place()
        source = item
        rows = self.handle.ref.at[pl.ds(pl.multiple_of(place.dp * self.chunk, 16), self.chunk)]

        def to(number, role):
            return place.copy(
                source, rows, send.at[number], recv, place.role_device(self.layer, role)
            )

        targets = {0: (1,), 1: (2, 3), 2: (), 3: ()}
        for role in range(4):

            @pl.when(place.role(self.layer, role))
            def _():
                if phase == "a":
                    for number, target in enumerate(targets[role]):
                        to(number, target).start()
                    if role == 0:
                        pltpu.make_async_copy(source, rows, own).start()
                if phase == "b":
                    if role == 0:
                        pltpu.make_async_copy(source, rows, own).wait()
                    else:
                        place.copy(
                            rows, rows, send.at[0], recv, place.role_device(self.layer, 0)
                        ).wait_recv()
                if phase == "c":
                    for number, target in enumerate(targets[role]):
                        to(number, target).wait_send()


class Widen(Task):
    def __init__(self, handle):
        self.handle = handle
        self.handles = (handle,)
        chips = lax.axis_size("dp") // 2
        self.scratch = (DMA((chips,)),) * 4

    def rows(self, index):
        chunk = self.handle.shape[0] // lax.axis_size("dp")
        return self.handle.ref.at[pl.ds(pl.multiple_of(index * chunk, 16), chunk)]

    def run(self, phase, refs):
        _, _, (x_send, x_recv, c_send, c_recv) = refs
        place = Place()
        chips = place.n_dp // 2

        def across(step):
            return place.copy(
                self.rows(place.dp), self.rows(place.dp), x_send.at[step], x_recv.at[step],
                (place.section, place.same_core(step), place.high, place.low),
            )

        def landed(step):
            held = self.rows(place.same_core(chips - step))
            return place.copy(
                held, held, x_send.at[step], x_recv.at[step],
                (place.section, place.same_core(step), place.high, place.low),
            )

        def to_mate(step):
            held = self.rows(place.same_core(step))
            return place.copy(held, held, c_send.at[step], c_recv.at[step], place.core_mate())

        def from_mate(step):
            held = self.rows(lax.rem(place.core_mate()[1] + 2 * step, place.n_dp))
            return place.copy(held, held, c_send.at[step], c_recv.at[step], place.core_mate())

        if phase == "a":
            for step in range(1, chips):
                across(step).start()
            to_mate(0).start()
        if phase == "b":
            for step in range(1, chips):
                landed(step).wait_recv()
                to_mate(chips - step).start()
        if phase == "c":
            for step in range(chips):
                from_mate(step).wait_recv()
                to_mate(step).wait_send()
                if step:
                    across(step).wait_send()


class Narrow(Task):
    def __init__(self, grad):
        n_dp = lax.axis_size("dp")
        chips = n_dp // 2
        self.chunk = grad.shape[0] // n_dp
        block = (chips, self.chunk, grad.shape[1])
        self.inputs = ((grad, ANY),)
        self.outs = (((self.chunk, grad.shape[1]), BF16, VM),)
        self.scratch = (pltpu.VMEM(block, BF16),) * 3 + (DMA((chips,)),) * 5

    def run(self, phase, refs):
        (grad,), (out,), scratch = refs
        own, near, far, own_sem, c_send, c_recv, x_send, x_recv = scratch
        place = Place()
        chips = place.n_dp // 2

        def rows(index):
            return grad.at[pl.ds(pl.multiple_of(index * self.chunk, 16), self.chunk)]

        def to_mate(step):
            other = lax.rem(place.core_mate()[1] + 2 * step, place.n_dp)
            return place.copy(
                rows(other), near.at[step], c_send.at[step], c_recv.at[step], place.core_mate()
            )

        def load_own(step):
            return pltpu.make_async_copy(
                rows(place.same_core(step)), own.at[step], own_sem.at[step]
            )

        def across(step):
            return place.copy(
                own.at[step], far.at[step], x_send.at[step], x_recv.at[step],
                (place.section, place.same_core(step), place.high, place.low),
            )

        order = list(range(1, chips)) + [0]
        if phase == "a":
            for step in order:
                to_mate(step).start()
                load_own(step).start()
        if phase == "b":
            for step in order:
                load_own(step).wait()
                to_mate(step).wait_recv()

                def add(rows):
                    total = own[step, rows].astype(F32) + near[step, rows].astype(F32)
                    own[step, rows] = total.astype(BF16)

                by_rows(self.chunk, add)
                if step:
                    across(step).start()
        if phase == "c":
            for step in range(1, chips):
                across(step).wait_recv()

            def add(rows):
                total = own[0, rows].astype(F32)
                for step in range(1, chips):
                    total = total + far[step, rows].astype(F32)
                out[rows] = total.astype(BF16)

            by_rows(self.chunk, add)
            for step in range(chips):
                to_mate(step).wait_send()
                if step:
                    across(step).wait_send()


class Settle(Task):
    def __init__(self, part, layer, held=None, into=None):
        self.layer = layer
        self.held = held
        self.into = into
        self.inputs = () if held else ((part, ANY),)
        self.outs = () if into else ((part.shape, F32, VM),)
        self.scratch = (
            pltpu.VMEM((2,) + part.shape, BF16), pltpu.VMEM(part.shape, BF16),
            DMA((2,)), DMA((3,)), DMA,
        )

    def run(self, phase, refs):
        ins, outs, (land, temp, send, recv, own_sem) = refs
        (out,) = self.into.refs[1] if self.into else outs
        part = self.held() if self.held else ins[0]
        place = Place()
        layer = self.layer

        def to(src, dst, s, r, role):
            return place.copy(src, dst, send.at[s], recv.at[r], place.role_device(layer, role))

        def direct(role):
            if role == 2:
                return to(part, temp, 0, 2, 0)
            return to(part, land.at[0], 0, 0, 0 if role == 1 else 1)

        def relay():
            return to(temp, land.at[1], 1, 1, 1)

        for role in range(4):

            @pl.when(place.role(layer, role))
            def _():
                if phase == "z" and role == 1:
                    direct(role).start()
                if phase == "a":
                    if role > 1:
                        direct(role).start()
                    if role == 0:
                        pltpu.make_async_copy(part, land.at[1], own_sem).start()
                if phase == "b":
                    if role == 0:
                        to(temp, temp, 0, 2, 0).wait_recv()
                        relay().start()
                    if role > 1:
                        direct(role).wait_send()
                if phase == "s":
                    if role == 0:
                        relay().wait_send()
                    if role == 1:
                        direct(role).wait_send()
                if phase == "c":
                    if role == 0:
                        pltpu.make_async_copy(part, land.at[1], own_sem).wait()
                    if role < 2:
                        to(land.at[0], land.at[0], 0, 0, role).wait_recv()
                    if role == 1:
                        to(land.at[1], land.at[1], 0, 1, 1).wait_recv()
                    if role < 2:

                        def add(rows):
                            out[rows] = land[0, rows].astype(F32) + land[1, rows].astype(F32)

                        by_rows(part.shape[0], add)


class Deliver(Task):
    def __init__(self, rows, layer, into=None):
        self.layer = layer
        self.into = into
        self.inputs = ((rows, VM),)
        self.outs = () if into else (((2,) + rows.shape, rows.dtype, VM),)
        self.scratch = (pltpu.VMEM(rows.shape, rows.dtype), DMA((2,)), DMA((3,)))

    def run(self, phase, refs):
        (rows,), outs, (temp, send, recv) = refs
        (out,) = self.into.refs[1] if self.into else outs
        place = Place()
        layer = self.layer

        def to(src, dst, s, r, role):
            return place.copy(src, dst, send.at[s], recv.at[r], place.role_device(layer, role))

        def direct(role):
            if role == 2:
                return to(rows, temp, 0, 2, 0)
            return to(rows, out.at[1 - layer], 0, 0, 0 if role == 1 else 1)

        def relay():
            return to(temp, out.at[layer], 1, 1, 1)

        for role in range(4):

            @pl.when(place.role(layer, role))
            def _():
                if phase == "z" and role == 1:
                    direct(role).start()
                if phase == "a":
                    if role > 1:
                        direct(role).start()
                    if role == 0:
                        out[layer] = rows[...]
                if phase == "b" and role == 0:
                    to(temp, temp, 0, 2, 0).wait_recv()
                    relay().start()
                if phase == "c":
                    if role == 0:
                        relay().wait_send()
                    else:
                        direct(role).wait_send()
                    if role < 2:
                        to(out.at[1 - layer], out.at[1 - layer], 0, 0, role).wait_recv()
                    if role == 1:
                        to(out.at[layer], out.at[layer], 0, 1, 1).wait_recv()


class Tokens(Task):
    def __init__(self, rows):
        self.inputs = ((rows, VM),)
        self.outs = ((rows.shape[1:], rows.dtype, VM),)
        self.scratch = (DMA, DMA((2,)))

    def run(self, phase, refs):
        (rows,), (out,), (send, recv) = refs
        place = Place()
        half = rows.shape[1] // 2
        parts = (slice(0, half), slice(half, 2 * half))

        def copy(part, section):
            return place.copy(
                rows.at[1 - place.high, parts[part]], out.at[parts[part]], send, recv.at[part],
                place.plane(section, 1 - place.high),
            )

        @pl.when(place.section == place.high)
        def _():
            if phase == "a":
                copy(0, place.section).start()
                out[...] = rows[place.high]
            if phase == "c":
                copy(0, place.section).wait_send()

        @pl.when(place.section != place.high)
        def _():
            if phase == "a":
                copy(1, 1 - place.section).start()
            if phase == "c":
                copy(1, 1 - place.section).wait_send()
                copy(0, place.section).wait_recv()
                copy(1, place.section).wait_recv()


def launch(kernel, operands, outs, scratch, schedule, cid, name):
    tasks = []
    for point in schedule:
        for task, _ in point:
            if task not in tasks:
                tasks.append(task)
    operands, outs, scratch = list(operands), list(outs), list(scratch)
    n_in, n_out, n_scratch = len(operands), len(outs), len(scratch)
    spans = []
    for task in tasks:
        spans.append((len(operands), len(outs), len(scratch)))
        operands += task.inputs
        outs += task.outs
        scratch += task.scratch
    handles = []
    for task in tasks:
        for handle in task.handles:
            if handle not in handles:
                handles.append(handle)
    aliases = {}
    first_handle = len(outs)
    for handle in handles:
        if handle.array is not None:
            aliases[len(operands)] = len(outs)
            operands.append((handle.array, ANY))
        outs.append((handle.shape, handle.dtype, ANY))

    def body(*refs):
        ins = refs[: len(operands)]
        results = refs[len(operands) : len(operands) + len(outs)]
        rest = refs[len(operands) + len(outs) :]
        for number, handle in enumerate(handles):
            handle.ref = results[first_handle + number]
        views = []
        for task, (a, b, c) in zip(tasks, spans):
            views.append(
                (
                    ins[a : a + len(task.inputs)],
                    results[b : b + len(task.outs)],
                    rest[c : c + len(task.scratch)],
                )
            )
            task.refs = views[-1]

        def bg(point):
            for task, phase in schedule[point]:
                task.run(phase, task.refs)

        kernel(bg, *ins[:n_in], *results[:n_out], *rest[:n_scratch])

    done = pl.pallas_call(
        body,
        out_shape=tuple(jax.ShapeDtypeStruct(shape, dtype) for shape, dtype, _ in outs),
        in_specs=[spec for _, spec in operands],
        out_specs=tuple(spec for _, _, spec in outs),
        scratch_shapes=scratch,
        input_output_aliases=aliases,
        compiler_params=pltpu.CompilerParams(
            collective_id=cid, has_side_effects=True, vmem_limit_bytes=VMEM_LIMIT
        ),
        name=name,
    )(*[array for array, _ in operands])
    for number, handle in enumerate(handles):
        handle.array = done[first_handle + number]
        handle.ref = None
    for task, (_, b, _) in zip(tasks, spans):
        task.results = done[b : b + len(task.outs)]
    return done[:n_out]


def group_size():
    return lax.axis_size("section") * lax.axis_size("ml")


def comm_scratch(tokens, width):
    size = group_size()
    return [pltpu.VMEM((size, tokens, width), BF16)] * 2, [DMA((max(size, 6),))] * 4


def att_fwd(hidden, mod, bias, bproj, w, schedule, cid):
    tokens, width = hidden.shape
    size = group_size()
    part_width = width // size
    bufs, sems = comm_scratch(tokens, width)
    return launch(
        att_fwd_kernel,
        [(hidden, VM), (mod, VM), (bias, VM), (bproj, VM), (w.array, ANY)],
        [
            ((tokens, width), F32, VM),
            ((size, tokens, width), BF16, ANY),
            ((3, size, tokens, part_width), BF16, ANY),
            ((size, tokens, part_width), BF16, ANY),
            ((tokens, width), F32, VM),
        ],
        [
            pltpu.VMEM((size, tokens, width), BF16),
            pltpu.VMEM((3, size, tokens, part_width), BF16),
            pltpu.VMEM((size, tokens, part_width), BF16),
            DMA((3,)),
        ]
        + [pltpu.VMEM(w.shape, BF16), pltpu.VMEM((width, part_width), BF16)]
        + bufs
        + [DMA((1,))]
        + sems,
        schedule,
        cid,
        "att_fwd",
    )


def mlp_fwd(middle, mod, b1, b2, w1, w2, schedule, cid):
    tokens, width = middle.shape
    size = group_size()
    units = w1.shape[1]
    bufs, sems = comm_scratch(tokens, width)
    return launch(
        mlp_fwd_kernel,
        [(middle, VM), (mod, VM), (b1, VM), (b2, VM), (w1.array, ANY), (w2.array, ANY)],
        [
            ((tokens, width), BF16, VM),
            ((size, tokens, width), BF16, ANY),
            ((size, tokens, units), F32, ANY),
            ((size, tokens, units), BF16, ANY),
            ((tokens, width), F32, VM),
        ],
        [
            pltpu.VMEM((size, tokens, width), BF16),
            pltpu.VMEM((size, tokens, units), F32),
            pltpu.VMEM((size, tokens, units), BF16),
            DMA((3,)),
        ]
        + [pltpu.VMEM(w1.shape, BF16)] * 2 + bufs + [DMA((2,))] + sems,
        schedule,
        cid,
        "mlp_fwd",
    )


def mlp_bwd(grad, middle, mod, branch, normed, pre, gelu, w1, w2, schedule, cid):
    tokens, width = middle.shape
    size = group_size()
    units = w1.shape[1]
    bufs, sems = comm_scratch(tokens, width)
    ins = (grad, middle, mod, branch, normed, pre, gelu)
    return launch(
        mlp_bwd_kernel,
        [(array, spec) for array, spec in zip(ins, [VM] * 4 + [ANY] * 3)]
        + [(w1.array, ANY), (w2.array, ANY)],
        [
            ((tokens, width), F32, VM),
            (w1.shape, BF16, ANY),
            (w2.shape, BF16, ANY),
            ((1, units), F32, VM),
            ((1, width), F32, VM),
            ((3, width), F32, VM),
        ],
        [pltpu.VMEM(w1.shape, BF16)] * 2
        + [
            DMA((2,)),
            pltpu.VMEM(normed.shape, BF16),
            pltpu.VMEM(pre.shape, F32),
            pltpu.VMEM(gelu.shape, BF16),
            DMA((3,)),
        ]
        + [pltpu.VMEM(w1.shape, BF16)] * 2
        + [pltpu.VMEM((size, tokens, width), BF16), pltpu.VMEM((size, tokens, units), BF16)]
        + bufs
        + [DMA((2,))]
        + sems,
        schedule,
        cid,
        "mlp_bwd",
    )


def att_bwd(gmid, hidden, mod, branch, normed, proj, att, w, schedule, cid):
    tokens, width = gmid.shape
    size = group_size()
    part_width = width // size
    bufs, sems = comm_scratch(tokens, width)
    seq = size * tokens
    ins = (gmid, hidden, mod, branch, normed, proj, att)
    return launch(
        att_bwd_kernel,
        [(array, spec) for array, spec in zip(ins, [VM] * 4 + [ANY] * 3)] + [(w.array, ANY)],
        [
            ((tokens, width), BF16, VM),
            (w.shape, BF16, ANY),
            ((1, 3 * part_width), F32, VM),
            ((1, width), F32, VM),
            ((3, width), F32, VM),
        ],
        [
            pltpu.VMEM(w.shape, BF16),
            DMA((1,)),
            pltpu.VMEM(normed.shape, BF16),
            pltpu.VMEM(proj.shape, BF16),
            pltpu.VMEM(att.shape, BF16),
            DMA((3,)),
            pltpu.VMEM(w.shape, BF16),
            pltpu.VMEM((width, part_width), BF16),
            pltpu.VMEM((size, tokens, width), BF16),
            pltpu.VMEM((size, tokens, 3 * part_width), BF16),
            pltpu.VMEM((seq, part_width), F32),
            pltpu.VMEM((seq, part_width), F32),
        ]
        + bufs
        + [DMA((1,))]
        + sems,
        schedule,
        cid,
        "att_bwd",
    )


def prologue_kernel(
    bg,
    cond_ref, wada_ref, bada_ref, bias_ref,
    modul_ref, act_ref, bias_out,
    cond_land, share, land, cond_send, cond_recv, mod_send, mod_recv, b_send, b_recv,
):
    place = Place()
    section, dp, high = place.section, place.dp, place.high
    place.greet_all()

    def spread(step):
        other = lax.rem(dp + step, place.n_dp)
        return place.copy(
            cond_ref.at[other], cond_land.at[dp], cond_send.at[step], cond_recv.at[dp],
            (section, other, high, place.low),
        )

    def spread_wait(step):
        other = lax.rem(dp + step, place.n_dp)
        return place.copy(
            cond_land.at[other], cond_land.at[other], cond_send.at[step], cond_recv.at[other],
            (section, other, high, place.low),
        )

    cond_land[dp] = cond_ref[dp]
    for step in range(1, place.n_dp):
        spread(step).start()

    def bias_copy(target):
        return place.copy(
            bias_ref, bias_out.at[section], b_send.at[target], b_recv.at[section],
            place.plane(high, target),
        )

    here = section == high
    for target in range(2):

        @pl.when(jnp.logical_not(here & (high == target)))
        def _():
            bias_copy(target).start()

    @pl.when(here)
    def _():
        bias_out[section] = bias_ref[...]

    bg(0)
    for step in range(1, place.n_dp):
        spread_wait(step).wait_recv()
    parts = [cond_land[index] for index in range(place.n_dp)]
    act = jax.nn.silu(jnp.concatenate(parts, axis=0)).astype(BF16)
    act_ref[...] = act
    bias = jnp.where(dp == 0, bada_ref[...], 0.0)
    product = dot_nn(act, wada_ref[...])
    for row in range(2 * place.n_dp):
        share[row] = product[row : row + 1] + bias
    finish = place.exchange(
        lambda device: share.at[device[1] * 2 + device[2]], land, mod_send, mod_recv
    )
    bg(1)
    bg(2)
    finish()
    for layer in range(2):
        for part in range(2 * place.n_low):
            total = land[layer * place.n_dp * 2 * place.n_low + part]
            for index in range(1, place.n_dp):
                total = total + land[(layer * place.n_dp + index) * 2 * place.n_low + part]
            modul_ref[layer * 2 * place.n_low + part] = total
    bg(3)
    for step in range(1, place.n_dp):
        spread(step).wait_send()
    for target in range(2):

        @pl.when(jnp.logical_not(here & (high == target)))
        def _():
            bias_copy(target).wait_send()

        @pl.when(jnp.logical_not(here & (section == target)))
        def _():
            place.copy(
                bias_out.at[target], bias_out.at[target], b_send.at[0], b_recv.at[target],
                place.plane(section, 1 - high),
            ).wait_recv()

    bg(4)


def prologue(cond, wada, bada, bias, schedule, cid):
    n_dp, _, chunk = cond.shape
    n_mp = 2 * lax.axis_size("ml")
    total = 2 * n_dp * n_mp
    share = wada.shape[1]
    return launch(
        prologue_kernel,
        [(cond, VM), (wada, VM), (bada, VM), (bias, VM)],
        [
            ((2 * n_mp, 1, share), F32, VM),
            ((2 * n_dp, chunk), BF16, VM),
            ((2,) + bias.shape, F32, VM),
        ],
        [
            pltpu.VMEM((n_dp, 2, chunk), F32),
            pltpu.VMEM((2 * n_dp, 1, share), F32),
            pltpu.VMEM((total, 1, share), F32),
            DMA((n_dp,)),
            DMA((n_dp,)),
            DMA((total,)),
            DMA((total,)),
            DMA((2,)),
            DMA((2,)),
        ],
        schedule,
        cid,
        "prologue",
    )


def epilogue_kernel(
    bg,
    dmod_ref, wada_ref, dbias_ref,
    dmod_out, gbada_ref, gact_ref, gbias_ref,
    mod_land, act_stage, act_land, bias_land, bias_stage, bias_final,
    mod_send, mod_recv, act_send, act_recv, d_send, d_recv, b_send, b_recv,
):
    place = Place()
    section, dp, high = place.section, place.dp, place.high
    place.greet_all()
    finish_mod = place.exchange(
        lambda device: dmod_ref.at[(device[0] * 2 + device[2]) * place.n_low + device[3]],
        mod_land, mod_send, mod_recv,
    )

    def spread(step):
        other = lax.rem(dp + step, place.n_dp)
        return place.copy(
            dbias_ref, bias_land.at[dp], d_send.at[step], d_recv.at[dp],
            (section, other, high, place.low),
        )

    for step in range(1, place.n_dp):
        spread(step).start()
    bg(0)
    finish_mod()
    parts = 2 * place.n_low
    latents = []
    for index in range(place.n_dp):
        for micro in range(2):
            total = 0.0
            for sec in range(2):
                for low in range(place.n_low):
                    number = ((sec * place.n_dp + index) * 2 + micro) * place.n_low + low
                    total = total + mod_land[number]
            latents.append(total)
    dmod = jnp.concatenate(latents, axis=0).astype(BF16)
    back = dot_nt(dmod, wada_ref[...])
    for index in range(place.n_dp):
        act_stage[index] = back[2 * index : 2 * index + 2]
    finish_act = place.exchange(lambda device: act_stage.at[device[1]], act_land, act_send, act_recv)
    bias_sum = dbias_ref[...]
    for step in range(1, place.n_dp):
        other = lax.rem(dp + step, place.n_dp)
        place.copy(
            bias_land.at[other], bias_land.at[other], d_send.at[step], d_recv.at[other],
            (section, other, high, place.low),
        ).wait_recv()
        bias_sum = bias_sum + bias_land[other]
    bias_stage[...] = bias_sum

    def settle(layer):
        return place.copy(
            bias_stage.at[layer], bias_final.at[high], b_send.at[layer], b_recv.at[high],
            place.plane(layer, section),
        )

    for layer in range(2):
        here = (section == layer) & (high == section)

        @pl.when(here)
        def _():
            bias_final[high] = bias_stage[layer]

        @pl.when(jnp.logical_not(here))
        def _():
            settle(layer).start()

    bg(1)
    gbada_ref[...] = col_sum(dmod.astype(F32))
    dmod_out[...] = dmod
    bg(2)
    finish_act()
    for index in range(place.n_dp):
        total = 0.0
        for sec in range(2):
            for part in range(parts):
                total = total + act_land[(sec * place.n_dp + index) * parts + part]
        gact_ref[index] = total
    bg(3)
    for half in range(2):
        here = (section == high) & (high == half)

        @pl.when(jnp.logical_not(here))
        def _():
            place.copy(
                bias_final.at[half], bias_final.at[half], b_send.at[0], b_recv.at[half],
                place.plane(high, half),
            ).wait_recv()

    gbias_ref[...] = bias_final[0] + bias_final[1]
    for layer in range(2):

        @pl.when(jnp.logical_not((section == layer) & (high == section)))
        def _():
            settle(layer).wait_send()

    for step in range(1, place.n_dp):
        spread(step).wait_send()
    bg(4)


def epilogue(dmod, wada, dbias, schedule, cid):
    n_dp, n_mp = lax.axis_size("dp"), 2 * lax.axis_size("ml")
    total = 2 * n_dp * n_mp
    chunk, share = wada.shape
    row = dbias.shape[1:]
    return launch(
        epilogue_kernel,
        [(dmod, VM), (wada, VM), (dbias, VM)],
        [
            ((2 * n_dp, share), BF16, VM),
            ((1, share), F32, VM),
            ((n_dp, 2, chunk), F32, VM),
            (row, F32, VM),
        ],
        [
            pltpu.VMEM((total, 1, share), F32),
            pltpu.VMEM((n_dp, 2, chunk), F32),
            pltpu.VMEM((total, 2, chunk), F32),
            pltpu.VMEM((n_dp,) + dbias.shape, F32),
            pltpu.VMEM(dbias.shape, F32),
            pltpu.VMEM((2,) + row, F32),
            DMA((total,)),
            DMA((total,)),
            DMA((total,)),
            DMA((total,)),
            DMA((n_dp,)),
            DMA((n_dp,)),
            DMA((2,)),
            DMA((2,)),
        ],
        schedule,
        cid,
        "epilogue",
    )


def per_device(
    latents_in, condition, cotangent,
    modulation_weight, modulation_bias, query_key_value_weight, query_value_bias,
    output_proj_weight, output_proj_bias, first_dense_weight, first_dense_bias,
    second_dense_weight, second_dense_bias,
):
    dp = lax.axis_index("dp")
    n_dp, n_low = lax.axis_size("dp"), lax.axis_size("ml")
    n_mp = 2 * n_low
    width = latents_in.shape[-1]
    rows = modulation_weight.shape[1]
    cols = modulation_weight.shape[2]
    part_width = query_key_value_weight.shape[3]
    units = first_dense_weight.shape[2]

    item = (
        jnp.concatenate(
            [query_key_value_weight[0].reshape(rows, -1), output_proj_weight[0].T], axis=1
        ),
        first_dense_weight[0],
        second_dense_weight[0].T,
    )
    cond = condition[:, 0].astype(F32)
    packed = jnp.concatenate(
        [
            query_value_bias[0, 0], query_value_bias[0, 1], first_dense_bias[0],
            output_proj_bias[0], second_dense_bias[0],
        ]
    ).astype(F32)[None]
    w = [[Handle((width, units), BF16) for _ in range(3)] for _ in range(2)]
    collect = [[Collect(item[t], l, w[l][t]) for t in range(3)] for l in range(2)]
    widen = [[Widen(w[l][t]) for t in range(3)] for l in range(2)]
    tokens_in = Tokens(latents_in[:, 0])
    tokens_cot = Tokens(cotangent[:, 0])

    def plan(*points):
        out = []
        for point in points:
            out.append([(task, phase) for task, phases in point for phase in phases])
        return out

    c, x = collect, widen
    modul, act_rows, biases = prologue(
        cond.reshape(2, n_dp, rows).transpose(1, 0, 2),
        modulation_weight[0],
        modulation_bias.astype(F32),
        packed,
        plan(
            [(tokens_in, "a"), (c[0][0], "a"), (c[1][0], "a")],
            [(c[0][0], "c"), (c[1][0], "c"), (c[0][1], "a"), (c[1][1], "a")]
            + [(c[0][0], "b"), (x[0][0], "a"), (c[1][0], "b")],
            [(c[0][1], "c"), (c[1][1], "c"), (c[0][2], "a"), (c[1][2], "a")]
            + [(x[0][0], "b"), (c[0][1], "b"), (x[0][1], "a"), (c[1][1], "b")],
            [],
            [(c[0][2], "c"), (c[1][2], "c"), (c[0][2], "b"), (c[1][2], "b"), (x[0][1], "b")]
            + [(tokens_in, "c"), (x[0][0], "c"), (x[0][1], "c")],
        ),
        1,
    )
    modul = modul.reshape(2, 6, width)
    bounds = [0, part_width, 2 * part_width, 2 * part_width + units, 2 * part_width + units + width]
    bqkv = jnp.concatenate(
        [
            biases[..., : bounds[1]], jnp.zeros((2, 1, part_width), F32),
            biases[..., bounds[1] : bounds[2]],
        ],
        axis=-1,
    )
    b1 = biases[..., bounds[2] : bounds[3]]
    bproj = biases[..., bounds[3] : bounds[4]]
    b2 = biases[..., bounds[4] :]

    hidden = [tokens_in.results[0]]
    att_plan = [
        plan(
            [(x[0][2], "a")],
            [],
            [],
            [(x[0][2], "b")],
            [(x[0][2], "c")],
        ),
        plan(
            [(x[1][1], "a"), (x[1][2], "a"), (tokens_cot, "a")],
            [],
            [],
            [(x[1][1], "b"), (x[1][2], "b")],
            [(x[1][1], "c"), (x[1][2], "c"), (tokens_cot, "c")],
        ),
    ]
    saved = []
    for layer in range(2):
        middle, normed, proj, att, branch = att_fwd(
            hidden[layer], modul[layer], bqkv[layer], bproj[layer], w[layer][0], att_plan[layer],
            2 + 2 * layer,
        )
        if layer == 0:
            mlp_plan = plan(
                [(x[1][0], "a")],
                [],
                [],
                [(x[1][0], "b")],
                [(x[1][0], "c")],
            )
        else:
            acts_first = Deliver(hidden[1], 0)
            mlp_plan = plan([], [], [], [], [])
        out, normed2, pre, gelu, branch2 = mlp_fwd(
            middle, modul[layer], b1[layer], b2[layer], w[layer][1], w[layer][2], mlp_plan,
            3 + 2 * layer,
        )
        saved.append((middle, normed, proj, att, branch, normed2, pre, gelu, branch2))
        hidden.append(out)

    grad = tokens_cot.results[0]
    narrow = [[None] * 3 for _ in range(2)]
    settle = [[None] * 3 for _ in range(2)]
    d_bias, d_mod, gins = {}, {}, {}
    acts_second = Deliver(hidden[2], 1, acts_first)
    for layer in (1, 0):
        middle, normed, proj, att, branch, normed2, pre, gelu, branch2 = saved[layer]
        if layer == 1:
            mlp_plan = plan([], [], [], [], [])
        else:
            third = narrow[1][0]
            mlp_plan = plan([(third, "a")], [(third, "b")], [], [], [(third, "c")])
        gmid, dw1, dw2, db1, db2, dmod2 = mlp_bwd(
            grad, middle, modul[layer], branch2, normed2, pre, gelu, w[layer][1], w[layer][2],
            mlp_plan, 6 + 2 * (1 - layer),
        )
        narrow[layer][1], narrow[layer][2] = Narrow(dw1), Narrow(dw2)
        one, two = narrow[layer][1], narrow[layer][2]
        if layer == 0:
            settle[1][0] = Settle(narrow[1][0].results[0], 1)
            gin_second = Deliver(gins[1], 1)
        att_plan = plan(
            [(two, "a"), (one, "a")], [(two, "b"), (one, "b")], [], [], [(two, "c"), (one, "c")]
        )
        if layer == 1:
            for task in (acts_first, acts_second):
                att_plan[0].append((task, "a"))
                att_plan[1] += [(task, "z"), (task, "b")]
                att_plan[4].append((task, "c"))
        gin, dw, dbqkv, dbproj, dmod1 = att_bwd(
            gmid, hidden[layer], modul[layer], branch, normed, proj, att, w[layer][0],
            att_plan, 7 + 2 * (1 - layer),
        )
        for tensor in (1, 2):
            into = None if layer else settle[1][tensor]
            settle[layer][tensor] = Settle(narrow[layer][tensor].results[0], layer, into=into)
        narrow[layer][0] = Narrow(dw)
        gins[layer] = grad = gin
        d_bias[layer] = jnp.concatenate(
            [dbqkv[:, :part_width], dbqkv[:, 2 * part_width :], db1, dbproj, db2], axis=1
        )
        d_mod[layer] = jnp.concatenate([dmod1.reshape(-1), dmod2.reshape(-1)])

    last = narrow[0][0]
    final = Settle(jax.ShapeDtypeStruct((rows, units), BF16), 0, held=lambda: last.refs[1][0], into=settle[1][0])
    settle[0][0] = final
    gin_first = Deliver(gins[0], 0, gin_second)
    dmod = jnp.stack([d_mod[0], d_mod[1]]).reshape(2 * n_mp, 1, cols)
    dmod_all, g_bada, g_act, g_bias = epilogue(
        dmod,
        modulation_weight[0],
        jnp.stack([d_bias[0], d_bias[1]]),
        plan(
            [(gin_first, "az"), (gin_second, "az"), (last, "a"), (gin_first, "b"), (gin_second, "b")]
            + [(settle[0][2], "az"), (settle[1][2], "az")],
            [(settle[0][2], "b"), (settle[1][2], "b"), (settle[0][1], "a"), (settle[1][1], "a"), (last, "b")]
            + [(settle[0][2], "s"), (settle[1][2], "s"), (settle[0][1], "bz"), (settle[1][1], "bz")],
            [(last, "c"), (settle[1][0], "a"), (final, "a"), (settle[0][1], "s"), (settle[1][1], "s")]
            + [(settle[1][0], "bz"), (final, "bz")],
            [(settle[0][2], "c"), (settle[1][2], "c"), (settle[0][1], "c"), (settle[1][1], "c")],
            [(gin_first, "c"), (gin_second, "c"), (settle[1][0], "s"), (final, "s")]
            + [(settle[1][0], "c"), (final, "c")],
        ),
        10,
    )
    g_wada = dot_tn(act_rows, dmod_all)
    g_act = g_act.transpose(1, 0, 2).reshape(2, width)
    g_att, g_one, g_two = [settle[1][t].results[0] for t in range(3)]
    g_qkv = g_att[:, : 3 * part_width].reshape(rows, 3, part_width)
    g_proj = g_att[:, 3 * part_width :].T

    def dp_part(vec):
        size = vec.shape[-1] // n_dp
        return lax.dynamic_slice_in_dim(vec, dp * size, size, vec.ndim - 1)

    g_bias = g_bias[0]
    g_bqv = dp_part(g_bias[: bounds[2]].reshape(2, part_width))
    g_b1 = dp_part(g_bias[bounds[2] : bounds[3]])
    g_bproj = dp_part(g_bias[bounds[3] : bounds[4]])
    g_b2 = dp_part(g_bias[bounds[4] :])
    g_bada = dp_part(g_bada[0])
    _, silu_back = jax.vjp(jax.nn.silu, cond)
    g_cond = silu_back(g_act)[0][:, None]
    acts_out = acts_first.results[0][None, :, None]
    grad_input = gin_second.results[0].astype(F32)[None, :, None]
    return (
        acts_out,
        grad_input,
        g_cond,
        g_wada[None],
        g_bada[None],
        g_qkv[None],
        g_bqv[None],
        g_proj[None],
        g_bproj[None],
        g_one[None],
        g_b1[None],
        g_two.T[None],
        g_b2[None],
    )


def solution(mesh):
    sizes = mesh.shape
    grid = mesh.devices.reshape(sizes["section"], sizes["dp"], 2, sizes["mp"] // 2)
    fine = Mesh(grid, ("section", "dp", "mh", "ml"))
    mp = ("mh", "ml")
    in_specs = (
        P(None, "dp", mp, None),
        P(None, "dp", None),
        P(None, "dp", mp, None),
        P("section", "dp", mp),
        P("section", mp),
        P("section", "dp", None, mp),
        P("section", None, mp),
        P("section", mp, "dp"),
        P("section", None),
        P("section", "dp", mp),
        P("section", mp),
        P("section", mp, "dp"),
        P("section", None),
    )
    mpdp = ("mh", "ml", "dp")
    out_specs = (
        P("section", None, "dp", mp, None),
        P("section", None, "dp", mp, None),
        P(None, "dp", None),
        P("section", "dp", mp),
        P("section", mpdp),
        P("section", "dp", None, mp),
        P("section", None, mpdp),
        P("section", mp, "dp"),
        P("section", "dp"),
        P("section", "dp", mp),
        P("section", mpdp),
        P("section", mp, "dp"),
        P("section", "dp"),
    )
    return jax.shard_map(
        per_device, mesh=fine, in_specs=in_specs, out_specs=out_specs, check_vma=False
    )
```
